256 devices in a mesh: dp: 2 (over y_hi), tm: 32 (over z, y_lo, core), rows: 4 (over x).
Axes of the slice: x: 4, y: 4 (y_hi: 2, y_lo: 2; y = y_hi * 2 + y_lo), z: 8, core: 2. Of those that a mesh axis runs over, the one named last changes fastest.
Arguments:
- clips: bfloat16 [2, 64, 4, 128, 256], P('dp', 'tm', 'rows'), may hold values from -12 to 12
- weight: bfloat16 [3, 3, 3, 256, 256], replicated, may hold values from -0.078125 to 0.078125
- bias: float32 [256], replicated, may hold values from -1 to 1
- head: float32 [256], replicated, may hold values from -4 to 4
Outputs:
- grad_weight: float32 [3, 3, 3, 256, 256], replicated
- grad_bias: float32 [256], replicated
- grad_head: float32 [256], replicated
The draws below stay inside these ranges and needn't reach their ends.
All inputs are finite; a program needn't handle non-finite values.
Results may differ from the reference program's by a relative error of at most 0.0003.
Values may be sent and summed in bfloat16 or wider, within the bound.
A program may use at most 128 MiB of HBM per device.

```python
import jax
import jax.numpy as jnp
from jax import lax

C = 256
WID = 128
NT = 64
NH = 4
CLIPS = 2


def draw_clips(key, part):
    shape = (CLIPS, NT, NH, WID, C)
    frame_scale = 3.0 ** (jnp.arange(NT, dtype=jnp.float32) / max(NT - 1, 1))
    values = jnp.clip(jax.random.normal(key, shape, jnp.float32), -4.0, 4.0)
    return (values * frame_scale[None, :, None, None, None]).astype(jnp.bfloat16)


def centred(key, shape, width, most, kind=jnp.bfloat16):
    return jnp.clip(width * jax.random.normal(key, shape, jnp.float32), -most, most).astype(kind)


def setup_inputs(seed: int = 0) -> dict:
    seeds = jax.random.split(jax.random.key(seed), 5)
    return {
        "clips": draw_clips(jax.random.fold_in(seeds[4], 71), 0),
        "weight": centred(seeds[1], (3, 3, 3, C, C), (27 * C) ** -0.5, 0.078125),
        "bias": jnp.clip(jax.random.uniform(seeds[2], (C,), jnp.float32, -1.0, 1.0), -1.0, 1.0),
        "head": centred(seeds[3], (C,), 1.0, 4.0, jnp.float32),
    }


penalty_weight = 0.01


def conv_offsets(padded, weight, transpose):
    nclip, tpad, rpad, wpad, chans = padded.shape
    frames, rowsn, cols = tpad - 2, rpad - 2, wpad - 2
    total = jnp.zeros((nclip * frames * rowsn * cols, weight.shape[4]), jnp.float32)
    for a in range(3):
        for b in range(3):
            for d in range(3):
                if transpose:
                    piece = padded[:, 2 - a:2 - a + frames, 2 - b:2 - b + rowsn, 2 - d:2 - d + cols]
                    total = total + lax.dot_general(piece.reshape(-1, chans), weight[a, b, d], (((1,), (1,)), ((), ())), preferred_element_type=jnp.float32)
                else:
                    piece = padded[:, a:a + frames, b:b + rowsn, d:d + cols]
                    total = total + jnp.dot(piece.reshape(-1, chans), weight[a, b, d], preferred_element_type=jnp.float32)
    return total.reshape(nclip, frames, rowsn, cols, -1)


def correlate(padded, right):
    nclip, tpad, rpad, wpad, chans = padded.shape
    frames, rowsn, cols = tpad - 2, rpad - 2, wpad - 2
    right_rows = right.reshape(-1, right.shape[-1])
    blocks = []
    for a in range(3):
        for b in range(3):
            for d in range(3):
                piece = padded[:, a:a + frames, b:b + rowsn, d:d + cols].reshape(-1, chans)
                blocks.append(lax.dot_general(piece, right_rows, (((0,), (0,)), ((), ())), preferred_element_type=jnp.float32))
    return jnp.stack(blocks).reshape(3, 3, 3, chans, right.shape[-1])


def pad_all(field):
    return jnp.pad(field, ((0, 0), (1, 1), (1, 1), (1, 1), (0, 0)))


def reference(clips, weight, bias, head):
    clip_pad = pad_all(clips)
    pre = conv_offsets(clip_pad, weight, False) + bias
    sig = jax.nn.sigmoid(pre)
    slope = sig * (1.0 + pre * (1.0 - sig))
    curve = sig * (1.0 - sig) * (2.0 + pre * (1.0 - 2.0 * sig))
    score_grad = (head * slope).astype(jnp.bfloat16)
    input_grad = conv_offsets(pad_all(score_grad), weight, True).astype(jnp.bfloat16)
    grad_pad = pad_all(input_grad)
    back_grad = penalty_weight * conv_offsets(grad_pad, weight, False)
    pre_grad = back_grad * head * curve
    pre_grad_b = pre_grad.astype(jnp.bfloat16)
    grad_weight = penalty_weight * correlate(grad_pad, score_grad) + correlate(clip_pad, pre_grad_b)
    grad_bias = jnp.sum(pre_grad, axis=(0, 1, 2, 3))
    grad_head = jnp.sum(back_grad * slope, axis=(0, 1, 2, 3))
    return grad_weight, grad_bias, grad_head
```

```python
import functools
import math

import jax
import jax.numpy as jnp
from jax import lax
from jax.experimental import pallas as pl
from jax.experimental.pallas import tpu as pltpu
from jax.sharding import PartitionSpec as P

penalty_weight = 0.01
MESH = pl.DeviceIdType.MESH
SUB = 8
TAPS = 3
SPAN = 120.0


def make_plan(sizes, shares):
    dp, tm, rows = sizes
    pair = ("tm", 1, 2)
    wide, near, deep = ("rows", 1, rows), ("tm", 2, 2), ("dp", 1, dp)
    rest = (("tm", 4, tm // 4),)
    across, along, ahead = (wide, near, deep), (near, deep, wide), (deep, near, wide)
    return pair, (across, along, across, ahead, across, along), rest


def kernel(
    sizes, plan, clips_ref, weight_ref, bias_ref, head_ref,
    out_ref, bias_out, head_out,
    w_ref, clip_pad, score_pad, grad_pad, acc, slope_ref, curve_ref, cat_s, cat_p, total,
    land_pair, code, land, full, small_mine, small_land,
    local_sem, halo_send, halo_recv, pair_send, pair_recv, part_send, part_recv, gath_send, gath_recv,
    small_send, small_recv, out_sem,
):
    small_refs = (bias_out, head_out)
    dp, tm, rows = sizes
    frames, cols, chans = clips_ref.shape
    count = frames * cols
    me = {"dp": lax.axis_index("dp"), "tm": lax.axis_index("tm"), "rows": lax.axis_index("rows")}

    def device(**moved):
        place = dict(me, **moved)
        return (place["dp"], place["tm"], place["rows"])

    weight_copy = pltpu.make_async_copy(weight_ref, w_ref, local_sem.at[0])
    weight_copy.start()
    clip_copy = pltpu.make_async_copy(
        clips_ref, clip_pad.at[pl.ds(1, frames), 1], local_sem.at[1]
    )
    clip_copy.start()
    for pad in (clip_pad, score_pad, grad_pad):
        pad[:, 0] = jnp.zeros((frames + 2, cols, chans), pad.dtype)
        pad[:, 2] = jnp.zeros((frames + 2, cols, chans), pad.dtype)
        pad[0, 1] = jnp.zeros((cols, chans), pad.dtype)
        pad[frames + 1, 1] = jnp.zeros((cols, chans), pad.dtype)

    barrier = pltpu.get_barrier_semaphore()
    flat = me["tm"] * rows + me["rows"]
    plane = tm * rows

    def greet(step, carry):
        other = lax.rem(flat + step, plane)
        pl.semaphore_signal(
            barrier, inc=1, device_id=device(tm=other // rows, rows=lax.rem(other, rows)),
            device_id_type=MESH,
        )
        return carry

    lax.fori_loop(1, plane, greet, 0)
    for step in range(1, dp):
        pl.semaphore_signal(
            barrier, inc=1, device_id=device(dp=lax.rem(me["dp"] + step, dp)), device_id_type=MESH
        )
    pl.semaphore_wait(barrier, plane - 1 + dp - 1)

    moves = [(t, r) for t in (-1, 0, 1) for r in (-1, 0, 1) if (t, r) != (0, 0)]

    def inside(t, r):
        ok = None
        for axis, step, size in (("tm", t, tm), ("rows", r, rows)):
            if step:
                cond = me[axis] > 0 if step < 0 else me[axis] < size - 1
                ok = cond if ok is None else jnp.logical_and(ok, cond)
        return ok

    def halo_copy(which, pad, source, t, r):
        slot = which * len(moves) + moves.index((t, r))
        if t == 0:
            here, there = pl.ds(0, frames), pl.ds(1, frames)
        elif t > 0:
            here, there = pl.ds(frames - 1, 1), pl.ds(0, 1)
        else:
            here, there = pl.ds(0, 1), pl.ds(frames + 1, 1)
        return pltpu.make_async_remote_copy(
            src_ref=source.at[here], dst_ref=pad.at[there, 1 - r],
            send_sem=halo_send.at[slot], recv_sem=halo_recv.at[slot],
            device_id=device(tm=me["tm"] + t, rows=me["rows"] + r), device_id_type=MESH,
        )

    def halo_start(which, pad, source):
        for t, r in moves:
            @pl.when(inside(t, r))
            def _():
                halo_copy(which, pad, source, t, r).start()

    def halo_wait(which, pad, source, level):
        for t, r in moves:
            if (t == 0) != level:
                continue

            @pl.when(inside(t, r))
            def _():
                halo_copy(which, pad, source, t, r).wait_send()

            @pl.when(inside(-t, -r))
            def _():
                halo_copy(which, pad, source, t, r).wait_recv()

    column = lax.rem(lax.broadcasted_iota(jnp.int32, (count, chans), 0), cols)

    def earlier(value):
        return jnp.where(column == 0, 0.0, pltpu.roll(value, 1, 0))

    def later(value):
        return jnp.where(column == cols - 1, 0.0, pltpu.roll(value, count - 1, 0))

    def conv(which, pad, source, transpose):
        def step(a):
            base = (TAPS - 1 - a) if transpose else a
            pieces = [
                pad[pl.ds(base, frames), (TAPS - 1 - b) if transpose else b].reshape(count, chans)
                for b in range(TAPS)
            ]
            left = jnp.concatenate(pieces, axis=1)
            for d in range(TAPS):
                taps = [w_ref[(a * TAPS + b) * TAPS + d] for b in range(TAPS)]
                if transpose:
                    part = lax.dot_general(
                        left, jnp.concatenate(taps, axis=1), (((1,), (1,)), ((), ())),
                        preferred_element_type=jnp.float32,
                    )
                else:
                    part = jnp.dot(
                        left, jnp.concatenate(taps, axis=0), preferred_element_type=jnp.float32
                    )
                acc[d] = part if a == 1 else acc[d] + part

        halo_wait(which, pad, source, True)
        step(1)
        halo_wait(which, pad, source, False)
        step(0)
        step(2)
        if transpose:
            return later(acc[0]) + acc[1] + earlier(acc[2])
        return earlier(acc[0]) + acc[1] + later(acc[2])

    def shifted(value):
        value = value.astype(jnp.float32)
        return jnp.concatenate(
            [later(value), value, earlier(value)], axis=1
        ).astype(jnp.bfloat16)

    halo_start(0, clip_pad, clips_ref)
    clip_copy.wait()
    weight_copy.wait()
    pre = conv(0, clip_pad, clips_ref, False) + bias_ref[...]
    sig = jax.nn.sigmoid(pre)
    slope = sig * (1.0 + pre * (1.0 - sig))
    slope_ref[...] = slope
    curve_ref[...] = sig * (1.0 - sig) * (2.0 + pre * (1.0 - 2.0 * sig))
    score = (head_ref[...] * slope).astype(jnp.bfloat16)
    score_pad[pl.ds(1, frames), 1] = score.reshape(frames, cols, chans)
    score_own = score_pad.at[pl.ds(1, frames), 1]
    cat_s[...] = shifted(score)
    halo_start(1, score_pad, score_own)

    input_grad = conv(1, score_pad, score_own, True).astype(jnp.bfloat16)
    grad_pad[pl.ds(1, frames), 1] = input_grad.reshape(frames, cols, chans)
    grad_own = grad_pad.at[pl.ds(1, frames), 1]
    halo_start(2, grad_pad, grad_own)

    back = penalty_weight * conv(2, grad_pad, grad_own, False)
    pre_grad = back * head_ref[...] * curve_ref[...]
    cat_p[...] = shifted(pre_grad.astype(jnp.bfloat16))
    small_mine[...] = jnp.zeros_like(small_mine)
    small_mine[pl.ds(0, 1)] = jnp.sum(pre_grad, axis=0, keepdims=True)
    small_mine[pl.ds(1, 1)] = jnp.sum(back * slope_ref[...], axis=0, keepdims=True)

    pair, orders, rest = plan
    parts, shares, taps = total.shape[:3]
    lanes = land.shape[-1]
    split = chans // lanes
    half = shares // pair[2]
    units = chans // SUB

    def place_in(group):
        axis, stride, size = group
        return lax.rem(me[axis] // stride, size)

    def peer(group, step):
        axis, stride, size = group
        mine = place_in(group)
        other = lax.rem(mine + step, size)
        return other, device(**{axis: me[axis] + (other - mine) * stride})

    def pair_copy(a):
        other, target = peer(pair, 1)
        here = pl.ds(a * split, split)
        return pltpu.make_async_remote_copy(
            src_ref=total.at[here, pl.ds(other * half, half)], dst_ref=land_pair.at[here],
            send_sem=pair_send.at[a], recv_sem=pair_recv.at[a],
            device_id=target, device_id_type=MESH,
        )

    def correlate(a):
        def step(b, carry):
            dims = (((0,), (0,)), ((), ()))
            first = lax.dot_general(
                grad_pad[a : a + frames, b].reshape(count, chans), cat_s[...], dims,
                preferred_element_type=jnp.float32,
            )
            second = lax.dot_general(
                clip_pad[a : a + frames, b].reshape(count, chans), cat_p[...], dims,
                preferred_element_type=jnp.float32,
            )
            both = penalty_weight * first + second
            for d in range(TAPS):
                for p in range(split):
                    at = d * chans + p * lanes
                    total[a * split + p, :, b * TAPS + d] = both[:, at : at + lanes].reshape(
                        units, SUB, lanes
                    )
            return carry

        lax.fori_loop(0, TAPS, step, 0)
        if pair[2] > 1:
            pair_copy(a).start()

    def finish_pair(a):
        if pair[2] == 1:
            return
        mine = place_in(pair) * half
        pair_copy(a).wait()

        def add(step, carry):
            for p in range(a * split, (a + 1) * split):
                total[p, mine + step] = total[p, mine + step] + land_pair[p, step]
            return carry

        lax.fori_loop(0, half, add, 0)

    def encode(value):
        top = (jnp.max(jnp.abs(value), axis=0) * 1.01 + 1e-30).astype(jnp.bfloat16)
        rate = SPAN / top.astype(jnp.float32)
        return jnp.exp2(value * rate[None]).astype(jnp.bfloat16), top

    sems = {"part": 0, "gath": 0, "land": 0}

    def scatter_start(p, group, base, size, whole=False):
        share = size if whole else size // group[2]
        copies = []
        for step in range(1, group[2]):
            other, target = peer(group, step)
            origin = base if whole else base + other * share
            at = sems["land"]

            def fill(k, carry):
                value, top = encode(total[p, origin + k])
                code[at + k, pl.ds(0, taps)] = value
                code[at + k, taps] = top
                return carry

            lax.fori_loop(0, share, fill, 0)
            copy = pltpu.make_async_remote_copy(
                src_ref=code.at[pl.ds(at, share)], dst_ref=land.at[pl.ds(at, share)],
                send_sem=part_send.at[sems["part"]], recv_sem=part_recv.at[sems["part"]],
                device_id=target, device_id_type=MESH,
            )
            copy.start()
            copies.append((copy, at))
            sems["land"] += share
            sems["part"] += 1
        return copies, base if whole else base + place_in(group) * share, share

    def scatter_end(p, copies, base, share):
        for copy, _ in copies:
            copy.wait()
        if not copies:
            return

        def add(step, carry):
            value = total[p, base + step]
            for _, at in copies:
                value = value + decode(land[at + step], taps)
            total[p, base + step] = value
            return carry

        lax.fori_loop(0, share, add, 0)

    def gather_start(p, group, base, size):
        copies = []
        for step in range(1, group[2]):
            _, target = peer(group, step)
            block = full.at[p, pl.ds(base, size)]
            copy = pltpu.make_async_remote_copy(
                src_ref=block, dst_ref=block,
                send_sem=gath_send.at[sems["gath"]], recv_sem=gath_recv.at[sems["gath"]],
                device_id=target, device_id_type=MESH,
            )
            copy.start()
            copies.append(copy)
            sems["gath"] += 1
        return copies

    base = place_in(pair) * half
    state = [(base, half)] * parts
    trail = [[] for _ in range(parts)]
    started = [None] * parts
    depth = len(orders[0])

    def small_start(number, group, at):
        copies = []
        for step in range(1, group[2]):
            _, target = peer(group, step)
            copy = pltpu.make_async_remote_copy(
                src_ref=small_mine.at[pl.ds(number * SUB, SUB)],
                dst_ref=small_land.at[pl.ds(at * SUB, SUB)],
                send_sem=small_send.at[at], recv_sem=small_recv.at[at],
                device_id=target, device_id_type=MESH,
            )
            copy.start()
            copies.append((copy, at))
            at += 1
        return copies

    def small_end(number, copies):
        value = small_mine[pl.ds(number * SUB, SUB)]
        for copy, _ in copies:
            copy.wait()
        for _, slot in copies:
            value = value + small_land[pl.ds(slot * SUB, SUB)]
        small_mine[pl.ds((number + 1) * SUB, SUB)] = value

    def scatter(p, level):
        if level < depth:
            trail[p].append(state[p])
            started[p] = scatter_start(p, orders[p][level], *state[p])
        else:
            started[p] = scatter_start(p, rest[level - depth], *state[p], True)

    def end_scatter(p):
        copies, base, share = started[p]
        scatter_end(p, copies, base, share)
        state[p] = (base, share)

    small_groups = (pair, *orders[0], *rest)
    small_at = 0
    for a in range(TAPS):
        correlate(a)
        if a == 0:
            small = small_start(0, small_groups[0], small_at)
            small_at += len(small)
        else:
            finish_pair(a - 1)
            for p in range((a - 1) * split, a * split):
                scatter(p, 0)
    small_end(0, small)
    finish_pair(TAPS - 1)
    for p in range(parts - split, parts):
        scatter(p, 0)
    levels = depth + len(rest)
    for level in range(1, levels + 1):
        small = small_start(level, small_groups[level], small_at)
        small_at += len(small)
        for p in range(parts):
            end_scatter(p)
            if level < levels:
                scatter(p, level)
                continue
            base, size = state[p]

            def keep(k, carry):
                value, top = encode(total[p, base + k])
                full[p, base + k, pl.ds(0, taps)] = value
                full[p, base + k, taps] = top
                return carry

            lax.fori_loop(0, size, keep, 0)
            started[p] = gather_start(p, orders[p][depth - 1], *state[p])
        small_end(level, small)
    for k in range(2):
        small_refs[k][...] = small_mine[pl.ds((levels + 1) * SUB + k, 1)]
    for level in reversed(range(depth)):
        for p in range(parts):
            for copy in started[p]:
                copy.wait()
            state[p] = trail[p][level]
            group = orders[p][level - 1] if level else pair
            started[p] = gather_start(p, group, *state[p])
    outs = []
    for p in range(parts):
        for copy in started[p]:
            copy.wait()
        copy = pltpu.make_async_copy(full.at[p], out_ref.at[p], out_sem.at[p])
        copy.start()
        outs.append(copy)
    for copy in outs:
        copy.wait()


def decode(block, taps):
    unit = block[taps].astype(jnp.float32) * (1.0 / (SPAN * math.log(2.0)))
    return jnp.log(block[:taps].astype(jnp.float32)) * unit[None]


def decode_kernel(code_ref, bias_ref, head_ref, out_ref, bias_out, head_out):
    parts, shares, blocks, _, lanes = code_ref.shape
    taps = blocks - 1
    split = parts // TAPS
    for p in range(parts):
        at, lane = p // split * taps, p % split * lanes
        for k in range(shares):
            out_ref[at : at + taps, k, :, lane : lane + lanes] = decode(code_ref[p, k], taps)
    bias_out[...] = bias_ref[...]
    head_out[...] = head_ref[...]


def per_device(sizes, clips, weight, bias, head):
    _, frames, _, cols, chans = clips.shape
    count = frames * cols
    split = 2
    taps, shares, parts = TAPS**2, chans // SUB, TAPS * split
    lanes = chans // split
    plan = make_plan(sizes, shares)
    pair, orders, rest = plan
    half = shares // pair[2]
    small_n = sum(g[2] - 1 for g in (pair,) + orders[0] + rest)
    land = parts_n = gath_n = 0
    for order in orders:
        size = half
        for group in order:
            land += size // group[2] * (group[2] - 1)
            size //= group[2]
            parts_n += group[2] - 1
        for group in rest:
            land += size * (group[2] - 1)
            parts_n += group[2] - 1
        gath_n += sum(g[2] - 1 for g in order) + pair[2] - 1
    pad = pltpu.VMEM((frames + 2, 3, cols, chans), jnp.bfloat16)
    field = pltpu.VMEM((count, chans), jnp.float32)
    coded = pltpu.VMEM((max(land, 1), taps + 1, SUB, lanes), jnp.bfloat16)
    dma = pltpu.SemaphoreType.DMA
    vmem = pl.BlockSpec(memory_space=pltpu.VMEM)
    hbm = pl.BlockSpec(memory_space=pl.ANY)
    row = jax.ShapeDtypeStruct((1, chans), jnp.float32)
    code, *small = pl.pallas_call(
        functools.partial(kernel, sizes, plan),
        out_shape=(
            jax.ShapeDtypeStruct((parts, shares, taps + 1, SUB, lanes), jnp.bfloat16),
            row, row,
        ),
        in_specs=[hbm, hbm, vmem, vmem],
        out_specs=(hbm, vmem, vmem),
        scratch_shapes=[
            pltpu.VMEM((TAPS**3, chans, chans), jnp.bfloat16),
            pad, pad, pad,
            pltpu.VMEM((TAPS, count, chans), jnp.float32),
            field, field,
            pltpu.VMEM((count, TAPS * chans), jnp.bfloat16),
            pltpu.VMEM((count, TAPS * chans), jnp.bfloat16),
            pltpu.VMEM((parts, shares, taps, SUB, lanes), jnp.float32),
            pltpu.VMEM((parts, half, taps, SUB, lanes), jnp.float32),
            coded, coded,
            pltpu.VMEM((parts, shares, taps + 1, SUB, lanes), jnp.bfloat16),
            pltpu.VMEM(((len(rest) + 6) * SUB, chans), jnp.float32),
            pltpu.VMEM((max(small_n, 1) * SUB, chans), jnp.float32),
            dma((2,)), dma((24,)), dma((24,)), dma((TAPS,)), dma((TAPS,)),
            dma((max(parts_n, 1),)), dma((max(parts_n, 1),)),
            dma((max(gath_n, 1),)), dma((max(gath_n, 1),)),
            dma((max(small_n, 1),)), dma((max(small_n, 1),)), dma((parts,)),
        ],
        compiler_params=pltpu.CompilerParams(
            collective_id=0, has_side_effects=True, vmem_limit_bytes=60 * 1024 * 1024
        ),
    )(
        clips.reshape(frames, cols, chans),
        weight.reshape(TAPS**3, chans, chans),
        bias.reshape(1, chans),
        head.reshape(1, chans),
    )
    step = math.gcd(shares, 8)
    short = pl.BlockSpec((1, chans), lambda i: (0, 0))
    grad_weight, grad_bias, grad_head = pl.pallas_call(
        decode_kernel,
        out_shape=(jax.ShapeDtypeStruct((TAPS**3, shares, SUB, chans), jnp.float32), row, row),
        grid=(shares // step,),
        in_specs=[
            pl.BlockSpec((parts, step, taps + 1, SUB, lanes), lambda i: (0, i, 0, 0, 0)),
            short, short,
        ],
        out_specs=(
            pl.BlockSpec((TAPS**3, step, SUB, chans), lambda i: (0, i, 0, 0)), short, short
        ),
    )(code, *small)
    grad_weight = grad_weight.reshape(TAPS, TAPS, TAPS, chans, chans)
    return grad_weight, grad_bias.reshape(chans), grad_head.reshape(chans)


def solution(mesh):
    sizes = tuple(mesh.shape[axis] for axis in ("dp", "tm", "rows"))
    return jax.shard_map(
        functools.partial(per_device, sizes),
        mesh=mesh,
        in_specs=(P("dp", "tm", "rows", None, None), P(), P(), P()),
        out_specs=(P(), P(), P()),
        check_vma=False,
    )
```

```python
import functools
import math

import jax
import jax.numpy as jnp
from jax import lax
from jax.experimental import pallas as pl
from jax.experimental.pallas import tpu as pltpu
from jax.sharding import PartitionSpec as P

penalty_weight = 0.01
MESH = pl.DeviceIdType.MESH
SUB = 8
LANES = 128
TAPS = 3
SPAN = 120.0
RING = 4
DEEP = 8
CORES = 2
GROUPS = 4
SHARE = 7
UNITS = 16
PARTS = 2 * GROUPS


def flip(m):
    return m + 1 - 2 * lax.rem(m, 2)


def mirror(m):
    return RING - 1 - m


def kernel(
    sizes, clips_ref, weight_ref, bias_ref, head_ref,
    out_ref, bias_out, head_out,
    w_ref, clip_pad, score_pad, grad_pad, acc, slope_ref, curve_ref,
    cat_s, cat_p, stage_s, stage_p, total,
    code1, land1, code2, land2, code3, land3, code4, land4, full, small_mine, small_land,
    local_sem, halo_send, halo_recv, pair_send, pair_recv, send1, recv1, send2, recv2,
    send3, recv3, send4, recv4, zsend, zrecv, qsend, qrecv, near_send, near_recv,
    far_send, far_recv, core_send, core_recv, small_send, small_recv, out_sem,
):
    dp, tm, rows = sizes
    frames, cols, chans = clips_ref.shape
    count = frames * cols
    me = {"dp": lax.axis_index("dp"), "tm": lax.axis_index("tm"), "rows": lax.axis_index("rows")}
    core = lax.rem(me["tm"], CORES)
    here = {
        "x": me["rows"],
        "y": 2 * me["dp"] + lax.rem(me["tm"] // 2, 2),
        "z": me["tm"] // 4,
        "c": core,
    }

    def device(**moved):
        place = dict(me, **moved)
        return (place["dp"], place["tm"], place["rows"])

    def chip(**moved):
        place = dict(here, **moved)
        return (
            place["y"] // 2,
            place["z"] * 4 + lax.rem(place["y"], 2) * 2 + place["c"],
            place["x"],
        )

    partner = chip(c=1 - core)

    def ring_peers(axis, size):
        return [lax.rem(here[axis] + step, size) for step in range(1, size)]

    weight_copy = pltpu.make_async_copy(weight_ref, w_ref, local_sem.at[0])
    weight_copy.start()
    shift = 2 * core
    clip_copy = pltpu.make_async_copy(
        clips_ref, clip_pad.at[pl.ds(shift + 1, frames), 1], local_sem.at[1]
    )
    clip_copy.start()
    for pad, base in ((clip_pad, shift), (score_pad, 0), (grad_pad, shift)):
        pad[pl.ds(base, frames + 2), 0] = jnp.zeros((frames + 2, cols, chans), pad.dtype)
        pad[pl.ds(base, frames + 2), 2] = jnp.zeros((frames + 2, cols, chans), pad.dtype)
        pad[base, 1] = jnp.zeros((cols, chans), pad.dtype)
        pad[base + frames + 1, 1] = jnp.zeros((cols, chans), pad.dtype)

    moves = [(t, r) for t in (-1, 0, 1) for r in (-1, 0, 1) if (t, r) != (0, 0)]

    def inside(t, r):
        ok = None
        for axis, step, size in (("tm", t, tm), ("rows", r, rows)):
            if step:
                cond = me[axis] > 0 if step < 0 else me[axis] < size - 1
                ok = cond if ok is None else jnp.logical_and(ok, cond)
        return ok

    barrier = pltpu.get_barrier_semaphore()
    friends = [partner]
    friends += [chip(x=other) for other in ring_peers("x", RING)]
    friends += [chip(y=other) for other in ring_peers("y", RING)]
    friends += [chip(z=other) for other in ring_peers("z", DEEP)]
    for friend in friends:
        pl.semaphore_signal(barrier, inc=1, device_id=friend, device_id_type=MESH)
    corners = [(t, r) for t, r in moves if t != 0]
    for t, r in corners:
        @pl.when(inside(t, r))
        def _():
            pl.semaphore_signal(
                barrier, inc=1, device_id=device(tm=me["tm"] + t, rows=me["rows"] + r),
                device_id_type=MESH,
            )
    expected = len(friends)
    for t, r in corners:
        expected = expected + inside(t, r).astype(jnp.int32)
    pl.semaphore_wait(barrier, expected)

    def halo_copy(which, pad, source, t, r):
        slot = which * len(moves) + moves.index((t, r))
        wide = pad.shape[0] > frames + 2
        base = 0
        if wide:
            base = shift if t == 0 else 2 - shift
        if t == 0:
            src, dst = pl.ds(0, frames), pl.ds(base + 1, frames)
        elif t > 0:
            src, dst = pl.ds(frames - 1, 1), pl.ds(base, 1)
        else:
            src, dst = pl.ds(0, 1), pl.ds(base + frames + 1, 1)
        return pltpu.make_async_remote_copy(
            src_ref=source.at[src], dst_ref=pad.at[dst, 1 - r],
            send_sem=halo_send.at[slot], recv_sem=halo_recv.at[slot],
            device_id=device(tm=me["tm"] + t, rows=me["rows"] + r), device_id_type=MESH,
        )

    def halo_start(which, pad, source):
        for t, r in sorted(moves, key=lambda move: move[0] != 0):
            @pl.when(inside(t, r))
            def _():
                halo_copy(which, pad, source, t, r).start()

    def halo_wait(which, pad, source, level):
        for t, r in moves:
            if (t == 0) != level:
                continue

            @pl.when(inside(t, r))
            def _():
                halo_copy(which, pad, source, t, r).wait_send()

            @pl.when(inside(-t, -r))
            def _():
                halo_copy(which, pad, source, t, r).wait_recv()

    column = lax.rem(lax.broadcasted_iota(jnp.int32, (count, chans), 0), cols)

    def earlier(value):
        return jnp.where(column == 0, 0.0, pltpu.roll(value, 1, 0))

    def later(value):
        return jnp.where(column == cols - 1, 0.0, pltpu.roll(value, count - 1, 0))

    def send(src, dst, send_sem, recv_sem, target):
        return pltpu.make_async_remote_copy(
            src_ref=src, dst_ref=dst, send_sem=send_sem, recv_sem=recv_sem,
            device_id=target, device_id_type=MESH,
        )

    def pair_frames(pad, slot):
        block = pad.at[pl.ds(4 * core, 2)]
        return send(block, block, pair_send.at[slot], pair_recv.at[slot], partner)

    def conv(which, pad, source, transpose, ready=None):
        base = shift if pad.shape[0] > frames + 2 else 0

        def step(a):
            at = base + ((TAPS - 1 - a) if transpose else a)
            pieces = [
                pad[pl.ds(at, frames), (TAPS - 1 - b) if transpose else b].reshape(count, chans)
                for b in range(TAPS)
            ]
            left = jnp.concatenate(pieces, axis=1)
            for d in range(TAPS):
                taps = [w_ref[(a * TAPS + b) * TAPS + d] for b in range(TAPS)]
                if transpose:
                    part = lax.dot_general(
                        left, jnp.concatenate(taps, axis=1), (((1,), (1,)), ((), ())),
                        preferred_element_type=jnp.float32,
                    )
                else:
                    part = jnp.dot(
                        left, jnp.concatenate(taps, axis=0), preferred_element_type=jnp.float32
                    )
                acc[d] = part if a == 1 else acc[d] + part

        halo_wait(which, pad, source, True)
        step(1)
        halo_wait(which, pad, source, False)
        if ready is not None:
            ready()
        step(0)
        step(2)
        if transpose:
            return later(acc[0]) + acc[1] + earlier(acc[2])
        return earlier(acc[0]) + acc[1] + later(acc[2])

    def split_pair(value, cat, stage, slot):
        value = value.astype(jnp.float32)
        three = [later(value), value, earlier(value)]
        low = jnp.concatenate([v[:, :LANES] for v in three], axis=1)
        high = jnp.concatenate([v[:, LANES:] for v in three], axis=1)
        first = core == 0
        cat[core] = jnp.where(first, low, high).astype(jnp.bfloat16)
        stage[...] = jnp.where(first, high, low).astype(jnp.bfloat16)
        copy = send(stage, cat.at[core], pair_send.at[slot], pair_recv.at[slot], partner)
        copy.start()
        return copy

    halo_start(0, clip_pad, clips_ref)
    clip_copy.wait()
    weight_copy.wait()
    pair_clips, pair_grads = pair_frames(clip_pad, 0), pair_frames(grad_pad, 1)
    pre = conv(0, clip_pad, clips_ref, False, pair_clips.start) + bias_ref[...]
    sig = jax.nn.sigmoid(pre)
    slope = sig * (1.0 + pre * (1.0 - sig))
    slope_ref[...] = slope
    curve_ref[...] = sig * (1.0 - sig) * (2.0 + pre * (1.0 - 2.0 * sig))
    score = (head_ref[...] * slope).astype(jnp.bfloat16)
    score_pad[pl.ds(1, frames), 1] = score.reshape(frames, cols, chans)
    score_own = score_pad.at[pl.ds(1, frames), 1]
    halo_start(1, score_pad, score_own)
    pair_s = split_pair(score, cat_s, stage_s, 2)

    input_grad = conv(1, score_pad, score_own, True).astype(jnp.bfloat16)
    grad_pad[pl.ds(shift + 1, frames), 1] = input_grad.reshape(frames, cols, chans)
    grad_own = grad_pad.at[pl.ds(shift + 1, frames), 1]
    halo_start(2, grad_pad, grad_own)

    back = penalty_weight * conv(2, grad_pad, grad_own, False, pair_grads.start)
    pre_grad = back * head_ref[...] * curve_ref[...]
    pair_p = split_pair(pre_grad.astype(jnp.bfloat16), cat_p, stage_p, 3)

    small_mine[...] = jnp.zeros_like(small_mine)
    for k, value in enumerate((pre_grad, back * slope_ref[...])):
        whole = jnp.sum(value, axis=0, keepdims=True)
        small_mine[pl.ds(2 * k, 1)] = whole[:, :LANES]
        small_mine[pl.ds(2 * k + 1, 1)] = whole[:, LANES:]
    small_targets = [
        [partner],
        [chip(x=other) for other in ring_peers("x", RING)],
        [chip(y=other) for other in ring_peers("y", RING)],
        [chip(z=other) for other in ring_peers("z", DEEP)],
    ]
    sent = []
    smalls = []

    def small_start(level):
        at = sum(len(group) for group in small_targets[:level])
        copies = []
        for k, target in enumerate(small_targets[level]):
            copy = send(
                small_mine.at[pl.ds(level * SUB, SUB)], small_land.at[pl.ds((at + k) * SUB, SUB)],
                small_send.at[at + k], small_recv.at[at + k], target,
            )
            copy.start()
            copies.append((copy, at + k))
        smalls.append(copies)

    def small_end(level):
        value = small_mine[pl.ds(level * SUB, SUB)]
        for copy, slot in smalls[level]:
            copy.wait_recv()
            sent.append(copy)
            value = value + small_land[pl.ds(slot * SUB, SUB)]
        small_mine[pl.ds((level + 1) * SUB, SUB)] = value

    small_start(0)

    routes = []
    for p in range(PARTS):
        first, second = ("x", "y") if p < GROUPS else ("y", "x")
        m, n = here[first], here[second]
        if p % 2 == 0:
            near, bit1, far, bit2 = flip(m), lax.rem((m + 1) // 2, 2), mirror(m), m // 2
        else:
            near, bit1, far, bit2 = mirror(m), m // 2, flip(m), lax.rem(m, 2)
        eight = 8 * bit1
        four = eight + 4 * bit2
        routes.append(dict(
            near=chip(**{first: near}), far=chip(**{first: far}),
            eight=eight, other8=8 - eight, four=four, other4=2 * eight + 4 - four,
            unit=four + n, second=second,
        ))

    def encode(p, base, units, code, at):
        def peak(k, top):
            for t in range(SHARE):
                top = jnp.maximum(top, jnp.abs(total[p, base + k, t]))
            return top

        zero = jnp.zeros((SUB, LANES), jnp.float32)
        top = peak(0, zero) if units == 1 else lax.fori_loop(0, units, peak, zero)
        top = (top * 1.01 + 1e-30).astype(jnp.bfloat16)
        rate = SPAN / top.astype(jnp.float32)
        code[(*at, units * SHARE)] = top

        def fill(k, carry):
            code[(*at, pl.ds(k * SHARE, SHARE))] = jnp.exp2(
                total[p, base + k] * rate[None]
            ).astype(jnp.bfloat16)
            return carry

        if units == 1:
            fill(0, 0)
        else:
            lax.fori_loop(0, units, fill, 0)

    def absorb(p, base, units, lands):
        scales = [
            land[(*at, units * SHARE)].astype(jnp.float32) * (1.0 / (SPAN * math.log(2.0)))
            for land, at in lands
        ]

        def add(k, carry):
            value = total[p, base + k]
            for (land, at), scale in zip(lands, scales):
                block = land[(*at, pl.ds(k * SHARE, SHARE))].astype(jnp.float32)
                value = value + jnp.log(block) * scale[None]
            total[p, base + k] = value
            return carry

        if units == 1:
            add(0, 0)
        else:
            lax.fori_loop(0, units, add, 0)

    def copy1(p):
        return send(code1.at[p], land1.at[p], send1.at[p], recv1.at[p], routes[p]["near"])

    def copy2(p):
        return send(code2.at[p], land2.at[p], send2.at[p], recv2.at[p], routes[p]["far"])

    def copy3(p):
        second = routes[p]["second"]
        return [
            send(
                code3.at[p, k], land3.at[p, k], send3.at[p * 3 + k], recv3.at[p * 3 + k],
                chip(**{second: other}),
            )
            for k, other in enumerate(ring_peers(second, RING))
        ]

    def start1(p):
        encode(p, routes[p]["other8"], 8, code1, (p,))
        copy1(p).start()
        sent.append(copy1(p))

    def start2(p):
        encode(p, routes[p]["other4"], 4, code2, (p,))
        copy2(p).start()
        sent.append(copy2(p))

    def start3(p):
        second = routes[p]["second"]
        for k, (copy, other) in enumerate(zip(copy3(p), ring_peers(second, RING))):
            encode(p, routes[p]["four"] + other, 1, code3, (p, k))
            copy.start()
            sent.append(copy)

    def correlate(pad, cat, a, b):
        left = pad[a : a + 2 * frames, b].reshape(2 * count, chans)
        right = cat[...].reshape(2 * count, TAPS * LANES)
        return lax.dot_general(
            left, right, (((0,), (0,)), ((), ())), preferred_element_type=jnp.float32
        )

    def tiles(value, h, d):
        block = value[h * UNITS * SUB : (h + 1) * UNITS * SUB, d * LANES : (d + 1) * LANES]
        return block.reshape(UNITS, SUB, LANES)

    def place(a, b, d):
        tap = (a * TAPS + b) * TAPS + d
        return tap // SHARE, tap % SHARE

    for h in range(2):
        total[h * GROUPS + GROUPS - 1, :, SHARE - 1] = jnp.zeros((UNITS, SUB, LANES), jnp.float32)
    pair_s.wait()
    pair_grads.wait()
    for b in range(TAPS):
        first = penalty_weight * correlate(grad_pad, cat_s, 0, b)
        for d in range(TAPS):
            g, t = place(0, b, d)
            for h in range(2):
                total[h * GROUPS + g, :, t] = tiles(first, h, d)
    pair_clips.wait()
    pair_p.wait()
    begun = 0
    for a in range(TAPS):
        for b in range(TAPS):
            value = correlate(clip_pad, cat_p, a, b)
            if a > 0:
                value = value + penalty_weight * correlate(grad_pad, cat_s, a, b)
            for d in range(TAPS):
                g, t = place(a, b, d)
                for h in range(2):
                    p = h * GROUPS + g
                    block = tiles(value, h, d)
                    total[p, :, t] = block + total[p, :, t] if a == 0 else block
            done = (a * TAPS + b + 1) * TAPS
            while begun < GROUPS and done >= min((begun + 1) * SHARE, TAPS**3):
                for h in range(2):
                    start1(h * GROUPS + begun)
                begun += 1

    small_end(0)
    small_start(1)
    order = [h * GROUPS + g for g in range(GROUPS) for h in range(2)]
    for p in order:
        copy1(p).wait_recv()
        absorb(p, routes[p]["eight"], 8, [(land1, (p,))])
        start2(p)
    small_end(1)
    small_start(2)
    for p in order:
        copy2(p).wait_recv()
        absorb(p, routes[p]["four"], 4, [(land2, (p,))])
        start3(p)
    small_end(2)
    small_start(3)

    z = here["z"]

    def copy4(p):
        return send(code4.at[p], land4.at[z], send4.at[p], recv4.at[z], chip(z=p))

    def got4(p):
        return send(code4.at[p], land4.at[p], send4.at[p], recv4.at[p], chip(z=p))

    for p in order:
        for copy in copy3(p):
            copy.wait_recv()
        absorb(p, routes[p]["unit"], 1, [(land3, (p, k)) for k in range(RING - 1)])

        @pl.when(z != p)
        def _():
            encode(p, routes[p]["unit"], 1, code4, (p,))
            copy4(p).start()

    unit = None
    for p in range(PARTS):
        term = jnp.where(z == p, routes[p]["unit"], 0)
        unit = term if unit is None else unit + term
    others = ring_peers("z", DEEP)
    for other in others:
        send(
            code4.at[other], land4.at[other], send4.at[other], recv4.at[other], chip(z=other)
        ).wait_recv()
    absorb(z, unit, 1, [(land4, (other,)) for other in others])
    encode(z, unit, 1, full, (z, core, unit))

    def zcopy(k, other):
        block = full.at[z, core, unit]
        return send(block, block, zsend.at[k], zrecv.at[z], chip(z=other))

    def zgot(p):
        block = full.at[p, core, routes[p]["unit"]]
        return send(block, block, zsend.at[0], zrecv.at[p], chip(z=p))

    for k, other in enumerate(others):
        zcopy(k, other).start()
        sent.append(zcopy(k, other))
    small_end(3)

    def qcopies(p):
        second = routes[p]["second"]
        block = full.at[p, core, routes[p]["unit"]]
        return [
            send(block, block, qsend.at[p * 3 + k], qrecv.at[p * 3 + k], chip(**{second: other}))
            for k, other in enumerate(ring_peers(second, RING))
        ]

    def far_copy(p):
        block = full.at[p, core, pl.ds(routes[p]["four"], 4)]
        return send(block, block, far_send.at[p], far_recv.at[p], routes[p]["far"])

    def near_copy(p):
        block = full.at[p, core, pl.ds(routes[p]["eight"], 8)]
        return send(block, block, near_send.at[p], near_recv.at[p], routes[p]["near"])

    def core_copy(p, second):
        base = routes[p]["other8"] if second else routes[p]["eight"]
        block = full.at[p, core, pl.ds(base, 8)]
        slot = 2 * p + second
        return send(block, block, core_send.at[slot], core_recv.at[slot], partner)

    for p in order:
        @pl.when(z != p)
        def _():
            zgot(p).wait_recv()

        for copy in qcopies(p):
            copy.start()
            sent.append(copy)
    for p in order:
        for copy in qcopies(p):
            copy.wait_recv()
        far_copy(p).start()
        sent.append(far_copy(p))
    for p in order:
        far_copy(p).wait_recv()
        near_copy(p).start()
        core_copy(p, 0).start()
        sent += [near_copy(p), core_copy(p, 0)]
    for p in order:
        near_copy(p).wait_recv()
        core_copy(p, 1).start()
        sent.append(core_copy(p, 1))
    for k, ref in enumerate((bias_out, head_out)):
        at = (len(small_targets)) * SUB + 2 * k
        ref[:, pl.ds(0, LANES)] = small_mine[pl.ds(at, 1)]
        ref[:, pl.ds(LANES, LANES)] = small_mine[pl.ds(at + 1, 1)]
    outs = []
    for p in order:
        core_copy(p, 0).wait_recv()
        core_copy(p, 1).wait_recv()
        copy = pltpu.make_async_copy(full.at[p], out_ref.at[p], out_sem.at[p])
        copy.start()
        outs.append(copy)
    for copy in sent:
        copy.wait_send()
    for p in range(PARTS):
        @pl.when(z != p)
        def _():
            copy4(p).wait_send()
    for copy in outs:
        copy.wait()


def decode_kernel(code_ref, bias_ref, head_ref, out_ref, bias_out, head_out):
    step = code_ref.shape[2]
    for g in range(GROUPS):
        taps = min(SHARE, TAPS**3 - g * SHARE)
        for c in range(CORES):
            for k in range(step):
                unit = code_ref[g, c, k, SHARE].astype(jnp.float32) * (1.0 / (SPAN * math.log(2.0)))
                block = code_ref[g, c, k, pl.ds(0, taps)].astype(jnp.float32)
                out_ref[pl.ds(g * SHARE, taps), k, :, pl.ds(c * LANES, LANES)] = (
                    jnp.log(block) * unit[None]
                )
    bias_out[...] = bias_ref[...]
    head_out[...] = head_ref[...]


def per_device(sizes, clips, weight, bias, head):
    _, frames, _, cols, chans = clips.shape
    count = frames * cols
    dp, tm, rows = sizes
    assert (rows, dp * 2, tm // 4, chans) == (RING, RING, DEEP, 2 * LANES)
    dma = pltpu.SemaphoreType.DMA
    vmem = pl.BlockSpec(memory_space=pltpu.VMEM)
    hbm = pl.BlockSpec(memory_space=pl.ANY)
    row = jax.ShapeDtypeStruct((1, chans), jnp.float32)
    field = pltpu.VMEM((count, chans), jnp.float32)

    def pad(n):
        return pltpu.VMEM((n, 3, cols, chans), jnp.bfloat16)

    def coded(*lead, units):
        return pltpu.VMEM((*lead, units * SHARE + 1, SUB, LANES), jnp.bfloat16)

    cat = pltpu.VMEM((CORES, count, TAPS * LANES), jnp.bfloat16)
    stage = pltpu.VMEM((count, TAPS * LANES), jnp.bfloat16)
    smalls = 1 + 2 * (RING - 1) + DEEP - 1
    both = lambda n: [dma((n,)), dma((n,))]
    code, *small = pl.pallas_call(
        functools.partial(kernel, sizes),
        out_shape=(
            jax.ShapeDtypeStruct((PARTS, CORES, UNITS, SHARE + 1, SUB, LANES), jnp.bfloat16),
            row, row,
        ),
        in_specs=[hbm, hbm, vmem, vmem],
        out_specs=(hbm, vmem, vmem),
        scratch_shapes=[
            pltpu.VMEM((TAPS**3, chans, chans), jnp.bfloat16),
            pad(2 * frames + 2), pad(frames + 2), pad(2 * frames + 2),
            pltpu.VMEM((TAPS, count, chans), jnp.float32),
            field, field,
            cat, cat, stage, stage,
            pltpu.VMEM((PARTS, UNITS, SHARE, SUB, LANES), jnp.float32),
            coded(PARTS, units=8), coded(PARTS, units=8),
            coded(PARTS, units=4), coded(PARTS, units=4),
            coded(PARTS, RING - 1, units=1), coded(PARTS, RING - 1, units=1),
            coded(DEEP, units=1), coded(DEEP, units=1),
            coded(PARTS, CORES, UNITS, units=1),
            pltpu.VMEM((5 * SUB, LANES), jnp.float32),
            pltpu.VMEM((smalls * SUB, LANES), jnp.float32),
            dma((2,)), *both(24), *both(4), *both(PARTS), *both(PARTS),
            *both(PARTS * 3), *both(DEEP), *both(DEEP), *both(PARTS * 3), *both(PARTS),
            *both(PARTS), *both(2 * PARTS), *both(smalls), dma((PARTS,)),
        ],
        compiler_params=pltpu.CompilerParams(
            collective_id=0, has_side_effects=True, vmem_limit_bytes=60 * 1024 * 1024
        ),
    )(
        clips.reshape(frames, cols, chans),
        weight.reshape(TAPS**3, chans, chans),
        bias.reshape(1, chans),
        head.reshape(1, chans),
    )
    step = 4
    turns = UNITS // step
    short = pl.BlockSpec((1, chans), lambda h, i: (0, 0))
    grad_weight, grad_bias, grad_head = pl.pallas_call(
        decode_kernel,
        out_shape=(jax.ShapeDtypeStruct((TAPS**3, 2 * UNITS, SUB, chans), jnp.float32), row, row),
        grid=(2, turns),
        in_specs=[
            pl.BlockSpec(
                (GROUPS, CORES, step, SHARE + 1, SUB, LANES), lambda h, i: (h, 0, i, 0, 0, 0)
            ),
            short, short,
        ],
        out_specs=(
            pl.BlockSpec((TAPS**3, step, SUB, chans), lambda h, i: (0, h * turns + i, 0, 0)),
            short, short,
        ),
    )(code, *small)
    grad_weight = grad_weight.reshape(TAPS, TAPS, TAPS, chans, chans)
    return grad_weight, grad_bias.reshape(chans), grad_head.reshape(chans)


def solution(mesh):
    sizes = tuple(mesh.shape[axis] for axis in ("dp", "tm", "rows"))
    return jax.shard_map(
        functools.partial(per_device, sizes),
        mesh=mesh,
        in_specs=(P("dp", "tm", "rows", None, None), P(), P(), P()),
        out_specs=(P(), P(), P()),
        check_vma=False,
    )
```

```python
import functools
import math

import jax
import jax.numpy as jnp
from jax import lax
from jax.experimental import pallas as pl
from jax.experimental.pallas import tpu as pltpu
from jax.sharding import PartitionSpec as P

penalty_weight = 0.01
MESH = pl.DeviceIdType.MESH
SUB = 8
LANES = 128
TAPS = 3
SPAN = 120.0
RING = 4
DEEP = 8
CORES = 2
GROUPS = 4
SHARE = 7
UNITS = 16
PARTS = 2 * GROUPS


def flip(m):
    return m + 1 - 2 * lax.rem(m, 2)


def mirror(m):
    return RING - 1 - m


def kernel(
    sizes, clips_ref, weight_ref, bias_hbm, head_hbm,
    out_ref, bias_out, head_out,
    bias_ref, head_ref, w_ref, clip_pad, score_pad, grad_pad, acc, slope_ref, curve_ref,
    cat_s, cat_p, stage_s, stage_p, total,
    code1, land1, code2, land2, code3, land3, code4, land4, full, small_mine, small_land,
    local_sem, halo_send, halo_recv, pair_send, pair_recv, send1, recv1, send2, recv2,
    send3, recv3, send4, recv4, zsend, zrecv, qsend, qrecv, near_send, near_recv,
    far_send, far_recv, core_send, core_recv, small_send, small_recv,
):
    dp, tm, rows = sizes
    frames, cols, chans = clips_ref.shape
    count = frames * cols
    me = {"dp": lax.axis_index("dp"), "tm": lax.axis_index("tm"), "rows": lax.axis_index("rows")}
    core = lax.rem(me["tm"], CORES)
    here = {
        "x": me["rows"],
        "y": 2 * me["dp"] + lax.rem(me["tm"] // 2, 2),
        "z": me["tm"] // 4,
        "c": core,
    }

    def device(**moved):
        place = dict(me, **moved)
        return (place["dp"], place["tm"], place["rows"])

    def chip(**moved):
        place = dict(here, **moved)
        return (
            place["y"] // 2,
            place["z"] * 4 + lax.rem(place["y"], 2) * 2 + place["c"],
            place["x"],
        )

    partner = chip(c=1 - core)

    def ring_peers(axis, size):
        return [lax.rem(here[axis] + step, size) for step in range(1, size)]

    weight_copy = pltpu.make_async_copy(weight_ref, w_ref, local_sem.at[0])
    weight_copy.start()
    shift = 2 * core
    clip_copy = pltpu.make_async_copy(
        clips_ref, clip_pad.at[pl.ds(shift + 1, frames), 1], local_sem.at[1]
    )
    clip_copy.start()
    bias_copy = pltpu.make_async_copy(bias_hbm, bias_ref, local_sem.at[2])
    head_copy = pltpu.make_async_copy(head_hbm, head_ref, local_sem.at[3])
    bias_copy.start()
    head_copy.start()
    for pad, base in ((clip_pad, shift), (score_pad, 0), (grad_pad, shift)):
        pad[pl.ds(base, frames + 2), 0] = jnp.zeros((frames + 2, cols, chans), pad.dtype)
        pad[pl.ds(base, frames + 2), 2] = jnp.zeros((frames + 2, cols, chans), pad.dtype)
        pad[base, 1] = jnp.zeros((cols, chans), pad.dtype)
        pad[base + frames + 1, 1] = jnp.zeros((cols, chans), pad.dtype)

    moves = [(t, r) for t in (-1, 0, 1) for r in (-1, 0, 1) if (t, r) != (0, 0)]

    def inside(t, r):
        ok = None
        for axis, step, size in (("tm", t, tm), ("rows", r, rows)):
            if step:
                cond = me[axis] > 0 if step < 0 else me[axis] < size - 1
                ok = cond if ok is None else jnp.logical_and(ok, cond)
        return ok

    barrier = pltpu.get_barrier_semaphore()
    friends = [partner]
    friends += [chip(x=other) for other in ring_peers("x", RING)]
    friends += [chip(y=other) for other in ring_peers("y", RING)]
    friends += [chip(z=other) for other in ring_peers("z", DEEP)]
    for friend in friends:
        pl.semaphore_signal(barrier, inc=1, device_id=friend, device_id_type=MESH)
    corners = [(t, r) for t, r in moves if t != 0]
    for t, r in corners:
        @pl.when(inside(t, r))
        def _():
            pl.semaphore_signal(
                barrier, inc=1, device_id=device(tm=me["tm"] + t, rows=me["rows"] + r),
                device_id_type=MESH,
            )
    expected = len(friends)
    for t, r in corners:
        expected = expected + inside(t, r).astype(jnp.int32)
    pl.semaphore_wait(barrier, expected)

    def halo_copy(which, pad, source, t, r):
        slot = which * len(moves) + moves.index((t, r))
        wide = pad.shape[0] > frames + 2
        base = 0
        if wide:
            base = shift if t == 0 else 2 - shift
        if t == 0:
            src, dst = pl.ds(0, frames), pl.ds(base + 1, frames)
        elif t > 0:
            src, dst = pl.ds(frames - 1, 1), pl.ds(base, 1)
        else:
            src, dst = pl.ds(0, 1), pl.ds(base + frames + 1, 1)
        return pltpu.make_async_remote_copy(
            src_ref=source.at[src], dst_ref=pad.at[dst, 1 - r],
            send_sem=halo_send.at[slot], recv_sem=halo_recv.at[slot],
            device_id=device(tm=me["tm"] + t, rows=me["rows"] + r), device_id_type=MESH,
        )

    def halo_start(which, pad, source):
        for t, r in sorted(moves, key=lambda move: move[0] != 0):
            @pl.when(inside(t, r))
            def _():
                halo_copy(which, pad, source, t, r).start()

    def halo_wait(which, pad, source, level):
        for t, r in moves:
            if (t == 0) != level:
                continue

            @pl.when(inside(t, r))
            def _():
                halo_copy(which, pad, source, t, r).wait_send()

            @pl.when(inside(-t, -r))
            def _():
                halo_copy(which, pad, source, t, r).wait_recv()

    column = lax.rem(lax.broadcasted_iota(jnp.int32, (count, chans), 0), cols)

    def earlier(value):
        return jnp.where(column == 0, 0.0, pltpu.roll(value, 1, 0))

    def later(value):
        return jnp.where(column == cols - 1, 0.0, pltpu.roll(value, count - 1, 0))

    def send(src, dst, send_sem, recv_sem, target):
        return pltpu.make_async_remote_copy(
            src_ref=src, dst_ref=dst, send_sem=send_sem, recv_sem=recv_sem,
            device_id=target, device_id_type=MESH,
        )

    def pair_frames(pad, slot):
        block = pad.at[pl.ds(4 * core, 2)]
        return send(block, block, pair_send.at[slot], pair_recv.at[slot], partner)

    def conv(which, pad, source, transpose, ready=None):
        base = shift if pad.shape[0] > frames + 2 else 0

        def step(a):
            at = base + ((TAPS - 1 - a) if transpose else a)
            pieces = [
                pad[pl.ds(at, frames), (TAPS - 1 - b) if transpose else b].reshape(count, chans)
                for b in range(TAPS)
            ]
            left = jnp.concatenate(pieces, axis=1)
            for d in range(TAPS):
                taps = [w_ref[(a * TAPS + b) * TAPS + d] for b in range(TAPS)]
                if transpose:
                    part = lax.dot_general(
                        left, jnp.concatenate(taps, axis=1), (((1,), (1,)), ((), ())),
                        preferred_element_type=jnp.float32,
                    )
                else:
                    part = jnp.dot(
                        left, jnp.concatenate(taps, axis=0), preferred_element_type=jnp.float32
                    )
                acc[d] = part if a == 1 else acc[d] + part

        halo_wait(which, pad, source, True)
        step(1)
        halo_wait(which, pad, source, False)
        if ready is not None:
            ready()
        step(0)
        step(2)
        if transpose:
            return later(acc[0]) + acc[1] + earlier(acc[2])
        return earlier(acc[0]) + acc[1] + later(acc[2])

    def split_pair(value, cat, stage, slot):
        value = value.astype(jnp.float32)
        three = [later(value), value, earlier(value)]
        low = jnp.concatenate([v[:, :LANES] for v in three], axis=1)
        high = jnp.concatenate([v[:, LANES:] for v in three], axis=1)
        first = core == 0
        cat[core] = jnp.where(first, low, high).astype(jnp.bfloat16)
        stage[...] = jnp.where(first, high, low).astype(jnp.bfloat16)
        copy = send(stage, cat.at[core], pair_send.at[slot], pair_recv.at[slot], partner)
        copy.start()
        return copy

    halo_start(0, clip_pad, clips_ref)
    clip_copy.wait()
    weight_copy.wait()
    bias_copy.wait()
    head_copy.wait()
    pair_clips, pair_grads = pair_frames(clip_pad, 0), pair_frames(grad_pad, 1)
    pre = conv(0, clip_pad, clips_ref, False, pair_clips.start) + bias_ref[...]
    sig = jax.nn.sigmoid(pre)
    slope = sig * (1.0 + pre * (1.0 - sig))
    slope_ref[...] = slope
    curve_ref[...] = sig * (1.0 - sig) * (2.0 + pre * (1.0 - 2.0 * sig))
    score = (head_ref[...] * slope).astype(jnp.bfloat16)
    score_pad[pl.ds(1, frames), 1] = score.reshape(frames, cols, chans)
    score_own = score_pad.at[pl.ds(1, frames), 1]
    halo_start(1, score_pad, score_own)
    pair_s = split_pair(score, cat_s, stage_s, 2)

    input_grad = conv(1, score_pad, score_own, True).astype(jnp.bfloat16)
    grad_pad[pl.ds(shift + 1, frames), 1] = input_grad.reshape(frames, cols, chans)
    grad_own = grad_pad.at[pl.ds(shift + 1, frames), 1]
    halo_start(2, grad_pad, grad_own)

    back = penalty_weight * conv(2, grad_pad, grad_own, False, pair_grads.start)
    pre_grad = back * head_ref[...] * curve_ref[...]
    pair_p = split_pair(pre_grad.astype(jnp.bfloat16), cat_p, stage_p, 3)

    small_mine[...] = jnp.zeros_like(small_mine)
    for k, value in enumerate((pre_grad, back * slope_ref[...])):
        whole = jnp.sum(value, axis=0, keepdims=True)
        small_mine[pl.ds(2 * k, 1)] = whole[:, :LANES]
        small_mine[pl.ds(2 * k + 1, 1)] = whole[:, LANES:]
    small_targets = [
        [partner],
        [chip(x=other) for other in ring_peers("x", RING)],
        [chip(y=other) for other in ring_peers("y", RING)],
        [chip(z=other) for other in ring_peers("z", DEEP)],
    ]
    smalls = []

    def small_start(level):
        at = sum(len(group) for group in small_targets[:level])
        copies = []
        for k, target in enumerate(small_targets[level]):
            copy = send(
                small_mine.at[pl.ds(level * SUB, SUB)], small_land.at[pl.ds((at + k) * SUB, SUB)],
                small_send.at[0], small_recv.at[level], target,
            )
            copy.start()
            copies.append(at + k)
        smalls.append(copies)

    def small_end(level):
        value = small_mine[pl.ds(level * SUB, SUB)]
        slots = smalls[level]
        lands = small_land.at[pl.ds(slots[0] * SUB, len(slots) * SUB)]
        send(lands, lands, small_send.at[0], small_recv.at[level], partner).wait_recv()
        for slot in slots:
            value = value + small_land[pl.ds(slot * SUB, SUB)]
        small_mine[pl.ds((level + 1) * SUB, SUB)] = value

    small_start(0)

    routes = []
    for p in range(PARTS):
        first, second = ("x", "y") if p < GROUPS else ("y", "x")
        m, n = here[first], here[second]
        if p % 2 == 0:
            near, bit1, far, bit2 = flip(m), lax.rem((m + 1) // 2, 2), mirror(m), m // 2
        else:
            near, bit1, far, bit2 = mirror(m), m // 2, flip(m), lax.rem(m, 2)
        eight = 8 * bit1
        four = eight + 4 * bit2
        routes.append(dict(
            near=chip(**{first: near}), far=chip(**{first: far}),
            eight=eight, other8=8 - eight, four=four, other4=2 * eight + 4 - four,
            unit=four + n, second=second,
        ))

    def encode(p, base, units, code, at):
        def peak(k, top):
            for t in range(SHARE):
                top = jnp.maximum(top, jnp.abs(total[p, base + k, t]))
            return top

        zero = jnp.zeros((SUB, LANES), jnp.float32)
        top = peak(0, zero) if units == 1 else lax.fori_loop(0, units, peak, zero)
        top = (top * 1.01 + 1e-30).astype(jnp.bfloat16)
        rate = SPAN / top.astype(jnp.float32)
        code[(*at, units * SHARE)] = top

        def fill(k, carry):
            code[(*at, pl.ds(k * SHARE, SHARE))] = jnp.exp2(
                total[p, base + k] * rate[None]
            ).astype(jnp.bfloat16)
            return carry

        if units == 1:
            fill(0, 0)
        else:
            lax.fori_loop(0, units, fill, 0)

    def absorb(p, base, units, lands):
        scales = [
            land[(*at, units * SHARE)].astype(jnp.float32) * (1.0 / (SPAN * math.log(2.0)))
            for land, at in lands
        ]

        def add(k, carry):
            value = total[p, base + k]
            for (land, at), scale in zip(lands, scales):
                block = land[(*at, pl.ds(k * SHARE, SHARE))].astype(jnp.float32)
                value = value + jnp.log(block) * scale[None]
            total[p, base + k] = value
            return carry

        if units == 1:
            add(0, 0)
        else:
            lax.fori_loop(0, units, add, 0)

    def copy1(p):
        return send(code1.at[p], land1.at[p], send1.at[0], recv1.at[p], routes[p]["near"])

    def copy2(p):
        return send(code2.at[p], land2.at[p], send2.at[0], recv2.at[p], routes[p]["far"])

    def copy3(p):
        second = routes[p]["second"]
        return [
            send(
                code3.at[p, k], land3.at[p, k], send3.at[0], recv3.at[p],
                chip(**{second: other}),
            )
            for k, other in enumerate(ring_peers(second, RING))
        ]

    def start1(p):
        encode(p, routes[p]["other8"], 8, code1, (p,))
        copy1(p).start()

    def start2(p):
        encode(p, routes[p]["other4"], 4, code2, (p,))
        copy2(p).start()

    def start3(p):
        second = routes[p]["second"]
        for k, (copy, other) in enumerate(zip(copy3(p), ring_peers(second, RING))):
            encode(p, routes[p]["four"] + other, 1, code3, (p, k))
            copy.start()

    def correlate(pad, cat, a, b):
        left = pad[a : a + 2 * frames, b].reshape(2 * count, chans)
        right = cat[...].reshape(2 * count, TAPS * LANES)
        return lax.dot_general(
            left, right, (((0,), (0,)), ((), ())), preferred_element_type=jnp.float32
        )

    def tiles(value, h, d):
        block = value[h * UNITS * SUB : (h + 1) * UNITS * SUB, d * LANES : (d + 1) * LANES]
        return block.reshape(UNITS, SUB, LANES)

    def place(a, b, d):
        tap = (a * TAPS + b) * TAPS + d
        return tap // SHARE, tap % SHARE

    for h in range(2):
        total[h * GROUPS + GROUPS - 1, :, SHARE - 1] = jnp.zeros((UNITS, SUB, LANES), jnp.float32)
    pair_s.wait()
    pair_grads.wait()
    for b in range(TAPS):
        first = penalty_weight * correlate(grad_pad, cat_s, 0, b)
        for d in range(TAPS):
            g, t = place(0, b, d)
            for h in range(2):
                total[h * GROUPS + g, :, t] = tiles(first, h, d)
    pair_clips.wait()
    pair_p.wait()
    begun = 0
    for a in range(TAPS):
        for b in range(TAPS):
            value = correlate(clip_pad, cat_p, a, b)
            if a > 0:
                value = value + penalty_weight * correlate(grad_pad, cat_s, a, b)
            for d in range(TAPS):
                g, t = place(a, b, d)
                for h in range(2):
                    p = h * GROUPS + g
                    block = tiles(value, h, d)
                    total[p, :, t] = block + total[p, :, t] if a == 0 else block
            done = (a * TAPS + b + 1) * TAPS
            while begun < GROUPS and done >= min((begun + 1) * SHARE, TAPS**3):
                for h in range(2):
                    start1(h * GROUPS + begun)
                begun += 1

    small_end(0)
    small_start(1)
    order = [h * GROUPS + g for g in range(GROUPS) for h in range(2)]
    for p in order:
        copy1(p).wait_recv()
        absorb(p, routes[p]["eight"], 8, [(land1, (p,))])
        start2(p)
    small_end(1)
    small_start(2)
    for p in order:
        copy2(p).wait_recv()
        absorb(p, routes[p]["four"], 4, [(land2, (p,))])
        start3(p)
    small_end(2)
    small_start(3)

    z = here["z"]

    def copy4(p):
        return send(code4.at[p], land4.at[z], send4.at[0], recv4.at[0], chip(z=p))

    for p in order:
        send(land3.at[p], land3.at[p], send3.at[0], recv3.at[p], partner).wait_recv()
        absorb(p, routes[p]["unit"], 1, [(land3, (p, k)) for k in range(RING - 1)])

        @pl.when(z != p)
        def _():
            encode(p, routes[p]["unit"], 1, code4, (p,))
            copy4(p).start()

    unit = None
    for p in range(PARTS):
        term = jnp.where(z == p, routes[p]["unit"], 0)
        unit = term if unit is None else unit + term
    others = ring_peers("z", DEEP)
    seven = land4.at[pl.ds(0, DEEP - 1)]
    send(seven, seven, send4.at[0], recv4.at[0], partner).wait_recv()
    absorb(z, unit, 1, [(land4, (other,)) for other in others])
    encode(z, unit, 1, full, (z, core, unit))

    def zcopy(k, other):
        block = full.at[z, core, unit]
        return send(block, block, zsend.at[0], zrecv.at[z], chip(z=other))

    def zgot(p):
        block = full.at[p, core, routes[p]["unit"]]
        return send(block, block, zsend.at[0], zrecv.at[p], chip(z=p))

    for k, other in enumerate(others):
        zcopy(k, other).start()
    small_end(3)

    def qcopies(p):
        second = routes[p]["second"]
        block = full.at[p, core, routes[p]["unit"]]
        return [
            send(block, block, qsend.at[0], qrecv.at[p], chip(**{second: other}))
            for k, other in enumerate(ring_peers(second, RING))
        ]

    def far_copy(p):
        block = full.at[p, core, pl.ds(routes[p]["four"], 4)]
        return send(block, block, far_send.at[0], far_recv.at[p], routes[p]["far"])

    def near_copy(p):
        block = full.at[p, core, pl.ds(routes[p]["eight"], 8)]
        return send(block, block, near_send.at[0], near_recv.at[p], routes[p]["near"])

    def core_copy(p, second):
        base = routes[p]["other8"] if second else routes[p]["eight"]
        block = full.at[p, core, pl.ds(base, 8)]
        slot = 2 * p + second
        return send(block, block, core_send.at[0], core_recv.at[slot], partner)

    for p in order:
        @pl.when(z != p)
        def _():
            zgot(p).wait_recv()

        for copy in qcopies(p):
            copy.start()
    for p in order:
        three = full.at[p, core, pl.ds(0, RING - 1)]
        send(three, three, qsend.at[0], qrecv.at[p], partner).wait_recv()
        far_copy(p).start()
    def reveal(p, c, base):
        h, g = p // GROUPS, p % GROUPS
        taps = min(SHARE, TAPS**3 - g * SHARE)
        lane = pl.ds(pl.multiple_of(c * LANES, LANES), LANES)

        def one(k, carry):
            scale = full[p, c, base + k, SHARE].astype(jnp.float32) * (1.0 / (SPAN * math.log(2.0)))
            block = full[p, c, base + k, pl.ds(0, taps)].astype(jnp.float32)
            out_ref[pl.ds(g * SHARE, taps), h * UNITS + base + k, :, lane] = (
                jnp.log(block) * scale[None]
            )
            return carry

        lax.fori_loop(0, 8, one, 0)

    for k, ref in enumerate((bias_out, head_out)):
        at = (len(small_targets)) * SUB + 2 * k
        ref[:, pl.ds(0, LANES)] = small_mine[pl.ds(at, 1)]
        ref[:, pl.ds(LANES, LANES)] = small_mine[pl.ds(at + 1, 1)]
    for p in order:
        far_copy(p).wait_recv()
        near_copy(p).start()
        core_copy(p, 0).start()
    for p in order:
        reveal(p, core, routes[p]["eight"])
        near_copy(p).wait_recv()
        core_copy(p, 1).start()
    for p in order:
        reveal(p, core, routes[p]["other8"])
        core_copy(p, 0).wait_recv()
        reveal(p, 1 - core, routes[p]["eight"])
    for p in order:
        core_copy(p, 1).wait_recv()
        reveal(p, 1 - core, routes[p]["other8"])
    for block, sem in (
        (small_land, small_send), (code1, send1), (code2, send2), (code3, send3),
        (code4.at[pl.ds(0, DEEP - 1)], send4), (full.at[0, 0, pl.ds(0, DEEP - 1)], zsend),
        (full.at[pl.ds(0, 3), 0, pl.ds(0, 8)], qsend), (full.at[0], far_send),
        (full.at[pl.ds(0, 2)], near_send), (full.at[pl.ds(0, 4)], core_send),
    ):
        send(block, block, sem.at[0], sem.at[0], partner).wait_send()


def store_kernel(grad_ref, bias_ref, head_ref, grad_out, bias_out, head_out, sem):
    step = TAPS
    copies = [
        pltpu.make_async_copy(
            grad_ref.at[pl.ds(k * step, step)], grad_out.at[pl.ds(k * step, step)], sem.at[k]
        )
        for k in range(TAPS**3 // step)
    ]
    copies.append(pltpu.make_async_copy(bias_ref, bias_out, sem.at[TAPS**2]))
    copies.append(pltpu.make_async_copy(head_ref, head_out, sem.at[TAPS**2 + 1]))
    for copy in copies:
        copy.start()
    for copy in copies:
        copy.wait()


def per_device(sizes, clips, weight, bias, head):
    _, frames, _, cols, chans = clips.shape
    count = frames * cols
    dp, tm, rows = sizes
    assert (rows, dp * 2, tm // 4, chans) == (RING, RING, DEEP, 2 * LANES)
    dma = pltpu.SemaphoreType.DMA
    vmem = pl.BlockSpec(memory_space=pltpu.VMEM)
    hbm = pl.BlockSpec(memory_space=pltpu.HBM)
    row = jax.ShapeDtypeStruct((1, chans), jnp.float32)
    field = pltpu.VMEM((count, chans), jnp.float32)

    def pad(n):
        return pltpu.VMEM((n, 3, cols, chans), jnp.bfloat16)

    def coded(*lead, units):
        return pltpu.VMEM((*lead, units * SHARE + 1, SUB, LANES), jnp.bfloat16)

    cat = pltpu.VMEM((CORES, count, TAPS * LANES), jnp.bfloat16)
    stage = pltpu.VMEM((count, TAPS * LANES), jnp.bfloat16)
    smalls = 1 + 2 * (RING - 1) + DEEP - 1
    both = lambda n: [dma((n,)), dma((n,))]
    one = lambda n: [dma((1,)), dma((n,))]
    grad_weight, grad_bias, grad_head = pl.pallas_call(
        functools.partial(kernel, sizes),
        out_shape=(
            jax.ShapeDtypeStruct((TAPS**3, 2 * UNITS, SUB, chans), jnp.float32),
            row, row,
        ),
        in_specs=[hbm, hbm, hbm, hbm],
        out_specs=(vmem, vmem, vmem),
        scratch_shapes=[
            pltpu.VMEM((1, chans), jnp.float32), pltpu.VMEM((1, chans), jnp.float32),
            pltpu.VMEM((TAPS**3, chans, chans), jnp.bfloat16),
            pad(2 * frames + 2), pad(frames + 2), pad(2 * frames + 2),
            pltpu.VMEM((TAPS, count, chans), jnp.float32),
            field, field,
            cat, cat, stage, stage,
            pltpu.VMEM((PARTS, UNITS, SHARE, SUB, LANES), jnp.float32),
            coded(PARTS, units=8), coded(PARTS, units=8),
            coded(PARTS, units=4), coded(PARTS, units=4),
            coded(PARTS, RING - 1, units=1), coded(PARTS, RING - 1, units=1),
            coded(DEEP, units=1), coded(DEEP, units=1),
            coded(PARTS, CORES, UNITS, units=1),
            pltpu.VMEM((5 * SUB, LANES), jnp.float32),
            pltpu.VMEM((smalls * SUB, LANES), jnp.float32),
            dma((4,)), *both(24), *both(4), *one(PARTS), *one(PARTS), *one(PARTS), *one(1),
            *one(DEEP), *one(PARTS), *one(PARTS), *one(PARTS), *one(2 * PARTS), *one(4),
        ],
        compiler_params=pltpu.CompilerParams(
            collective_id=0, has_side_effects=True, vmem_limit_bytes=40 * 1024 * 1024
        ),
    )(
        *[
            pltpu.with_memory_space_constraint(value, pltpu.HBM)
            for value in (
                clips.reshape(frames, cols, chans), weight.reshape(TAPS**3, chans, chans),
                bias.reshape(1, chans), head.reshape(1, chans),
            )
        ]
    )
    grad_weight, grad_bias, grad_head = pl.pallas_call(
        store_kernel,
        out_shape=(
            jax.ShapeDtypeStruct((TAPS**3, 2 * UNITS, SUB, chans), jnp.float32), row, row,
        ),
        in_specs=[vmem, vmem, vmem],
        out_specs=(hbm, hbm, hbm),
        scratch_shapes=[dma((TAPS**2 + 2,))],
        compiler_params=pltpu.CompilerParams(vmem_limit_bytes=8 * 1024 * 1024),
    )(grad_weight, grad_bias, grad_head)
    grad_weight = grad_weight.reshape(TAPS, TAPS, TAPS, chans, chans)
    return grad_weight, grad_bias.reshape(chans), grad_head.reshape(chans)


def solution(mesh):
    sizes = tuple(mesh.shape[axis] for axis in ("dp", "tm", "rows"))
    return jax.shard_map(
        functools.partial(per_device, sizes),
        mesh=mesh,
        in_specs=(P("dp", "tm", "rows", None, None), P(), P(), P()),
        out_specs=(P(), P(), P()),
        check_vma=False,
    )
```

```python
import functools
import math

import jax
import jax.numpy as jnp
from jax import lax
from jax.experimental import pallas as pl
from jax.experimental.pallas import tpu as pltpu
from jax.sharding import PartitionSpec as P

penalty_weight = 0.01
MESH = pl.DeviceIdType.MESH
SUB = 8
LANES = 128
TAPS = 3
SPAN = 120.0
RING = 4
DEEP = 8
CORES = 2
GROUPS = 4
SHARE = 7
UNITS = 16
PARTS = 2 * GROUPS


def flip(m):
    return m + 1 - 2 * lax.rem(m, 2)


def mirror(m):
    return RING - 1 - m


def kernel(
    sizes, clips_ref, weight_ref, bias_hbm, head_hbm,
    out_ref, bias_out, head_out,
    bias_ref, head_ref, w_ref, clips_vm, clip_pad, score_pad, grad_pad, acc, slope_ref, curve_ref,
    cat_s, cat_p, stage_s, stage_p, raw_p, edge_out, edge_in, last_out, last_in, total,
    code1, land1, code2, land2, code3, land3, code4, land4, full, small_mine, small_land,
    local_sem, turn_send, turn_recv, halo_send, halo_recv, last_send, last_recv,
    pair_send, pair_recv, send1, recv1, send2, recv2,
    send3, recv3, send4, recv4, zsend, zrecv, qsend, qrecv, near_send, near_recv,
    far_send, far_recv, core_send, core_recv, small_send, small_recv,
):
    dp, tm, rows = sizes
    frames, wide, chans = clips_ref.shape
    cols = wide // RING
    lines = frames * RING
    count = lines * cols
    half = count // 2
    me = {"dp": lax.axis_index("dp"), "tm": lax.axis_index("tm"), "rows": lax.axis_index("rows")}
    core = lax.rem(me["tm"], CORES)
    here = {
        "x": me["rows"],
        "y": 2 * me["dp"] + lax.rem(me["tm"] // 2, 2),
        "z": me["tm"] // 4,
        "c": core,
    }

    def device(**moved):
        place = dict(me, **moved)
        return (place["dp"], place["tm"], place["rows"])

    def chip(**moved):
        place = dict(here, **moved)
        return (
            place["y"] // 2,
            place["z"] * 4 + lax.rem(place["y"], 2) * 2 + place["c"],
            place["x"],
        )

    partner = chip(c=1 - core)

    def ring_peers(axis, size):
        return [lax.rem(here[axis] + step, size) for step in range(1, size)]

    weight_copy = pltpu.make_async_copy(weight_ref, w_ref, local_sem.at[0])
    weight_copy.start()
    shift = 2 * core
    clip_copy = pltpu.make_async_copy(clips_ref, clips_vm, local_sem.at[1])
    clip_copy.start()
    bias_copy = pltpu.make_async_copy(bias_hbm, bias_ref, local_sem.at[2])
    head_copy = pltpu.make_async_copy(head_hbm, head_ref, local_sem.at[3])
    bias_copy.start()
    head_copy.start()
    for pad, base in ((clip_pad, shift), (score_pad, 0), (grad_pad, shift)):
        pad[:, 0] = jnp.zeros((pad.shape[0], cols, chans), pad.dtype)
        pad[:, RING + 1] = jnp.zeros((pad.shape[0], cols, chans), pad.dtype)
        for at in (base, base + frames + 1):
            pad[at, pl.ds(1, RING)] = jnp.zeros((RING, cols, chans), pad.dtype)
    edge_in[...] = jnp.zeros_like(edge_in)
    last_in[...] = jnp.zeros_like(last_in)

    moves = [(t, r) for t in (-1, 0, 1) for r in (-1, 0, 1) if (t, r) != (0, 0)]

    def inside(t, r):
        ok = None
        for axis, step, size in (("tm", t, tm), ("rows", r, rows)):
            if step:
                cond = me[axis] > 0 if step < 0 else me[axis] < size - 1
                ok = cond if ok is None else jnp.logical_and(ok, cond)
        return ok

    barrier = pltpu.get_barrier_semaphore()
    friends = [partner]
    friends += [chip(x=other) for other in ring_peers("x", RING)]
    friends += [chip(y=other) for other in ring_peers("y", RING)]
    friends += [chip(z=other) for other in ring_peers("z", DEEP)]
    for friend in friends:
        pl.semaphore_signal(barrier, inc=1, device_id=friend, device_id_type=MESH)
    expected = len(friends)
    for t in (-1, 1):
        expected = expected + RING * inside(t, 0).astype(jnp.int32)

        @pl.when(inside(t, 0))
        def _():
            for row in range(RING):
                pl.semaphore_signal(
                    barrier, inc=1, device_id=device(tm=me["tm"] + t, rows=row),
                    device_id_type=MESH,
                )
    pl.semaphore_wait(barrier, expected)

    def send(src, dst, send_sem, recv_sem, target):
        return pltpu.make_async_remote_copy(
            src_ref=src, dst_ref=dst, send_sem=send_sem, recv_sem=recv_sem,
            device_id=target, device_id_type=MESH,
        )

    def turn_copy(t, step):
        other = lax.rem(me["rows"] + step, RING)
        part = pl.ds(pl.multiple_of(other * cols, cols), cols)
        base = shift if t == 0 else 2 - shift
        src = {0: pl.ds(0, frames), 1: pl.ds(frames - 1, 1), -1: pl.ds(0, 1)}[t]
        dst = {0: pl.ds(base + 1, frames), 1: pl.ds(base, 1), -1: pl.ds(base + frames + 1, 1)}[t]
        return send(
            clips_vm.at[src, part], clip_pad.at[dst, 1 + me["rows"]],
            turn_send.at[1 + t], turn_recv.at[1 + t],
            device(tm=me["tm"] + t, rows=other),
        )

    def turn_start():
        for step in range(1, RING):
            turn_copy(0, step).start()
        for t in (-1, 1):
            @pl.when(inside(t, 0))
            def _():
                for step in range(RING):
                    turn_copy(t, step).start()

    def turn_wait(level):
        if level:
            block = clip_pad.at[pl.ds(shift + 1, frames), pl.ds(1, RING - 1)]
            copy = send(block, block, turn_send.at[1], turn_recv.at[1], partner)
            copy.wait_recv()
            copy.wait_send()
            return
        for t in (-1, 1):
            block = clip_pad.at[shift, pl.ds(1, RING)]
            copy = send(block, block, turn_send.at[1 + t], turn_recv.at[1 + t], partner)

            @pl.when(inside(t, 0))
            def _():
                copy.wait_send()

            @pl.when(inside(-t, 0))
            def _():
                copy.wait_recv()

    def halo_copy(which, pad, t, r):
        slot = which * len(moves) + moves.index((t, r))
        target = device(tm=me["tm"] + t, rows=me["rows"] + r)
        sems = halo_send.at[slot], halo_recv.at[slot]
        if r != 0:
            side = 0 if r > 0 else 1
            return send(edge_out.at[which, side], edge_in.at[which, side, 1 - t], *sems, target)
        pair = pad.shape[0] > frames + 2
        mine, base = (shift, 2 - shift) if pair else (0, 0)
        src = mine + frames if t > 0 else mine + 1
        dst = base if t > 0 else base + frames + 1
        return send(
            pad.at[src, pl.ds(1, RING)], pad.at[dst, pl.ds(1, RING)], *sems, target
        )

    def edge_rows(value):
        block = value.reshape(lines, cols, value.shape[-1])
        return block[:, cols - 1], block[:, 0]

    def halo_start(which, pad, value, skip=False):
        for side, rows_out in enumerate(edge_rows(value)):
            edge_out[which, side] = rows_out
        for t, r in sorted(moves, key=lambda move: move[1] != 0):
            if skip and r == 0:
                continue

            @pl.when(inside(t, r))
            def _():
                halo_copy(which, pad, t, r).start()

    def halo_wait(which, pad, skip=False):
        for t, r in moves:
            if skip and r == 0:
                continue

            @pl.when(inside(t, r))
            def _():
                halo_copy(which, pad, t, r).wait_send()

            @pl.when(inside(-t, -r))
            def _():
                halo_copy(which, pad, t, r).wait_recv()

    def columns(value):
        return lax.rem(lax.broadcasted_iota(jnp.int32, value.shape, 0), cols)

    def spread(edge):
        return jnp.broadcast_to(edge[:, None, :], (lines, cols, edge.shape[-1])).reshape(count, -1)

    def earlier(value, edge):
        return jnp.where(columns(value) == 0, spread(edge), pltpu.roll(value, 1, 0))

    def later(value, edge):
        return jnp.where(columns(value) == cols - 1, spread(edge), pltpu.roll(value, count - 1, 0))

    def pair_frames(pad, slot):
        block = pad.at[pl.ds(4 * core, 2), pl.ds(1, RING)]
        return send(block, block, pair_send.at[slot], pair_recv.at[slot], partner)

    def edge_left(which):
        line = lax.broadcasted_iota(jnp.int32, (lines, chans), 0)
        row = lax.rem(line, RING)

        def piece(side, s, q):
            below, level, above = (edge_in[which, side, k] for k in range(3))
            if s == 1:
                value = level
            else:
                value = pltpu.roll(level, RING, 0)
                if s == 0:
                    value = jnp.where(line < RING, pltpu.roll(below, RING, 0), value)
                else:
                    value = jnp.where(line < RING, value, pltpu.roll(above, RING, 0))
            if q == 0:
                value = jnp.where(row == 0, 0.0, pltpu.roll(value, 1, 0))
            elif q == 2:
                value = jnp.where(row == RING - 1, 0.0, pltpu.roll(value, lines - 1, 0))
            return value

        return [
            jnp.concatenate([
                jnp.concatenate([piece(side, s, q) for q in range(TAPS)], axis=1)
                for side in range(2)
            ], axis=0).astype(jnp.bfloat16)
            for s in range(TAPS)
        ]

    def conv(which, pad, transpose, wait, ready):
        base = shift if pad.shape[0] > frames + 2 else 0

        def left(at, size):
            return jnp.concatenate([
                pad[pl.ds(base + at, size), pl.ds(q, RING)].reshape(size * half, chans)
                for q in range(TAPS)
            ], axis=1)

        def product(value, s, d):
            a = TAPS - 1 - s if transpose else s
            taps = [
                w_ref[(a * TAPS + (TAPS - 1 - q if transpose else q)) * TAPS + d]
                for q in range(TAPS)
            ]
            if transpose:
                return lax.dot_general(
                    value, jnp.concatenate(taps, axis=1), (((1,), (1,)), ((), ())),
                    preferred_element_type=jnp.float32,
                )
            return jnp.dot(
                value, jnp.concatenate(taps, axis=0), preferred_element_type=jnp.float32
            )

        own = left(1, frames)
        for d in range(TAPS):
            level = product(own, 1, d)
            acc[d, pl.ds(0, half)] = level[:half] + product(own[half:], 2, d)
            acc[d, pl.ds(half, half)] = level[half:] + product(own[:half], 0, d)
        wait()
        ready()
        edges = edge_left(which)
        below = jnp.concatenate([left(0, 1), edges[0]], axis=0)
        above = jnp.concatenate([left(frames + 1, 1), edges[2]], axis=0)
        sums, sides = [], []
        for d in range(TAPS):
            low, high = product(below, 0, d), product(above, 2, d)
            sums.append(jnp.concatenate([
                acc[d, pl.ds(0, half)] + low[:half], acc[d, pl.ds(half, half)] + high[:half]
            ], axis=0))
            sides.append(
                None if d == 1 else low[half:] + high[half:] + product(edges[1], 1, d)
            )
        d0, d2 = (2, 0) if transpose else (0, 2)
        return (
            earlier(sums[d0], sides[d0][:lines]) + sums[1] + later(sums[d2], sides[d2][lines:])
        )


    def lane_half(value, mine=True):
        low, high = value[:, :LANES], value[:, LANES:]
        return jnp.where(core == 0, low, high) if mine else jnp.where(core == 0, high, low)

    def three(value, before, after):
        return jnp.concatenate(
            [later(value, after), value, earlier(value, before)], axis=1
        ).astype(jnp.bfloat16)

    clip_copy.wait()
    turn_start()
    mine = pl.ds(pl.multiple_of(me["rows"] * cols, cols), cols)
    clip_pad[pl.ds(shift + 1, frames), 1 + me["rows"]] = clips_vm[:, mine]
    weight_copy.wait()
    bias_copy.wait()
    head_copy.wait()
    pair_clips, pair_grads = pair_frames(clip_pad, 0), pair_frames(grad_pad, 1)
    turn_wait(True)
    clips = clip_pad[pl.ds(shift + 1, frames), pl.ds(1, RING)].reshape(count, chans)
    halo_start(0, clip_pad, clips.astype(jnp.float32), True)

    def wait_clips():
        turn_wait(False)
        halo_wait(0, clip_pad, True)

    pre = conv(0, clip_pad, False, wait_clips, pair_clips.start) + bias_ref[...]
    sig = jax.nn.sigmoid(pre)
    slope = sig * (1.0 + pre * (1.0 - sig))
    slope_ref[...] = slope
    curve_ref[...] = sig * (1.0 - sig) * (2.0 + pre * (1.0 - 2.0 * sig))
    score = (head_ref[...] * slope).astype(jnp.bfloat16)
    score_pad[pl.ds(1, frames), pl.ds(1, RING)] = score.reshape(frames, RING, cols, chans)
    halo_start(1, score_pad, score.astype(jnp.float32))

    input_grad = conv(
        1, score_pad, True, lambda: halo_wait(1, score_pad), lambda: None
    ).astype(jnp.bfloat16)
    grad_pad[pl.ds(shift + 1, frames), pl.ds(1, RING)] = input_grad.reshape(
        frames, RING, cols, chans
    )
    halo_start(2, grad_pad, input_grad.astype(jnp.float32))

    value = score_pad[pl.ds(1, frames), pl.ds(1, RING)].reshape(count, chans).astype(jnp.float32)
    for mine, ref in ((True, cat_s.at[core]), (False, stage_s)):
        ref[...] = three(
            lane_half(value, mine),
            lane_half(edge_in[1, 0, 1], mine), lane_half(edge_in[1, 1, 1], mine),
        )
    pair_s = send(stage_s, cat_s.at[core], pair_send.at[2], pair_recv.at[2], partner)
    pair_s.start()

    back = penalty_weight * conv(
        2, grad_pad, False, lambda: halo_wait(2, grad_pad), pair_grads.start
    )
    pre_grad = back * head_ref[...] * curve_ref[...]
    value = pre_grad.astype(jnp.bfloat16).astype(jnp.float32)
    for side, rows_out in enumerate(edge_rows(value)):
        last_out[side] = rows_out
    stage_p[...] = lane_half(value, False).astype(jnp.bfloat16)
    pair_p = send(stage_p, raw_p.at[1], pair_send.at[3], pair_recv.at[3], partner)
    pair_p.start()
    raw_p[0] = lane_half(value).astype(jnp.bfloat16)

    def last_copy(r, c):
        side = 0 if r > 0 else 1
        slot = 2 * side + c
        other = core if c == 0 else 1 - core
        return send(
            last_out.at[side], last_in.at[side, c], last_send.at[slot], last_recv.at[slot],
            device(tm=me["tm"] - core + other, rows=me["rows"] + r),
        )

    for r in (-1, 1):
        @pl.when(inside(0, r))
        def _():
            for c in range(CORES):
                last_copy(r, c).start()

    small_mine[...] = jnp.zeros_like(small_mine)
    for k, value in enumerate((pre_grad, back * slope_ref[...])):
        whole = jnp.sum(value, axis=0, keepdims=True)
        small_mine[pl.ds(2 * k, 1)] = whole[:, :LANES]
        small_mine[pl.ds(2 * k + 1, 1)] = whole[:, LANES:]
    small_targets = [
        [partner],
        [chip(x=other) for other in ring_peers("x", RING)],
        [chip(y=other) for other in ring_peers("y", RING)],
        [chip(z=other) for other in ring_peers("z", DEEP)],
    ]
    smalls = []

    def small_start(level):
        at = sum(len(group) for group in small_targets[:level])
        copies = []
        for k, target in enumerate(small_targets[level]):
            copy = send(
                small_mine.at[pl.ds(level * SUB, SUB)], small_land.at[pl.ds((at + k) * SUB, SUB)],
                small_send.at[0], small_recv.at[level], target,
            )
            copy.start()
            copies.append(at + k)
        smalls.append(copies)

    def small_end(level):
        value = small_mine[pl.ds(level * SUB, SUB)]
        slots = smalls[level]
        lands = small_land.at[pl.ds(slots[0] * SUB, len(slots) * SUB)]
        send(lands, lands, small_send.at[0], small_recv.at[level], partner).wait_recv()
        for slot in slots:
            value = value + small_land[pl.ds(slot * SUB, SUB)]
        small_mine[pl.ds((level + 1) * SUB, SUB)] = value

    small_start(0)

    routes = []
    for p in range(PARTS):
        first, second = ("x", "y") if p < GROUPS else ("y", "x")
        m, n = here[first], here[second]
        if p % 2 == 0:
            near, bit1, far, bit2 = flip(m), lax.rem((m + 1) // 2, 2), mirror(m), m // 2
        else:
            near, bit1, far, bit2 = mirror(m), m // 2, flip(m), lax.rem(m, 2)
        eight = 8 * bit1
        four = eight + 4 * bit2
        routes.append(dict(
            near=chip(**{first: near}), far=chip(**{first: far}),
            eight=eight, other8=8 - eight, four=four, other4=2 * eight + 4 - four,
            unit=four + n, second=second,
        ))

    def encode(p, base, units, code, at):
        def peak(k, top):
            for t in range(SHARE):
                top = jnp.maximum(top, jnp.abs(total[p, base + k, t]))
            return top

        zero = jnp.zeros((SUB, LANES), jnp.float32)
        top = peak(0, zero) if units == 1 else lax.fori_loop(0, units, peak, zero)
        top = (top * 1.01 + 1e-30).astype(jnp.bfloat16)
        rate = SPAN / top.astype(jnp.float32)
        code[(*at, units * SHARE)] = top

        def fill(k, carry):
            code[(*at, pl.ds(k * SHARE, SHARE))] = jnp.exp2(
                total[p, base + k] * rate[None]
            ).astype(jnp.bfloat16)
            return carry

        if units == 1:
            fill(0, 0)
        else:
            lax.fori_loop(0, units, fill, 0)

    def absorb(p, base, units, lands):
        scales = [
            land[(*at, units * SHARE)].astype(jnp.float32) * (1.0 / (SPAN * math.log(2.0)))
            for land, at in lands
        ]

        def add(k, carry):
            value = total[p, base + k]
            for (land, at), scale in zip(lands, scales):
                block = land[(*at, pl.ds(k * SHARE, SHARE))].astype(jnp.float32)
                value = value + jnp.log(block) * scale[None]
            total[p, base + k] = value
            return carry

        if units == 1:
            add(0, 0)
        else:
            lax.fori_loop(0, units, add, 0)

    def copy1(p):
        return send(code1.at[p], land1.at[p], send1.at[0], recv1.at[p], routes[p]["near"])

    def copy2(p):
        return send(code2.at[p], land2.at[p], send2.at[0], recv2.at[p], routes[p]["far"])

    def copy3(p):
        second = routes[p]["second"]
        return [
            send(
                code3.at[p, k], land3.at[p, k], send3.at[0], recv3.at[p],
                chip(**{second: other}),
            )
            for k, other in enumerate(ring_peers(second, RING))
        ]

    def start1(p):
        encode(p, routes[p]["other8"], 8, code1, (p,))
        copy1(p).start()

    def start2(p):
        encode(p, routes[p]["other4"], 4, code2, (p,))
        copy2(p).start()

    def start3(p):
        second = routes[p]["second"]
        for k, (copy, other) in enumerate(zip(copy3(p), ring_peers(second, RING))):
            encode(p, routes[p]["four"] + other, 1, code3, (p, k))
            copy.start()

    def correlate(pad, cat, a, b):
        left = pad[a : a + 2 * frames, b : b + RING].reshape(2 * count, chans)
        right = cat[...].reshape(2 * count, TAPS * LANES)
        return lax.dot_general(
            left, right, (((0,), (0,)), ((), ())), preferred_element_type=jnp.float32
        )

    def tiles(value, h, d):
        block = value[h * UNITS * SUB : (h + 1) * UNITS * SUB, d * LANES : (d + 1) * LANES]
        return block.reshape(UNITS, SUB, LANES)

    def place(a, b, d):
        tap = (a * TAPS + b) * TAPS + d
        return tap // SHARE, tap % SHARE

    for h in range(2):
        total[h * GROUPS + GROUPS - 1, :, SHARE - 1] = jnp.zeros((UNITS, SUB, LANES), jnp.float32)
    pair_s.wait()
    pair_grads.wait()
    for a in range(TAPS):
        for b in range(TAPS):
            value = penalty_weight * correlate(grad_pad, cat_s, a, b)
            for d in range(TAPS):
                g, t = place(a, b, d)
                for h in range(2):
                    total[h * GROUPS + g, :, t] = tiles(value, h, d)
    pair_clips.wait()
    pair_p.wait()
    for r in (-1, 1):
        for c in range(CORES):
            @pl.when(inside(0, r))
            def _():
                last_copy(r, c).wait_send()

            @pl.when(inside(0, -r))
            def _():
                last_copy(r, c).wait_recv()

    for c in range(CORES):
        ref = cat_p.at[core if c == 0 else 1 - core]
        ref[...] = three(
            raw_p[c].astype(jnp.float32), lane_half(last_in[0, c]), lane_half(last_in[1, c])
        )
    begun = 0
    for a in range(TAPS):
        for b in range(TAPS):
            value = correlate(clip_pad, cat_p, a, b)
            for d in range(TAPS):
                g, t = place(a, b, d)
                for h in range(2):
                    p = h * GROUPS + g
                    block = tiles(value, h, d)
                    total[p, :, t] = block + total[p, :, t]
            done = (a * TAPS + b + 1) * TAPS
            while begun < GROUPS and done >= min((begun + 1) * SHARE, TAPS**3):
                for h in range(2):
                    start1(h * GROUPS + begun)
                begun += 1

    small_end(0)
    small_start(1)
    order = [h * GROUPS + g for g in range(GROUPS) for h in range(2)]
    for p in order:
        copy1(p).wait_recv()
        absorb(p, routes[p]["eight"], 8, [(land1, (p,))])
        start2(p)
    small_end(1)
    small_start(2)
    for p in order:
        copy2(p).wait_recv()
        absorb(p, routes[p]["four"], 4, [(land2, (p,))])
        start3(p)
    small_end(2)
    small_start(3)

    z = here["z"]

    def copy4(p):
        return send(code4.at[p], land4.at[z], send4.at[0], recv4.at[0], chip(z=p))

    for p in order:
        send(land3.at[p], land3.at[p], send3.at[0], recv3.at[p], partner).wait_recv()
        absorb(p, routes[p]["unit"], 1, [(land3, (p, k)) for k in range(RING - 1)])

        @pl.when(z != p)
        def _():
            encode(p, routes[p]["unit"], 1, code4, (p,))
            copy4(p).start()

    unit = None
    for p in range(PARTS):
        term = jnp.where(z == p, routes[p]["unit"], 0)
        unit = term if unit is None else unit + term
    others = ring_peers("z", DEEP)
    seven = land4.at[pl.ds(0, DEEP - 1)]
    send(seven, seven, send4.at[0], recv4.at[0], partner).wait_recv()
    absorb(z, unit, 1, [(land4, (other,)) for other in others])
    encode(z, unit, 1, full, (z, core, unit))

    def zcopy(k, other):
        block = full.at[z, core, unit]
        return send(block, block, zsend.at[0], zrecv.at[z], chip(z=other))

    def zgot(p):
        block = full.at[p, core, routes[p]["unit"]]
        return send(block, block, zsend.at[0], zrecv.at[p], chip(z=p))

    for k, other in enumerate(others):
        zcopy(k, other).start()
    small_end(3)

    def qcopies(p):
        second = routes[p]["second"]
        block = full.at[p, core, routes[p]["unit"]]
        return [
            send(block, block, qsend.at[0], qrecv.at[p], chip(**{second: other}))
            for k, other in enumerate(ring_peers(second, RING))
        ]

    def far_copy(p):
        block = full.at[p, core, pl.ds(routes[p]["four"], 4)]
        return send(block, block, far_send.at[0], far_recv.at[p], routes[p]["far"])

    def near_copy(p):
        block = full.at[p, core, pl.ds(routes[p]["eight"], 8)]
        return send(block, block, near_send.at[0], near_recv.at[p], routes[p]["near"])

    def core_copy(p, second):
        base = routes[p]["other8"] if second else routes[p]["eight"]
        block = full.at[p, core, pl.ds(base, 8)]
        slot = 2 * p + second
        return send(block, block, core_send.at[0], core_recv.at[slot], partner)

    for p in order:
        @pl.when(z != p)
        def _():
            zgot(p).wait_recv()

        for copy in qcopies(p):
            copy.start()
    for p in order:
        three = full.at[p, core, pl.ds(0, RING - 1)]
        send(three, three, qsend.at[0], qrecv.at[p], partner).wait_recv()
        far_copy(p).start()
    def reveal(p, c, base):
        h, g = p // GROUPS, p % GROUPS
        taps = min(SHARE, TAPS**3 - g * SHARE)
        lane = pl.ds(pl.multiple_of(c * LANES, LANES), LANES)

        def one(k, carry):
            scale = full[p, c, base + k, SHARE].astype(jnp.float32) * (1.0 / (SPAN * math.log(2.0)))
            block = full[p, c, base + k, pl.ds(0, taps)].astype(jnp.float32)
            out_ref[pl.ds(g * SHARE, taps), h * UNITS + base + k, :, lane] = (
                jnp.log(block) * scale[None]
            )
            return carry

        lax.fori_loop(0, 8, one, 0)

    for k, ref in enumerate((bias_out, head_out)):
        at = (len(small_targets)) * SUB + 2 * k
        ref[:, pl.ds(0, LANES)] = small_mine[pl.ds(at, 1)]
        ref[:, pl.ds(LANES, LANES)] = small_mine[pl.ds(at + 1, 1)]
    for p in order:
        far_copy(p).wait_recv()
        near_copy(p).start()
        core_copy(p, 0).start()
    for p in order:
        reveal(p, core, routes[p]["eight"])
        near_copy(p).wait_recv()
        core_copy(p, 1).start()
    for p in order:
        reveal(p, core, routes[p]["other8"])
        core_copy(p, 0).wait_recv()
        reveal(p, 1 - core, routes[p]["eight"])
    for p in order:
        core_copy(p, 1).wait_recv()
        reveal(p, 1 - core, routes[p]["other8"])
    for block, sem in (
        (small_land, small_send), (code1, send1), (code2, send2), (code3, send3),
        (code4.at[pl.ds(0, DEEP - 1)], send4), (full.at[0, 0, pl.ds(0, DEEP - 1)], zsend),
        (full.at[pl.ds(0, 3), 0, pl.ds(0, 8)], qsend), (full.at[0], far_send),
        (full.at[pl.ds(0, 2)], near_send), (full.at[pl.ds(0, 4)], core_send),
    ):
        send(block, block, sem.at[0], sem.at[0], partner).wait_send()


def store_kernel(grad_ref, bias_ref, head_ref, grad_out, bias_out, head_out, sem):
    step = TAPS
    copies = [
        pltpu.make_async_copy(
            grad_ref.at[pl.ds(k * step, step)], grad_out.at[pl.ds(k * step, step)], sem.at[k]
        )
        for k in range(TAPS**3 // step)
    ]
    copies.append(pltpu.make_async_copy(bias_ref, bias_out, sem.at[TAPS**2]))
    copies.append(pltpu.make_async_copy(head_ref, head_out, sem.at[TAPS**2 + 1]))
    for copy in copies:
        copy.start()
    for copy in copies:
        copy.wait()


def per_device(sizes, clips, weight, bias, head):
    _, frames, _, cols, chans = clips.shape
    count = frames * cols
    lines = frames * RING
    dp, tm, rows = sizes
    assert (rows, dp * 2, tm // 4, chans) == (RING, RING, DEEP, 2 * LANES)
    dma = pltpu.SemaphoreType.DMA
    vmem = pl.BlockSpec(memory_space=pltpu.VMEM)
    hbm = pl.BlockSpec(memory_space=pltpu.HBM)
    row = jax.ShapeDtypeStruct((1, chans), jnp.float32)
    field = pltpu.VMEM((count, chans), jnp.float32)

    def pad(n):
        return pltpu.VMEM((n, RING + 2, cols // RING, chans), jnp.bfloat16)

    def coded(*lead, units):
        return pltpu.VMEM((*lead, units * SHARE + 1, SUB, LANES), jnp.bfloat16)

    cat = pltpu.VMEM((CORES, count, TAPS * LANES), jnp.bfloat16)
    stage = pltpu.VMEM((count, TAPS * LANES), jnp.bfloat16)
    smalls = 1 + 2 * (RING - 1) + DEEP - 1
    both = lambda n: [dma((n,)), dma((n,))]
    one = lambda n: [dma((1,)), dma((n,))]
    grad_weight, grad_bias, grad_head = pl.pallas_call(
        functools.partial(kernel, sizes),
        out_shape=(
            jax.ShapeDtypeStruct((TAPS**3, 2 * UNITS, SUB, chans), jnp.float32),
            row, row,
        ),
        in_specs=[hbm, hbm, hbm, hbm],
        out_specs=(vmem, vmem, vmem),
        scratch_shapes=[
            pltpu.VMEM((1, chans), jnp.float32), pltpu.VMEM((1, chans), jnp.float32),
            pltpu.VMEM((TAPS**3, chans, chans), jnp.bfloat16),
            pltpu.VMEM((frames, cols, chans), jnp.bfloat16),
            pad(2 * frames + 2), pad(frames + 2), pad(2 * frames + 2),
            pltpu.VMEM((TAPS, count, chans), jnp.float32),
            field, field,
            cat, cat, stage, pltpu.VMEM((count, LANES), jnp.bfloat16),
            pltpu.VMEM((CORES, count, LANES), jnp.bfloat16),
            pltpu.VMEM((TAPS, 2, lines, chans), jnp.float32),
            pltpu.VMEM((TAPS, 2, 3, lines, chans), jnp.float32),
            pltpu.VMEM((2, lines, chans), jnp.float32),
            pltpu.VMEM((2, CORES, lines, chans), jnp.float32),
            pltpu.VMEM((PARTS, UNITS, SHARE, SUB, LANES), jnp.float32),
            coded(PARTS, units=8), coded(PARTS, units=8),
            coded(PARTS, units=4), coded(PARTS, units=4),
            coded(PARTS, RING - 1, units=1), coded(PARTS, RING - 1, units=1),
            coded(DEEP, units=1), coded(DEEP, units=1),
            coded(PARTS, CORES, UNITS, units=1),
            pltpu.VMEM((5 * SUB, LANES), jnp.float32),
            pltpu.VMEM((smalls * SUB, LANES), jnp.float32),
            dma((4,)), *both(3), *both(24), *both(4), *both(4), *one(PARTS), *one(PARTS), *one(PARTS), *one(1),
            *one(DEEP), *one(PARTS), *one(PARTS), *one(PARTS), *one(2 * PARTS), *one(4),
        ],
        compiler_params=pltpu.CompilerParams(
            collective_id=0, has_side_effects=True, vmem_limit_bytes=40 * 1024 * 1024
        ),
    )(
        *[
            pltpu.with_memory_space_constraint(value, pltpu.HBM)
            for value in (
                clips.reshape(frames, cols, chans), weight.reshape(TAPS**3, chans, chans),
                bias.reshape(1, chans), head.reshape(1, chans),
            )
        ]
    )
    grad_weight, grad_bias, grad_head = pl.pallas_call(
        store_kernel,
        out_shape=(
            jax.ShapeDtypeStruct((TAPS**3, 2 * UNITS, SUB, chans), jnp.float32), row, row,
        ),
        in_specs=[vmem, vmem, vmem],
        out_specs=(hbm, hbm, hbm),
        scratch_shapes=[dma((TAPS**2 + 2,))],
        compiler_params=pltpu.CompilerParams(vmem_limit_bytes=8 * 1024 * 1024),
    )(grad_weight, grad_bias, grad_head)
    grad_weight = grad_weight.reshape(TAPS, TAPS, TAPS, chans, chans)
    return grad_weight, grad_bias.reshape(chans), grad_head.reshape(chans)


def solution(mesh):
    sizes = tuple(mesh.shape[axis] for axis in ("dp", "tm", "rows"))
    return jax.shard_map(
        functools.partial(per_device, sizes),
        mesh=mesh,
        in_specs=(P("dp", "tm", "rows", None, None), P(), P(), P()),
        out_specs=(P(), P(), P()),
        check_vma=False,
    )
```

```python
import functools
import math

import jax
import jax.numpy as jnp
from jax import lax
from jax.experimental import pallas as pl
from jax.experimental.pallas import tpu as pltpu
from jax.sharding import PartitionSpec as P

penalty_weight = 0.01
MESH = pl.DeviceIdType.MESH
SUB = 8
LANES = 128
TAPS = 3
SPAN = 120.0
RING = 4
DEEP = 8
CORES = 2
GROUPS = 4
SHARE = 7
UNITS = 16
UNROLL = 4
WAYS = 2
PARTS = 2 * GROUPS


def flip(m):
    return m + 1 - 2 * lax.rem(m, 2)


def mirror(m):
    return RING - 1 - m


def kernel(
    sizes, clips_ref, weight_ref, bias_hbm, head_hbm,
    out_ref, bias_out, head_out,
    bias_ref, head_ref, w_ref, clips_vm, clip_pad, score_pad, grad_pad, acc, slope_ref, curve_ref,
    cat_s, cat_p, stage_s, stage_p, raw_p, edge_out, edge_in, last_out, last_in, total,
    code1, land1, code2, land2, code3, land3, code4, land4, full, small_mine, small_land,
    local_sem, turn_send, turn_recv, halo_send, halo_recv, last_send, last_recv,
    pair_send, pair_recv, send1, recv1, send2, recv2,
    send3, recv3, send4, recv4, zsend, zrecv, qsend, qrecv, near_send, near_recv,
    far_send, far_recv, core_send, core_recv, small_send, small_recv,
):
    dp, tm, rows = sizes
    frames, wide, chans = clips_ref.shape
    cols = wide // RING
    lines = frames * RING
    count = lines * cols
    half = count // 2
    me = {"dp": lax.axis_index("dp"), "tm": lax.axis_index("tm"), "rows": lax.axis_index("rows")}
    core = lax.rem(me["tm"], CORES)
    here = {
        "x": me["rows"],
        "y": 2 * me["dp"] + lax.rem(me["tm"] // 2, 2),
        "z": me["tm"] // 4,
        "c": core,
    }

    def device(**moved):
        place = dict(me, **moved)
        return (place["dp"], place["tm"], place["rows"])

    def chip(**moved):
        place = dict(here, **moved)
        return (
            place["y"] // 2,
            place["z"] * 4 + lax.rem(place["y"], 2) * 2 + place["c"],
            place["x"],
        )

    partner = chip(c=1 - core)

    def ring_peers(axis, size):
        return [lax.rem(here[axis] + step, size) for step in range(1, size)]

    weight_copy = pltpu.make_async_copy(weight_ref, w_ref, local_sem.at[0])
    weight_copy.start()
    shift = 2 * core
    clip_copy = pltpu.make_async_copy(clips_ref, clips_vm, local_sem.at[1])
    clip_copy.start()
    bias_copy = pltpu.make_async_copy(bias_hbm, bias_ref, local_sem.at[2])
    head_copy = pltpu.make_async_copy(head_hbm, head_ref, local_sem.at[3])
    bias_copy.start()
    head_copy.start()
    for pad, base in ((clip_pad, shift), (score_pad, 0), (grad_pad, shift)):
        pad[:, 0] = jnp.zeros((pad.shape[0], cols, chans), pad.dtype)
        pad[:, RING + 1] = jnp.zeros((pad.shape[0], cols, chans), pad.dtype)
        for at in (base, base + frames + 1):
            pad[at, pl.ds(1, RING)] = jnp.zeros((RING, cols, chans), pad.dtype)
    edge_in[...] = jnp.zeros_like(edge_in)
    last_in[...] = jnp.zeros_like(last_in)

    moves = [(t, r) for t in (-1, 0, 1) for r in (-1, 0, 1) if (t, r) != (0, 0)]

    def inside(t, r):
        ok = None
        for axis, step, size in (("tm", t, tm), ("rows", r, rows)):
            if step:
                cond = me[axis] > 0 if step < 0 else me[axis] < size - 1
                ok = cond if ok is None else jnp.logical_and(ok, cond)
        return ok

    barrier = pltpu.get_barrier_semaphore()
    friends = [partner]
    friends += [chip(x=other) for other in ring_peers("x", RING)]
    friends += [chip(y=other) for other in ring_peers("y", RING)]
    friends += [chip(z=other) for other in ring_peers("z", DEEP)]
    for friend in friends:
        pl.semaphore_signal(barrier, inc=1, device_id=friend, device_id_type=MESH)
    expected = len(friends)
    for t in (-1, 1):
        expected = expected + RING * inside(t, 0).astype(jnp.int32)

        @pl.when(inside(t, 0))
        def _():
            for row in range(RING):
                pl.semaphore_signal(
                    barrier, inc=1, device_id=device(tm=me["tm"] + t, rows=row),
                    device_id_type=MESH,
                )
    pl.semaphore_wait(barrier, expected)

    def send(src, dst, send_sem, recv_sem, target):
        return pltpu.make_async_remote_copy(
            src_ref=src, dst_ref=dst, send_sem=send_sem, recv_sem=recv_sem,
            device_id=target, device_id_type=MESH,
        )

    def turn_copy(t, step):
        other = lax.rem(me["rows"] + step, RING)
        part = pl.ds(pl.multiple_of(other * cols, cols), cols)
        base = shift if t == 0 else 2 - shift
        src = {0: pl.ds(0, frames), 1: pl.ds(frames - 1, 1), -1: pl.ds(0, 1)}[t]
        dst = {0: pl.ds(base + 1, frames), 1: pl.ds(base, 1), -1: pl.ds(base + frames + 1, 1)}[t]
        return send(
            clips_vm.at[src, part], clip_pad.at[dst, 1 + me["rows"]],
            turn_send.at[1 + t], turn_recv.at[1 + t],
            device(tm=me["tm"] + t, rows=other),
        )

    def turn_start():
        for step in range(1, RING):
            turn_copy(0, step).start()
        for t in (-1, 1):
            @pl.when(inside(t, 0))
            def _():
                for step in range(RING):
                    turn_copy(t, step).start()

    def turn_wait(level):
        if level:
            block = clip_pad.at[pl.ds(shift + 1, frames), pl.ds(1, RING - 1)]
            copy = send(block, block, turn_send.at[1], turn_recv.at[1], partner)
            copy.wait_recv()
            copy.wait_send()
            return
        for t in (-1, 1):
            block = clip_pad.at[shift, pl.ds(1, RING)]
            copy = send(block, block, turn_send.at[1 + t], turn_recv.at[1 + t], partner)

            @pl.when(inside(t, 0))
            def _():
                copy.wait_send()

            @pl.when(inside(-t, 0))
            def _():
                copy.wait_recv()

    def halo_copy(which, pad, t, r):
        slot = which * len(moves) + moves.index((t, r))
        target = device(tm=me["tm"] + t, rows=me["rows"] + r)
        sems = halo_send.at[slot], halo_recv.at[slot]
        if r != 0:
            side = 0 if r > 0 else 1
            return send(edge_out.at[which, side], edge_in.at[which, side, 1 - t], *sems, target)
        pair = pad.shape[0] > frames + 2
        mine, base = (shift, 2 - shift) if pair else (0, 0)
        src = mine + frames if t > 0 else mine + 1
        dst = base if t > 0 else base + frames + 1
        return send(
            pad.at[src, pl.ds(1, RING)], pad.at[dst, pl.ds(1, RING)], *sems, target
        )

    def edge_rows(value):
        block = value.reshape(lines, cols, value.shape[-1])
        return block[:, cols - 1], block[:, 0]

    def halo_start(which, pad, value, skip=False):
        for side, rows_out in enumerate(edge_rows(value)):
            edge_out[which, side] = rows_out
        for t, r in sorted(moves, key=lambda move: move[1] != 0):
            if skip and r == 0:
                continue

            @pl.when(inside(t, r))
            def _():
                halo_copy(which, pad, t, r).start()

    def halo_wait(which, pad, skip=False):
        for t, r in moves:
            if skip and r == 0:
                continue

            @pl.when(inside(t, r))
            def _():
                halo_copy(which, pad, t, r).wait_send()

            @pl.when(inside(-t, -r))
            def _():
                halo_copy(which, pad, t, r).wait_recv()

    def columns(value):
        return lax.rem(lax.broadcasted_iota(jnp.int32, value.shape, 0), cols)

    def spread(edge):
        return jnp.broadcast_to(edge[:, None, :], (lines, cols, edge.shape[-1])).reshape(count, -1)

    def earlier(value, edge):
        return jnp.where(columns(value) == 0, spread(edge), pltpu.roll(value, 1, 0))

    def later(value, edge):
        return jnp.where(columns(value) == cols - 1, spread(edge), pltpu.roll(value, count - 1, 0))

    def pair_frames(pad, slot):
        block = pad.at[pl.ds(4 * core, 2), pl.ds(1, RING)]
        return send(block, block, pair_send.at[slot], pair_recv.at[slot], partner)

    def edge_left(which):
        line = lax.broadcasted_iota(jnp.int32, (lines, chans), 0)
        row = lax.rem(line, RING)

        def piece(side, s, q):
            below, level, above = (edge_in[which, side, k] for k in range(3))
            if s == 1:
                value = level
            else:
                value = pltpu.roll(level, RING, 0)
                if s == 0:
                    value = jnp.where(line < RING, pltpu.roll(below, RING, 0), value)
                else:
                    value = jnp.where(line < RING, value, pltpu.roll(above, RING, 0))
            if q == 0:
                value = jnp.where(row == 0, 0.0, pltpu.roll(value, 1, 0))
            elif q == 2:
                value = jnp.where(row == RING - 1, 0.0, pltpu.roll(value, lines - 1, 0))
            return value

        return [
            jnp.concatenate([
                jnp.concatenate([piece(side, s, q) for q in range(TAPS)], axis=1)
                for side in range(2)
            ], axis=0).astype(jnp.bfloat16)
            for s in range(TAPS)
        ]

    def conv(which, pad, transpose, wait, ready):
        base = shift if pad.shape[0] > frames + 2 else 0

        def left(at, size):
            return jnp.concatenate([
                pad[pl.ds(base + at, size), pl.ds(q, RING)].reshape(size * half, chans)
                for q in range(TAPS)
            ], axis=1)

        def product(value, s, d):
            a = TAPS - 1 - s if transpose else s
            taps = [
                w_ref[(a * TAPS + (TAPS - 1 - q if transpose else q)) * TAPS + d]
                for q in range(TAPS)
            ]
            if transpose:
                return lax.dot_general(
                    value, jnp.concatenate(taps, axis=1), (((1,), (1,)), ((), ())),
                    preferred_element_type=jnp.float32,
                )
            return jnp.dot(
                value, jnp.concatenate(taps, axis=0), preferred_element_type=jnp.float32
            )

        own = left(1, frames)
        for d in range(TAPS):
            level = product(own, 1, d)
            acc[d, pl.ds(0, half)] = level[:half] + product(own[half:], 2, d)
            acc[d, pl.ds(half, half)] = level[half:] + product(own[:half], 0, d)
        wait()
        ready()
        edges = edge_left(which)
        below = jnp.concatenate([left(0, 1), edges[0]], axis=0)
        above = jnp.concatenate([left(frames + 1, 1), edges[2]], axis=0)
        sums, sides = [], []
        for d in range(TAPS):
            low, high = product(below, 0, d), product(above, 2, d)
            sums.append(jnp.concatenate([
                acc[d, pl.ds(0, half)] + low[:half], acc[d, pl.ds(half, half)] + high[:half]
            ], axis=0))
            sides.append(
                None if d == 1 else low[half:] + high[half:] + product(edges[1], 1, d)
            )
        d0, d2 = (2, 0) if transpose else (0, 2)
        return (
            earlier(sums[d0], sides[d0][:lines]) + sums[1] + later(sums[d2], sides[d2][lines:])
        )


    def lane_half(value, mine=True):
        low, high = value[:, :LANES], value[:, LANES:]
        return jnp.where(core == 0, low, high) if mine else jnp.where(core == 0, high, low)

    def three(value, before, after):
        return jnp.concatenate(
            [later(value, after), value, earlier(value, before)], axis=1
        ).astype(jnp.bfloat16)

    clip_copy.wait()
    turn_start()
    mine = pl.ds(pl.multiple_of(me["rows"] * cols, cols), cols)
    clip_pad[pl.ds(shift + 1, frames), 1 + me["rows"]] = clips_vm[:, mine]
    weight_copy.wait()
    bias_copy.wait()
    head_copy.wait()
    pair_clips, pair_grads = pair_frames(clip_pad, 0), pair_frames(grad_pad, 1)
    turn_wait(True)
    clips = clip_pad[pl.ds(shift + 1, frames), pl.ds(1, RING)].reshape(count, chans)
    halo_start(0, clip_pad, clips.astype(jnp.float32), True)

    def wait_clips():
        turn_wait(False)
        halo_wait(0, clip_pad, True)

    pre = conv(0, clip_pad, False, wait_clips, pair_clips.start) + bias_ref[...]
    sig = jax.nn.sigmoid(pre)
    slope = sig * (1.0 + pre * (1.0 - sig))
    slope_ref[...] = slope
    curve_ref[...] = sig * (1.0 - sig) * (2.0 + pre * (1.0 - 2.0 * sig))
    score = (head_ref[...] * slope).astype(jnp.bfloat16)
    score_pad[pl.ds(1, frames), pl.ds(1, RING)] = score.reshape(frames, RING, cols, chans)
    halo_start(1, score_pad, score.astype(jnp.float32))

    input_grad = conv(
        1, score_pad, True, lambda: halo_wait(1, score_pad), lambda: None
    ).astype(jnp.bfloat16)
    grad_pad[pl.ds(shift + 1, frames), pl.ds(1, RING)] = input_grad.reshape(
        frames, RING, cols, chans
    )
    halo_start(2, grad_pad, input_grad.astype(jnp.float32))

    value = score_pad[pl.ds(1, frames), pl.ds(1, RING)].reshape(count, chans).astype(jnp.float32)
    for mine, ref in ((True, cat_s.at[core]), (False, stage_s)):
        ref[...] = three(
            lane_half(value, mine),
            lane_half(edge_in[1, 0, 1], mine), lane_half(edge_in[1, 1, 1], mine),
        )
    pair_s = send(stage_s, cat_s.at[core], pair_send.at[2], pair_recv.at[2], partner)
    pair_s.start()

    back = penalty_weight * conv(
        2, grad_pad, False, lambda: halo_wait(2, grad_pad), pair_grads.start
    )
    pre_grad = back * head_ref[...] * curve_ref[...]
    value = pre_grad.astype(jnp.bfloat16).astype(jnp.float32)
    for side, rows_out in enumerate(edge_rows(value)):
        last_out[side] = rows_out
    stage_p[...] = lane_half(value, False).astype(jnp.bfloat16)
    pair_p = send(stage_p, raw_p.at[1], pair_send.at[3], pair_recv.at[3], partner)
    pair_p.start()
    raw_p[0] = lane_half(value).astype(jnp.bfloat16)

    def last_copy(r, c):
        side = 0 if r > 0 else 1
        slot = 2 * side + c
        other = core if c == 0 else 1 - core
        return send(
            last_out.at[side], last_in.at[side, c], last_send.at[slot], last_recv.at[slot],
            device(tm=me["tm"] - core + other, rows=me["rows"] + r),
        )

    for r in (-1, 1):
        @pl.when(inside(0, r))
        def _():
            for c in range(CORES):
                last_copy(r, c).start()

    small_mine[...] = jnp.zeros_like(small_mine)
    for k, value in enumerate((pre_grad, back * slope_ref[...])):
        whole = jnp.sum(value, axis=0, keepdims=True)
        small_mine[pl.ds(2 * k, 1)] = whole[:, :LANES]
        small_mine[pl.ds(2 * k + 1, 1)] = whole[:, LANES:]
    small_targets = [
        [partner],
        [chip(x=other) for other in ring_peers("x", RING)],
        [chip(y=other) for other in ring_peers("y", RING)],
        [chip(z=other) for other in ring_peers("z", DEEP)],
    ]
    smalls = []

    def small_start(level):
        at = sum(len(group) for group in small_targets[:level])
        copies = []
        for k, target in enumerate(small_targets[level]):
            copy = send(
                small_mine.at[pl.ds(level * SUB, SUB)], small_land.at[pl.ds((at + k) * SUB, SUB)],
                small_send.at[0], small_recv.at[level], target,
            )
            copy.start()
            copies.append(at + k)
        smalls.append(copies)

    def small_end(level):
        value = small_mine[pl.ds(level * SUB, SUB)]
        slots = smalls[level]
        lands = small_land.at[pl.ds(slots[0] * SUB, len(slots) * SUB)]
        send(lands, lands, small_send.at[0], small_recv.at[level], partner).wait_recv()
        for slot in slots:
            value = value + small_land[pl.ds(slot * SUB, SUB)]
        small_mine[pl.ds((level + 1) * SUB, SUB)] = value

    small_start(0)

    routes = []
    for p in range(PARTS):
        first, second = ("x", "y") if p < GROUPS else ("y", "x")
        m = here[first]
        ways = []
        for v in range(WAYS):
            if v == 0:
                near, bit1, far, bit2 = flip(m), lax.rem((m + 1) // 2, 2), mirror(m), m // 2
            else:
                near, bit1, far, bit2 = mirror(m), m // 2, flip(m), lax.rem(m, 2)
            four = 8 * v + 4 * bit1
            two = four + 2 * bit2
            ways.append(dict(
                near=chip(**{first: near}), far=chip(**{first: far}),
                four=four, other4=16 * v + 4 - four, two=two, other2=2 * four + 2 - two,
            ))
        routes.append(dict(ways=ways, second=second))

    def unit_of(p, n):
        low, high = (way["two"] for way in routes[p]["ways"])
        upper = n // 2
        return (1 - upper) * (low + n) + upper * (high + n - 2)

    for p, route in enumerate(routes):
        route["unit"] = unit_of(p, here[route["second"]])

    def encode(p, base, units, code, at):
        def peak(k, tops):
            for t in range(SHARE):
                tops = jnp.maximum(tops, jnp.abs(total[p, base + k, t]))
            return tops

        top = lax.fori_loop(
            0, units, peak, jnp.zeros((SUB, LANES), jnp.float32), unroll=min(units, UNROLL)
        )
        top = (top * 1.01 + 1e-30).astype(jnp.bfloat16)
        rate = SPAN / top.astype(jnp.float32)
        code[(*at, units * SHARE)] = top

        def fill(k, carry):
            code[(*at, pl.ds(k * SHARE, SHARE))] = jnp.exp2(
                total[p, base + k] * rate[None]
            ).astype(jnp.bfloat16)
            return carry

        lax.fori_loop(0, units, fill, 0, unroll=min(units, UNROLL))

    def absorb(p, base, units, lands):
        scales = [
            land[(*at, units * SHARE)].astype(jnp.float32) * (1.0 / (SPAN * math.log(2.0)))
            for land, at in lands
        ]

        def add(k, carry):
            value = total[p, base + k]
            for (land, at), scale in zip(lands, scales):
                block = land[(*at, pl.ds(k * SHARE, SHARE))].astype(jnp.float32)
                value = value + jnp.log(block) * scale[None]
            total[p, base + k] = value
            return carry

        lax.fori_loop(0, units, add, 0, unroll=min(units, UNROLL))

    def halving(p, v, code, land, send_sem, recv_sem, to):
        return send(
            code.at[p, v], land.at[p, v], send_sem.at[0], recv_sem.at[p], routes[p]["ways"][v][to]
        )

    def arrived(block, recv_sem, slot):
        send(block, block, send1.at[0], recv_sem.at[slot], partner).wait_recv()

    def copy3(p):
        second = routes[p]["second"]
        return [
            send(
                code3.at[p, k], land3.at[p, k], send3.at[0], recv3.at[p],
                chip(**{second: other}),
            )
            for k, other in enumerate(ring_peers(second, RING))
        ]

    def start1(p):
        for v, way in enumerate(routes[p]["ways"]):
            encode(p, way["other4"], 4, code1, (p, v))
            halving(p, v, code1, land1, send1, recv1, "near").start()

    def start2(p):
        for v, way in enumerate(routes[p]["ways"]):
            encode(p, way["other2"], 2, code2, (p, v))
            halving(p, v, code2, land2, send2, recv2, "far").start()

    def start3(p):
        second = routes[p]["second"]
        for k, (copy, other) in enumerate(zip(copy3(p), ring_peers(second, RING))):
            encode(p, unit_of(p, other), 1, code3, (p, k))
            copy.start()

    def correlate(pad, cat, a, b):
        left = pad[a : a + 2 * frames, b : b + RING].reshape(2 * count, chans)
        right = cat[...].reshape(2 * count, TAPS * LANES)
        return lax.dot_general(
            left, right, (((0,), (0,)), ((), ())), preferred_element_type=jnp.float32
        )

    def tiles(value, h, d):
        block = value[h * UNITS * SUB : (h + 1) * UNITS * SUB, d * LANES : (d + 1) * LANES]
        return block.reshape(UNITS, SUB, LANES)

    def place(a, b, d):
        tap = (a * TAPS + b) * TAPS + d
        return tap // SHARE, tap % SHARE

    for h in range(2):
        total[h * GROUPS + GROUPS - 1, :, SHARE - 1] = jnp.zeros((UNITS, SUB, LANES), jnp.float32)
    pair_s.wait()
    pair_grads.wait()
    for a in range(TAPS):
        for b in range(TAPS):
            value = penalty_weight * correlate(grad_pad, cat_s, a, b)
            for d in range(TAPS):
                g, t = place(a, b, d)
                for h in range(2):
                    total[h * GROUPS + g, :, t] = tiles(value, h, d)
    pair_clips.wait()
    pair_p.wait()
    for r in (-1, 1):
        for c in range(CORES):
            @pl.when(inside(0, r))
            def _():
                last_copy(r, c).wait_send()

            @pl.when(inside(0, -r))
            def _():
                last_copy(r, c).wait_recv()

    for c in range(CORES):
        ref = cat_p.at[core if c == 0 else 1 - core]
        ref[...] = three(
            raw_p[c].astype(jnp.float32), lane_half(last_in[0, c]), lane_half(last_in[1, c])
        )
    begun = 0
    for a in range(TAPS):
        for b in range(TAPS):
            value = correlate(clip_pad, cat_p, a, b)
            for d in range(TAPS):
                g, t = place(a, b, d)
                for h in range(2):
                    p = h * GROUPS + g
                    block = tiles(value, h, d)
                    total[p, :, t] = block + total[p, :, t]
            done = (a * TAPS + b + 1) * TAPS
            while begun < GROUPS and done >= min((begun + 1) * SHARE, TAPS**3):
                for h in range(2):
                    start1(h * GROUPS + begun)
                begun += 1

    small_end(0)
    small_start(1)
    order = [h * GROUPS + g for g in range(GROUPS) for h in range(2)]
    for p in order:
        arrived(land1.at[p], recv1, p)
        for v, way in enumerate(routes[p]["ways"]):
            absorb(p, way["four"], 4, [(land1, (p, v))])
        start2(p)
    small_end(1)
    small_start(2)
    for p in order:
        arrived(land2.at[p], recv2, p)
        for v, way in enumerate(routes[p]["ways"]):
            absorb(p, way["two"], 2, [(land2, (p, v))])
        start3(p)
    small_end(2)
    small_start(3)

    z = here["z"]

    def copy4(p):
        return send(code4.at[p], land4.at[z], send4.at[0], recv4.at[0], chip(z=p))

    for p in order:
        send(land3.at[p], land3.at[p], send3.at[0], recv3.at[p], partner).wait_recv()
        absorb(p, routes[p]["unit"], 1, [(land3, (p, k)) for k in range(RING - 1)])

        @pl.when(z != p)
        def _():
            encode(p, routes[p]["unit"], 1, code4, (p,))
            copy4(p).start()

    unit = None
    for p in range(PARTS):
        term = jnp.where(z == p, routes[p]["unit"], 0)
        unit = term if unit is None else unit + term
    others = ring_peers("z", DEEP)
    seven = land4.at[pl.ds(0, DEEP - 1)]
    send(seven, seven, send4.at[0], recv4.at[0], partner).wait_recv()
    absorb(z, unit, 1, [(land4, (other,)) for other in others])
    encode(z, unit, 1, full, (z, core, unit))

    def zcopy(k, other):
        block = full.at[z, core, unit]
        return send(block, block, zsend.at[0], zrecv.at[z], chip(z=other))

    def zgot(p):
        block = full.at[p, core, routes[p]["unit"]]
        return send(block, block, zsend.at[0], zrecv.at[p], chip(z=p))

    for k, other in enumerate(others):
        zcopy(k, other).start()
    small_end(3)

    def qcopies(p):
        second = routes[p]["second"]
        block = full.at[p, core, routes[p]["unit"]]
        return [
            send(block, block, qsend.at[0], qrecv.at[p], chip(**{second: other}))
            for k, other in enumerate(ring_peers(second, RING))
        ]

    def far_copy(p, v):
        block = full.at[p, core, pl.ds(routes[p]["ways"][v]["two"], 2)]
        return send(block, block, far_send.at[0], far_recv.at[p], routes[p]["ways"][v]["far"])

    def near_copy(p, v):
        block = full.at[p, core, pl.ds(routes[p]["ways"][v]["four"], 4)]
        return send(block, block, near_send.at[0], near_recv.at[p], routes[p]["ways"][v]["near"])

    def core_start(p, second):
        for way in routes[p]["ways"]:
            block = full.at[p, core, pl.ds(way["other4"] if second else way["four"], 4)]
            send(block, block, core_send.at[0], core_recv.at[2 * p + second], partner).start()

    def units(count):
        return full.at[0, 0, pl.ds(0, count)]

    for p in order:
        @pl.when(z != p)
        def _():
            zgot(p).wait_recv()

        for copy in qcopies(p):
            copy.start()
    for p in order:
        three = full.at[p, core, pl.ds(0, RING - 1)]
        send(three, three, qsend.at[0], qrecv.at[p], partner).wait_recv()
        for v in range(WAYS):
            far_copy(p, v).start()
    def reveal(p, c, which):
        h, g = p // GROUPS, p % GROUPS
        taps = min(SHARE, TAPS**3 - g * SHARE)
        lane = pl.ds(pl.multiple_of(c * LANES, LANES), LANES)

        def one(base, k, carry):
            scale = full[p, c, base + k, SHARE].astype(jnp.float32) * (1.0 / (SPAN * math.log(2.0)))
            block = full[p, c, base + k, pl.ds(0, taps)].astype(jnp.float32)
            out_ref[pl.ds(g * SHARE, taps), h * UNITS + base + k, :, lane] = (
                jnp.log(block) * scale[None]
            )
            return carry

        for way in routes[p]["ways"]:
            lax.fori_loop(0, 4, functools.partial(one, way[which]), 0, unroll=UNROLL)

    for k, ref in enumerate((bias_out, head_out)):
        at = (len(small_targets)) * SUB + 2 * k
        ref[:, pl.ds(0, LANES)] = small_mine[pl.ds(at, 1)]
        ref[:, pl.ds(LANES, LANES)] = small_mine[pl.ds(at + 1, 1)]
    for p in order:
        arrived(units(4), far_recv, p)
        for v in range(WAYS):
            near_copy(p, v).start()
        core_start(p, 0)
    def reveal_far(p):
        arrived(units(8), core_recv, 2 * p)
        reveal(p, 1 - core, "four")

    for k, p in enumerate(order):
        reveal(p, core, "four")
        if k >= 2:
            reveal_far(order[k - 2])
        arrived(units(8), near_recv, p)
        core_start(p, 1)
        if k >= 1:
            reveal(order[k - 1], core, "other4")
    for p in order[-2:]:
        reveal_far(p)
    reveal(order[-1], core, "other4")
    for p in order:
        arrived(units(8), core_recv, 2 * p + 1)
        reveal(p, 1 - core, "other4")
    for block, sem in (
        (small_land, small_send), (code1, send1), (code2, send2), (code3, send3),
        (code4.at[pl.ds(0, DEEP - 1)], send4), (full.at[0, 0, pl.ds(0, DEEP - 1)], zsend),
        (full.at[pl.ds(0, 3), 0, pl.ds(0, 8)], qsend), (full.at[0], far_send),
        (full.at[pl.ds(0, 2)], near_send), (full.at[pl.ds(0, 4)], core_send),
    ):
        send(block, block, sem.at[0], sem.at[0], partner).wait_send()


def store_kernel(grad_ref, bias_ref, head_ref, grad_out, bias_out, head_out, sem):
    step = TAPS
    copies = [
        pltpu.make_async_copy(
            grad_ref.at[pl.ds(k * step, step)], grad_out.at[pl.ds(k * step, step)], sem.at[k]
        )
        for k in range(TAPS**3 // step)
    ]
    copies.append(pltpu.make_async_copy(bias_ref, bias_out, sem.at[TAPS**2]))
    copies.append(pltpu.make_async_copy(head_ref, head_out, sem.at[TAPS**2 + 1]))
    for copy in copies:
        copy.start()
    for copy in copies:
        copy.wait()


def per_device(sizes, clips, weight, bias, head):
    _, frames, _, cols, chans = clips.shape
    count = frames * cols
    lines = frames * RING
    dp, tm, rows = sizes
    assert (rows, dp * 2, tm // 4, chans) == (RING, RING, DEEP, 2 * LANES)
    dma = pltpu.SemaphoreType.DMA
    vmem = pl.BlockSpec(memory_space=pltpu.VMEM)
    hbm = pl.BlockSpec(memory_space=pltpu.HBM)
    row = jax.ShapeDtypeStruct((1, chans), jnp.float32)
    field = pltpu.VMEM((count, chans), jnp.float32)

    def pad(n):
        return pltpu.VMEM((n, RING + 2, cols // RING, chans), jnp.bfloat16)

    def coded(*lead, units):
        return pltpu.VMEM((*lead, units * SHARE + 1, SUB, LANES), jnp.bfloat16)

    cat = pltpu.VMEM((CORES, count, TAPS * LANES), jnp.bfloat16)
    stage = pltpu.VMEM((count, TAPS * LANES), jnp.bfloat16)
    smalls = 1 + 2 * (RING - 1) + DEEP - 1
    both = lambda n: [dma((n,)), dma((n,))]
    one = lambda n: [dma((1,)), dma((n,))]
    grad_weight, grad_bias, grad_head = pl.pallas_call(
        functools.partial(kernel, sizes),
        out_shape=(
            jax.ShapeDtypeStruct((TAPS**3, 2 * UNITS, SUB, chans), jnp.float32),
            row, row,
        ),
        in_specs=[hbm, hbm, hbm, hbm],
        out_specs=(vmem, vmem, vmem),
        scratch_shapes=[
            pltpu.VMEM((1, chans), jnp.float32), pltpu.VMEM((1, chans), jnp.float32),
            pltpu.VMEM((TAPS**3, chans, chans), jnp.bfloat16),
            pltpu.VMEM((frames, cols, chans), jnp.bfloat16),
            pad(2 * frames + 2), pad(frames + 2), pad(2 * frames + 2),
            pltpu.VMEM((TAPS, count, chans), jnp.float32),
            field, field,
            cat, cat, stage, pltpu.VMEM((count, LANES), jnp.bfloat16),
            pltpu.VMEM((CORES, count, LANES), jnp.bfloat16),
            pltpu.VMEM((TAPS, 2, lines, chans), jnp.float32),
            pltpu.VMEM((TAPS, 2, 3, lines, chans), jnp.float32),
            pltpu.VMEM((2, lines, chans), jnp.float32),
            pltpu.VMEM((2, CORES, lines, chans), jnp.float32),
            pltpu.VMEM((PARTS, UNITS, SHARE, SUB, LANES), jnp.float32),
            coded(PARTS, WAYS, units=4), coded(PARTS, WAYS, units=4),
            coded(PARTS, WAYS, units=2), coded(PARTS, WAYS, units=2),
            coded(PARTS, RING - 1, units=1), coded(PARTS, RING - 1, units=1),
            coded(DEEP, units=1), coded(DEEP, units=1),
            coded(PARTS, CORES, UNITS, units=1),
            pltpu.VMEM((5 * SUB, LANES), jnp.float32),
            pltpu.VMEM((smalls * SUB, LANES), jnp.float32),
            dma((4,)), *both(3), *both(24), *both(4), *both(4), *one(PARTS), *one(PARTS), *one(PARTS), *one(1),
            *one(DEEP), *one(PARTS), *one(PARTS), *one(PARTS), *one(2 * PARTS), *one(4),
        ],
        compiler_params=pltpu.CompilerParams(
            collective_id=0, has_side_effects=True, vmem_limit_bytes=40 * 1024 * 1024
        ),
    )(
        *[
            pltpu.with_memory_space_constraint(value, pltpu.HBM)
            for value in (
                clips.reshape(frames, cols, chans), weight.reshape(TAPS**3, chans, chans),
                bias.reshape(1, chans), head.reshape(1, chans),
            )
        ]
    )
    grad_weight, grad_bias, grad_head = pl.pallas_call(
        store_kernel,
        out_shape=(
            jax.ShapeDtypeStruct((TAPS**3, 2 * UNITS, SUB, chans), jnp.float32), row, row,
        ),
        in_specs=[vmem, vmem, vmem],
        out_specs=(hbm, hbm, hbm),
        scratch_shapes=[dma((TAPS**2 + 2,))],
        compiler_params=pltpu.CompilerParams(vmem_limit_bytes=8 * 1024 * 1024),
    )(grad_weight, grad_bias, grad_head)
    grad_weight = grad_weight.reshape(TAPS, TAPS, TAPS, chans, chans)
    return grad_weight, grad_bias.reshape(chans), grad_head.reshape(chans)


def solution(mesh):
    sizes = tuple(mesh.shape[axis] for axis in ("dp", "tm", "rows"))
    return jax.shard_map(
        functools.partial(per_device, sizes),
        mesh=mesh,
        in_specs=(P("dp", "tm", "rows", None, None), P(), P(), P()),
        out_specs=(P(), P(), P()),
        check_vma=False,
    )
```

```python
import functools
import math

import jax
import jax.numpy as jnp
from jax import lax
from jax.experimental import pallas as pl
from jax.experimental.pallas import tpu as pltpu
from jax.sharding import PartitionSpec as P

penalty_weight = 0.01
MESH = pl.DeviceIdType.MESH
SUB = 8
LANES = 128
TAPS = 3
SPAN = 120.0
RING = 4
DEEP = 8
CORES = 2
GROUPS = 4
SHARE = 7
UNITS = 16
UNROLL = 4
WAYS = 2
PARTS = 2 * GROUPS


def flip(m):
    return m + 1 - 2 * lax.rem(m, 2)


def mirror(m):
    return RING - 1 - m


def kernel(
    sizes, clips_ref, weight_ref, bias_hbm, head_hbm,
    out_ref, bias_out, head_out,
    bias_ref, head_ref, w_ref, clips_vm, clip_pad, score_pad, grad_pad, acc, slope_ref, curve_ref,
    cat_s, cat_p, stage_s, stage_p, raw_p, side_out, side_in, edge_out, edge_in, last_out, last_in, total,
    code1, land1, code2, land2, code3, land3, code4, land4, full, small_mine, small_land,
    local_sem, turn_send, turn_recv, halo_send, halo_recv, last_send, last_recv,
    pair_send, pair_recv, send1, recv1, send2, recv2,
    send3, recv3, send4, recv4, zsend, zrecv, qsend, qrecv, near_send, near_recv,
    far_send, far_recv, core_send, core_recv, small_send, small_recv,
):
    dp, tm, rows = sizes
    frames, wide, chans = clips_ref.shape
    cols = wide // RING
    lines = frames * RING
    count = lines * cols
    half = count // 2
    me = {"dp": lax.axis_index("dp"), "tm": lax.axis_index("tm"), "rows": lax.axis_index("rows")}
    core = lax.rem(me["tm"], CORES)
    here = {
        "x": me["rows"],
        "y": 2 * me["dp"] + lax.rem(me["tm"] // 2, 2),
        "z": me["tm"] // 4,
        "c": core,
    }

    def device(**moved):
        place = dict(me, **moved)
        return (place["dp"], place["tm"], place["rows"])

    def chip(**moved):
        place = dict(here, **moved)
        return (
            place["y"] // 2,
            place["z"] * 4 + lax.rem(place["y"], 2) * 2 + place["c"],
            place["x"],
        )

    partner = chip(c=1 - core)

    def ring_peers(axis, size):
        return [lax.rem(here[axis] + step, size) for step in range(1, size)]

    weight_copy = pltpu.make_async_copy(weight_ref, w_ref, local_sem.at[0])
    weight_copy.start()
    shift = 2 * core
    clip_copy = pltpu.make_async_copy(clips_ref, clips_vm, local_sem.at[1])
    clip_copy.start()
    bias_copy = pltpu.make_async_copy(bias_hbm, bias_ref, local_sem.at[2])
    head_copy = pltpu.make_async_copy(head_hbm, head_ref, local_sem.at[3])
    bias_copy.start()
    head_copy.start()
    for pad, base in ((clip_pad, shift), (score_pad, 0), (grad_pad, shift)):
        pad[:, 0] = jnp.zeros((pad.shape[0], cols, chans), pad.dtype)
        pad[:, RING + 1] = jnp.zeros((pad.shape[0], cols, chans), pad.dtype)
        for at in (base, base + frames + 1):
            pad[at, pl.ds(1, RING)] = jnp.zeros((RING, cols, chans), pad.dtype)
    edge_in[...] = jnp.zeros_like(edge_in)
    side_in[...] = jnp.zeros_like(side_in)
    last_in[...] = jnp.zeros_like(last_in)

    moves = [(t, r) for t in (-1, 0, 1) for r in (-1, 0, 1) if (t, r) != (0, 0)]

    def inside(t, r):
        ok = None
        for axis, step, size in (("tm", t, tm), ("rows", r, rows)):
            if step:
                cond = me[axis] > 0 if step < 0 else me[axis] < size - 1
                ok = cond if ok is None else jnp.logical_and(ok, cond)
        return ok

    barrier = pltpu.get_barrier_semaphore()
    friends = [partner]
    friends += [chip(x=other) for other in ring_peers("x", RING)]
    friends += [chip(y=other) for other in ring_peers("y", RING)]
    friends += [chip(z=other) for other in ring_peers("z", DEEP)]
    for friend in friends:
        pl.semaphore_signal(barrier, inc=1, device_id=friend, device_id_type=MESH)
    expected = len(friends)
    for t in (-1, 1):
        expected = expected + RING * inside(t, 0).astype(jnp.int32)

        @pl.when(inside(t, 0))
        def _():
            for row in range(RING):
                pl.semaphore_signal(
                    barrier, inc=1, device_id=device(tm=me["tm"] + t, rows=row),
                    device_id_type=MESH,
                )
    pl.semaphore_wait(barrier, expected)

    def send(src, dst, send_sem, recv_sem, target):
        return pltpu.make_async_remote_copy(
            src_ref=src, dst_ref=dst, send_sem=send_sem, recv_sem=recv_sem,
            device_id=target, device_id_type=MESH,
        )

    def turn_copy(t, step):
        other = lax.rem(me["rows"] + step, RING)
        part = pl.ds(pl.multiple_of(other * cols, cols), cols)
        base = shift if t == 0 else 2 - shift
        src = {0: pl.ds(0, frames), 1: pl.ds(frames - 1, 1), -1: pl.ds(0, 1)}[t]
        dst = {0: pl.ds(base + 1, frames), 1: pl.ds(base, 1), -1: pl.ds(base + frames + 1, 1)}[t]
        return send(
            clips_vm.at[src, part], clip_pad.at[dst, 1 + me["rows"]],
            turn_send.at[1 + t], turn_recv.at[1 + t],
            device(tm=me["tm"] + t, rows=other),
        )

    def side_copy(t, step):
        other = lax.rem(me["rows"] + step, RING)
        return send(
            side_out.at[other], side_in.at[1 - t, me["rows"]],
            turn_send.at[4 + t], turn_recv.at[4 + t],
            device(tm=me["tm"] + t, rows=other),
        )

    def turn_start():
        for step in range(1, RING):
            turn_copy(0, step).start()
        for other in range(RING):
            at = other * cols
            lines_out = [
                clips_vm[f, c : c + 1].astype(jnp.float32) if 0 <= c < wide
                else jnp.zeros((1, chans), jnp.float32)
                for c in (at - 1, at + cols) for f in range(frames)
            ]
            lines_out.append(jnp.zeros((SUB - 2 * frames, chans), jnp.float32))
            side_out[other] = jnp.concatenate(lines_out, axis=0).astype(jnp.bfloat16)
        for step in range(1, RING):
            side_copy(0, step).start()
        for t in (-1, 1):
            @pl.when(inside(t, 0))
            def _():
                for step in range(RING):
                    turn_copy(t, step).start()
                    side_copy(t, step).start()
        side_in[1, me["rows"]] = side_out[me["rows"]]

    def turn_wait(level):
        if level:
            block = clip_pad.at[pl.ds(shift + 1, frames), pl.ds(1, RING - 1)]
            copy = send(block, block, turn_send.at[1], turn_recv.at[1], partner)
            copy.wait_recv()
            copy.wait_send()
            return
        block = side_in.at[1, pl.ds(0, RING - 1)]
        copy = send(block, block, turn_send.at[4], turn_recv.at[4], partner)
        copy.wait_recv()
        copy.wait_send()
        for t in (-1, 1):
            block, side = clip_pad.at[shift, pl.ds(1, RING)], side_in.at[0]
            copies = [
                send(block, block, turn_send.at[1 + t], turn_recv.at[1 + t], partner),
                send(side, side, turn_send.at[4 + t], turn_recv.at[4 + t], partner),
            ]

            @pl.when(inside(t, 0))
            def _():
                for copy in copies:
                    copy.wait_send()

            @pl.when(inside(-t, 0))
            def _():
                for copy in copies:
                    copy.wait_recv()

        line = lax.broadcasted_iota(jnp.int32, (lines, chans), 0)
        for k in range(3):
            blocks = [side_in[k, r].astype(jnp.float32) for r in range(RING)]
            for side in range(2):
                value = jnp.zeros((lines, chans), jnp.float32)
                for r in range(RING):
                    for f in range(frames):
                        at = side * frames + f
                        value = jnp.where(
                            line == f * RING + r,
                            jnp.broadcast_to(blocks[r][at : at + 1], (lines, chans)), value,
                        )
                edge_in[0, side, k] = value

    def halo_copy(which, pad, t, r):
        slot = (which - 1) * len(moves) + moves.index((t, r))
        target = device(tm=me["tm"] + t, rows=me["rows"] + r)
        sems = halo_send.at[slot], halo_recv.at[slot]
        if r != 0:
            side = 0 if r > 0 else 1
            return send(edge_out.at[which - 1, side], edge_in.at[which, side, 1 - t], *sems, target)
        pair = pad.shape[0] > frames + 2
        mine, base = (shift, 2 - shift) if pair else (0, 0)
        src = mine + frames if t > 0 else mine + 1
        dst = base if t > 0 else base + frames + 1
        return send(
            pad.at[src, pl.ds(1, RING)], pad.at[dst, pl.ds(1, RING)], *sems, target
        )

    def edge_rows(value):
        block = value.reshape(lines, cols, value.shape[-1])
        return block[:, cols - 1], block[:, 0]

    def halo_start(which, pad, value):
        for side, rows_out in enumerate(edge_rows(value)):
            edge_out[which - 1, side] = rows_out
        for t, r in sorted(moves, key=lambda move: move[1] != 0):
            @pl.when(inside(t, r))
            def _():
                halo_copy(which, pad, t, r).start()

    def halo_wait(which, pad):
        for t, r in moves:
            @pl.when(inside(t, r))
            def _():
                halo_copy(which, pad, t, r).wait_send()

            @pl.when(inside(-t, -r))
            def _():
                halo_copy(which, pad, t, r).wait_recv()

    def columns(value):
        return lax.rem(lax.broadcasted_iota(jnp.int32, value.shape, 0), cols)

    def spread(edge):
        return jnp.broadcast_to(edge[:, None, :], (lines, cols, edge.shape[-1])).reshape(count, -1)

    def earlier(value, edge):
        return jnp.where(columns(value) == 0, spread(edge), pltpu.roll(value, 1, 0))

    def later(value, edge):
        return jnp.where(columns(value) == cols - 1, spread(edge), pltpu.roll(value, count - 1, 0))

    def pair_frames(pad, slot):
        block = pad.at[pl.ds(4 * core, 2), pl.ds(1, RING)]
        return send(block, block, pair_send.at[slot], pair_recv.at[slot], partner)

    def edge_left(which):
        line = lax.broadcasted_iota(jnp.int32, (lines, chans), 0)
        row = lax.rem(line, RING)

        def piece(side, s, q):
            below, level, above = (edge_in[which, side, k] for k in range(3))
            if s == 1:
                value = level
            else:
                value = pltpu.roll(level, RING, 0)
                if s == 0:
                    value = jnp.where(line < RING, pltpu.roll(below, RING, 0), value)
                else:
                    value = jnp.where(line < RING, value, pltpu.roll(above, RING, 0))
            if q == 0:
                value = jnp.where(row == 0, 0.0, pltpu.roll(value, 1, 0))
            elif q == 2:
                value = jnp.where(row == RING - 1, 0.0, pltpu.roll(value, lines - 1, 0))
            return value

        return [
            jnp.concatenate([
                jnp.concatenate([piece(side, s, q) for q in range(TAPS)], axis=1)
                for side in range(2)
            ], axis=0).astype(jnp.bfloat16)
            for s in range(TAPS)
        ]

    def conv(which, pad, transpose, wait, ready):
        base = shift if pad.shape[0] > frames + 2 else 0

        def left(at, size):
            return jnp.concatenate([
                pad[pl.ds(base + at, size), pl.ds(q, RING)].reshape(size * half, chans)
                for q in range(TAPS)
            ], axis=1)

        def product(value, s, d):
            a = TAPS - 1 - s if transpose else s
            taps = [
                w_ref[(a * TAPS + (TAPS - 1 - q if transpose else q)) * TAPS + d]
                for q in range(TAPS)
            ]
            if transpose:
                return lax.dot_general(
                    value, jnp.concatenate(taps, axis=1), (((1,), (1,)), ((), ())),
                    preferred_element_type=jnp.float32,
                )
            return jnp.dot(
                value, jnp.concatenate(taps, axis=0), preferred_element_type=jnp.float32
            )

        own = left(1, frames)
        for d in range(TAPS):
            level = product(own, 1, d)
            acc[d, pl.ds(0, half)] = level[:half] + product(own[half:], 2, d)
            acc[d, pl.ds(half, half)] = level[half:] + product(own[:half], 0, d)
        wait()
        ready()
        edges = edge_left(which)
        below = jnp.concatenate([left(0, 1), edges[0]], axis=0)
        above = jnp.concatenate([left(frames + 1, 1), edges[2]], axis=0)
        sums, sides = [], []
        for d in range(TAPS):
            low, high = product(below, 0, d), product(above, 2, d)
            sums.append(jnp.concatenate([
                acc[d, pl.ds(0, half)] + low[:half], acc[d, pl.ds(half, half)] + high[:half]
            ], axis=0))
            sides.append(
                None if d == 1 else low[half:] + high[half:] + product(edges[1], 1, d)
            )
        d0, d2 = (2, 0) if transpose else (0, 2)
        return (
            earlier(sums[d0], sides[d0][:lines]) + sums[1] + later(sums[d2], sides[d2][lines:])
        )


    def lane_half(value, mine=True):
        low, high = value[:, :LANES], value[:, LANES:]
        return jnp.where(core == 0, low, high) if mine else jnp.where(core == 0, high, low)

    def three(value, before, after):
        return jnp.concatenate(
            [later(value, after), value, earlier(value, before)], axis=1
        ).astype(jnp.bfloat16)

    clip_copy.wait()
    turn_start()
    mine = pl.ds(pl.multiple_of(me["rows"] * cols, cols), cols)
    clip_pad[pl.ds(shift + 1, frames), 1 + me["rows"]] = clips_vm[:, mine]
    weight_copy.wait()
    bias_copy.wait()
    head_copy.wait()
    pair_clips, pair_grads = pair_frames(clip_pad, 0), pair_frames(grad_pad, 1)
    turn_wait(True)
    pre = conv(0, clip_pad, False, lambda: turn_wait(False), pair_clips.start) + bias_ref[...]
    sig = jax.nn.sigmoid(pre)
    slope = sig * (1.0 + pre * (1.0 - sig))
    slope_ref[...] = slope
    curve_ref[...] = sig * (1.0 - sig) * (2.0 + pre * (1.0 - 2.0 * sig))
    score = (head_ref[...] * slope).astype(jnp.bfloat16)
    score_pad[pl.ds(1, frames), pl.ds(1, RING)] = score.reshape(frames, RING, cols, chans)
    halo_start(1, score_pad, score.astype(jnp.float32))

    input_grad = conv(
        1, score_pad, True, lambda: halo_wait(1, score_pad), lambda: None
    ).astype(jnp.bfloat16)
    grad_pad[pl.ds(shift + 1, frames), pl.ds(1, RING)] = input_grad.reshape(
        frames, RING, cols, chans
    )
    halo_start(2, grad_pad, input_grad.astype(jnp.float32))

    value = score_pad[pl.ds(1, frames), pl.ds(1, RING)].reshape(count, chans).astype(jnp.float32)
    for mine, ref in ((True, cat_s.at[core]), (False, stage_s)):
        ref[...] = three(
            lane_half(value, mine),
            lane_half(edge_in[1, 0, 1], mine), lane_half(edge_in[1, 1, 1], mine),
        )
    pair_s = send(stage_s, cat_s.at[core], pair_send.at[2], pair_recv.at[2], partner)
    pair_s.start()

    back = penalty_weight * conv(
        2, grad_pad, False, lambda: halo_wait(2, grad_pad), pair_grads.start
    )
    pre_grad = back * head_ref[...] * curve_ref[...]
    value = pre_grad.astype(jnp.bfloat16).astype(jnp.float32)
    for side, rows_out in enumerate(edge_rows(value)):
        last_out[side] = rows_out
    stage_p[...] = lane_half(value, False).astype(jnp.bfloat16)
    pair_p = send(stage_p, raw_p.at[1], pair_send.at[3], pair_recv.at[3], partner)
    pair_p.start()
    raw_p[0] = lane_half(value).astype(jnp.bfloat16)

    def last_copy(r, c):
        side = 0 if r > 0 else 1
        slot = 2 * side + c
        other = core if c == 0 else 1 - core
        return send(
            last_out.at[side], last_in.at[side, c], last_send.at[slot], last_recv.at[slot],
            device(tm=me["tm"] - core + other, rows=me["rows"] + r),
        )

    for r in (-1, 1):
        @pl.when(inside(0, r))
        def _():
            for c in range(CORES):
                last_copy(r, c).start()

    small_mine[...] = jnp.zeros_like(small_mine)
    for k, value in enumerate((pre_grad, back * slope_ref[...])):
        whole = jnp.sum(value, axis=0, keepdims=True)
        small_mine[pl.ds(2 * k, 1)] = whole[:, :LANES]
        small_mine[pl.ds(2 * k + 1, 1)] = whole[:, LANES:]
    small_targets = [
        [partner],
        [chip(x=other) for other in ring_peers("x", RING)],
        [chip(y=other) for other in ring_peers("y", RING)],
        [chip(z=other) for other in ring_peers("z", DEEP)],
    ]
    smalls = []

    def small_start(level):
        at = sum(len(group) for group in small_targets[:level])
        copies = []
        for k, target in enumerate(small_targets[level]):
            copy = send(
                small_mine.at[pl.ds(level * SUB, SUB)], small_land.at[pl.ds((at + k) * SUB, SUB)],
                small_send.at[0], small_recv.at[level], target,
            )
            copy.start()
            copies.append(at + k)
        smalls.append(copies)

    def small_end(level):
        value = small_mine[pl.ds(level * SUB, SUB)]
        slots = smalls[level]
        lands = small_land.at[pl.ds(slots[0] * SUB, len(slots) * SUB)]
        send(lands, lands, small_send.at[0], small_recv.at[level], partner).wait_recv()
        for slot in slots:
            value = value + small_land[pl.ds(slot * SUB, SUB)]
        small_mine[pl.ds((level + 1) * SUB, SUB)] = value

    small_start(0)

    routes = []
    for p in range(PARTS):
        first, second = ("x", "y") if p < GROUPS else ("y", "x")
        m = here[first]
        ways = []
        for v in range(WAYS):
            if v == 0:
                near, bit1, far, bit2 = flip(m), lax.rem((m + 1) // 2, 2), mirror(m), m // 2
            else:
                near, bit1, far, bit2 = mirror(m), m // 2, flip(m), lax.rem(m, 2)
            four = 8 * v + 4 * bit1
            two = four + 2 * bit2
            ways.append(dict(
                near=chip(**{first: near}), far=chip(**{first: far}),
                four=four, other4=16 * v + 4 - four, two=two, other2=2 * four + 2 - two,
            ))
        routes.append(dict(ways=ways, second=second))

    def unit_of(p, n):
        low, high = (way["two"] for way in routes[p]["ways"])
        upper = n // 2
        return (1 - upper) * (low + n) + upper * (high + n - 2)

    for p, route in enumerate(routes):
        route["unit"] = unit_of(p, here[route["second"]])

    def encode(p, base, units, code, at):
        def peak(k, tops):
            for t in range(SHARE):
                tops = jnp.maximum(tops, jnp.abs(total[p, base + k, t]))
            return tops

        top = lax.fori_loop(
            0, units, peak, jnp.zeros((SUB, LANES), jnp.float32), unroll=min(units, UNROLL)
        )
        top = (top * 1.01 + 1e-30).astype(jnp.bfloat16)
        rate = SPAN / top.astype(jnp.float32)
        code[(*at, units * SHARE)] = top

        def fill(k, carry):
            code[(*at, pl.ds(k * SHARE, SHARE))] = jnp.exp2(
                total[p, base + k] * rate[None]
            ).astype(jnp.bfloat16)
            return carry

        lax.fori_loop(0, units, fill, 0, unroll=min(units, UNROLL))

    def absorb(p, base, units, lands):
        scales = [
            land[(*at, units * SHARE)].astype(jnp.float32) * (1.0 / (SPAN * math.log(2.0)))
            for land, at in lands
        ]

        def add(k, carry):
            value = total[p, base + k]
            for (land, at), scale in zip(lands, scales):
                block = land[(*at, pl.ds(k * SHARE, SHARE))].astype(jnp.float32)
                value = value + jnp.log(block) * scale[None]
            total[p, base + k] = value
            return carry

        lax.fori_loop(0, units, add, 0, unroll=min(units, UNROLL))

    def halving(p, v, code, land, send_sem, recv_sem, to):
        return send(
            code.at[p, v], land.at[p, v], send_sem.at[0], recv_sem.at[p], routes[p]["ways"][v][to]
        )

    def arrived(block, recv_sem, slot):
        send(block, block, send1.at[0], recv_sem.at[slot], partner).wait_recv()

    def copy3(p):
        second = routes[p]["second"]
        return [
            send(
                code3.at[p, k], land3.at[p, k], send3.at[0], recv3.at[p],
                chip(**{second: other}),
            )
            for k, other in enumerate(ring_peers(second, RING))
        ]

    def start1(p):
        for v, way in enumerate(routes[p]["ways"]):
            encode(p, way["other4"], 4, code1, (p, v))
            halving(p, v, code1, land1, send1, recv1, "near").start()

    def start2(p):
        for v, way in enumerate(routes[p]["ways"]):
            encode(p, way["other2"], 2, code2, (p, v))
            halving(p, v, code2, land2, send2, recv2, "far").start()

    def start3(p):
        second = routes[p]["second"]
        for k, (copy, other) in enumerate(zip(copy3(p), ring_peers(second, RING))):
            encode(p, unit_of(p, other), 1, code3, (p, k))
            copy.start()

    def correlate(pad, cat, a, b):
        left = pad[a : a + 2 * frames, b : b + RING].reshape(2 * count, chans)
        right = cat[...].reshape(2 * count, TAPS * LANES)
        return lax.dot_general(
            left, right, (((0,), (0,)), ((), ())), preferred_element_type=jnp.float32
        )

    def tiles(value, h, d):
        block = value[h * UNITS * SUB : (h + 1) * UNITS * SUB, d * LANES : (d + 1) * LANES]
        return block.reshape(UNITS, SUB, LANES)

    def place(a, b, d):
        tap = (a * TAPS + b) * TAPS + d
        return tap // SHARE, tap % SHARE

    for h in range(2):
        total[h * GROUPS + GROUPS - 1, :, SHARE - 1] = jnp.zeros((UNITS, SUB, LANES), jnp.float32)
    pair_s.wait()
    pair_grads.wait()
    for a in range(TAPS):
        for b in range(TAPS):
            value = penalty_weight * correlate(grad_pad, cat_s, a, b)
            for d in range(TAPS):
                g, t = place(a, b, d)
                for h in range(2):
                    total[h * GROUPS + g, :, t] = tiles(value, h, d)
    pair_clips.wait()
    pair_p.wait()
    for r in (-1, 1):
        for c in range(CORES):
            @pl.when(inside(0, r))
            def _():
                last_copy(r, c).wait_send()

            @pl.when(inside(0, -r))
            def _():
                last_copy(r, c).wait_recv()

    for c in range(CORES):
        ref = cat_p.at[core if c == 0 else 1 - core]
        ref[...] = three(
            raw_p[c].astype(jnp.float32), lane_half(last_in[0, c]), lane_half(last_in[1, c])
        )
    begun = 0
    for a in range(TAPS):
        for b in range(TAPS):
            value = correlate(clip_pad, cat_p, a, b)
            for d in range(TAPS):
                g, t = place(a, b, d)
                for h in range(2):
                    p = h * GROUPS + g
                    block = tiles(value, h, d)
                    total[p, :, t] = block + total[p, :, t]
            done = (a * TAPS + b + 1) * TAPS
            while begun < GROUPS and done >= min((begun + 1) * SHARE, TAPS**3):
                for h in range(2):
                    start1(h * GROUPS + begun)
                begun += 1

    small_end(0)
    small_start(1)
    order = [h * GROUPS + g for g in range(GROUPS) for h in range(2)]
    for p in order:
        arrived(land1.at[p], recv1, p)
        for v, way in enumerate(routes[p]["ways"]):
            absorb(p, way["four"], 4, [(land1, (p, v))])
        start2(p)
    small_end(1)
    small_start(2)
    for p in order:
        arrived(land2.at[p], recv2, p)
        for v, way in enumerate(routes[p]["ways"]):
            absorb(p, way["two"], 2, [(land2, (p, v))])
        start3(p)
    small_end(2)
    small_start(3)

    z = here["z"]

    def copy4(p):
        return send(code4.at[p], land4.at[z], send4.at[0], recv4.at[0], chip(z=p))

    for p in order:
        send(land3.at[p], land3.at[p], send3.at[0], recv3.at[p], partner).wait_recv()
        absorb(p, routes[p]["unit"], 1, [(land3, (p, k)) for k in range(RING - 1)])

        @pl.when(z != p)
        def _():
            encode(p, routes[p]["unit"], 1, code4, (p,))
            copy4(p).start()

    unit = None
    for p in range(PARTS):
        term = jnp.where(z == p, routes[p]["unit"], 0)
        unit = term if unit is None else unit + term
    others = ring_peers("z", DEEP)
    seven = land4.at[pl.ds(0, DEEP - 1)]
    send(seven, seven, send4.at[0], recv4.at[0], partner).wait_recv()
    absorb(z, unit, 1, [(land4, (other,)) for other in others])
    encode(z, unit, 1, full, (z, core, unit))

    def zcopy(k, other):
        block = full.at[z, core, unit]
        return send(block, block, zsend.at[0], zrecv.at[z], chip(z=other))

    def zgot(p):
        block = full.at[p, core, routes[p]["unit"]]
        return send(block, block, zsend.at[0], zrecv.at[p], chip(z=p))

    for k, other in enumerate(others):
        zcopy(k, other).start()
    small_end(3)

    def qcopies(p):
        second = routes[p]["second"]
        block = full.at[p, core, routes[p]["unit"]]
        return [
            send(block, block, qsend.at[0], qrecv.at[p], chip(**{second: other}))
            for k, other in enumerate(ring_peers(second, RING))
        ]

    def far_copy(p, v):
        block = full.at[p, core, pl.ds(routes[p]["ways"][v]["two"], 2)]
        return send(block, block, far_send.at[0], far_recv.at[p], routes[p]["ways"][v]["far"])

    def near_copy(p, v):
        block = full.at[p, core, pl.ds(routes[p]["ways"][v]["four"], 4)]
        return send(block, block, near_send.at[0], near_recv.at[p], routes[p]["ways"][v]["near"])

    def core_start(p, second):
        for way in routes[p]["ways"]:
            block = full.at[p, core, pl.ds(way["other4"] if second else way["four"], 4)]
            send(block, block, core_send.at[0], core_recv.at[2 * p + second], partner).start()

    def units(count):
        return full.at[0, 0, pl.ds(0, count)]

    for p in order:
        @pl.when(z != p)
        def _():
            zgot(p).wait_recv()

        for copy in qcopies(p):
            copy.start()
    for p in order:
        three = full.at[p, core, pl.ds(0, RING - 1)]
        send(three, three, qsend.at[0], qrecv.at[p], partner).wait_recv()
        for v in range(WAYS):
            far_copy(p, v).start()
    def reveal(p, c, which):
        h, g = p // GROUPS, p % GROUPS
        taps = min(SHARE, TAPS**3 - g * SHARE)
        lane = pl.ds(pl.multiple_of(c * LANES, LANES), LANES)

        def one(base, k, carry):
            scale = full[p, c, base + k, SHARE].astype(jnp.float32) * (1.0 / (SPAN * math.log(2.0)))
            block = full[p, c, base + k, pl.ds(0, taps)].astype(jnp.float32)
            out_ref[pl.ds(g * SHARE, taps), h * UNITS + base + k, :, lane] = (
                jnp.log(block) * scale[None]
            )
            return carry

        for way in routes[p]["ways"]:
            lax.fori_loop(0, 4, functools.partial(one, way[which]), 0, unroll=UNROLL)

    for k, ref in enumerate((bias_out, head_out)):
        at = (len(small_targets)) * SUB + 2 * k
        ref[:, pl.ds(0, LANES)] = small_mine[pl.ds(at, 1)]
        ref[:, pl.ds(LANES, LANES)] = small_mine[pl.ds(at + 1, 1)]
    for p in order:
        arrived(units(4), far_recv, p)
        for v in range(WAYS):
            near_copy(p, v).start()
        core_start(p, 0)
    def reveal_far(p):
        arrived(units(8), core_recv, 2 * p)
        reveal(p, 1 - core, "four")

    for k, p in enumerate(order):
        reveal(p, core, "four")
        if k >= 2:
            reveal_far(order[k - 2])
        arrived(units(8), near_recv, p)
        core_start(p, 1)
        if k >= 1:
            reveal(order[k - 1], core, "other4")
    for p in order[-2:]:
        reveal_far(p)
    reveal(order[-1], core, "other4")
    for p in order:
        arrived(units(8), core_recv, 2 * p + 1)
        reveal(p, 1 - core, "other4")
    for block, sem in (
        (small_land, small_send), (code1, send1), (code2, send2), (code3, send3),
        (code4.at[pl.ds(0, DEEP - 1)], send4), (full.at[0, 0, pl.ds(0, DEEP - 1)], zsend),
        (full.at[pl.ds(0, 3), 0, pl.ds(0, 8)], qsend), (full.at[0], far_send),
        (full.at[pl.ds(0, 2)], near_send), (full.at[pl.ds(0, 4)], core_send),
    ):
        send(block, block, sem.at[0], sem.at[0], partner).wait_send()


def store_kernel(grad_ref, bias_ref, head_ref, grad_out, bias_out, head_out, sem):
    step = TAPS
    copies = [
        pltpu.make_async_copy(
            grad_ref.at[pl.ds(k * step, step)], grad_out.at[pl.ds(k * step, step)], sem.at[k]
        )
        for k in range(TAPS**3 // step)
    ]
    copies.append(pltpu.make_async_copy(bias_ref, bias_out, sem.at[TAPS**2]))
    copies.append(pltpu.make_async_copy(head_ref, head_out, sem.at[TAPS**2 + 1]))
    for copy in copies:
        copy.start()
    for copy in copies:
        copy.wait()


def per_device(sizes, clips, weight, bias, head):
    _, frames, _, cols, chans = clips.shape
    count = frames * cols
    lines = frames * RING
    dp, tm, rows = sizes
    assert (rows, dp * 2, tm // 4, chans) == (RING, RING, DEEP, 2 * LANES)
    dma = pltpu.SemaphoreType.DMA
    vmem = pl.BlockSpec(memory_space=pltpu.VMEM)
    hbm = pl.BlockSpec(memory_space=pltpu.HBM)
    row = jax.ShapeDtypeStruct((1, chans), jnp.float32)
    field = pltpu.VMEM((count, chans), jnp.float32)

    def pad(n):
        return pltpu.VMEM((n, RING + 2, cols // RING, chans), jnp.bfloat16)

    def coded(*lead, units):
        return pltpu.VMEM((*lead, units * SHARE + 1, SUB, LANES), jnp.bfloat16)

    cat = pltpu.VMEM((CORES, count, TAPS * LANES), jnp.bfloat16)
    stage = pltpu.VMEM((count, TAPS * LANES), jnp.bfloat16)
    smalls = 1 + 2 * (RING - 1) + DEEP - 1
    both = lambda n: [dma((n,)), dma((n,))]
    one = lambda n: [dma((1,)), dma((n,))]
    grad_weight, grad_bias, grad_head = pl.pallas_call(
        functools.partial(kernel, sizes),
        out_shape=(
            jax.ShapeDtypeStruct((TAPS**3, 2 * UNITS, SUB, chans), jnp.float32),
            row, row,
        ),
        in_specs=[hbm, hbm, hbm, hbm],
        out_specs=(vmem, vmem, vmem),
        scratch_shapes=[
            pltpu.VMEM((1, chans), jnp.float32), pltpu.VMEM((1, chans), jnp.float32),
            pltpu.VMEM((TAPS**3, chans, chans), jnp.bfloat16),
            pltpu.VMEM((frames, cols, chans), jnp.bfloat16),
            pad(2 * frames + 2), pad(frames + 2), pad(2 * frames + 2),
            pltpu.VMEM((TAPS, count, chans), jnp.float32),
            field, field,
            cat, cat, stage, pltpu.VMEM((count, LANES), jnp.bfloat16),
            pltpu.VMEM((CORES, count, LANES), jnp.bfloat16),
            pltpu.VMEM((RING, SUB, chans), jnp.bfloat16),
            pltpu.VMEM((3, RING, SUB, chans), jnp.bfloat16),
            pltpu.VMEM((2, 2, lines, chans), jnp.float32),
            pltpu.VMEM((TAPS, 2, 3, lines, chans), jnp.float32),
            pltpu.VMEM((2, lines, chans), jnp.float32),
            pltpu.VMEM((2, CORES, lines, chans), jnp.float32),
            pltpu.VMEM((PARTS, UNITS, SHARE, SUB, LANES), jnp.float32),
            coded(PARTS, WAYS, units=4), coded(PARTS, WAYS, units=4),
            coded(PARTS, WAYS, units=2), coded(PARTS, WAYS, units=2),
            coded(PARTS, RING - 1, units=1), coded(PARTS, RING - 1, units=1),
            coded(DEEP, units=1), coded(DEEP, units=1),
            coded(PARTS, CORES, UNITS, units=1),
            pltpu.VMEM((5 * SUB, LANES), jnp.float32),
            pltpu.VMEM((smalls * SUB, LANES), jnp.float32),
            dma((4,)), *both(6), *both(16), *both(4), *both(4), *one(PARTS), *one(PARTS), *one(PARTS), *one(1),
            *one(DEEP), *one(PARTS), *one(PARTS), *one(PARTS), *one(2 * PARTS), *one(4),
        ],
        compiler_params=pltpu.CompilerParams(
            collective_id=0, has_side_effects=True, vmem_limit_bytes=40 * 1024 * 1024
        ),
    )(
        *[
            pltpu.with_memory_space_constraint(value, pltpu.HBM)
            for value in (
                clips.reshape(frames, cols, chans), weight.reshape(TAPS**3, chans, chans),
                bias.reshape(1, chans), head.reshape(1, chans),
            )
        ]
    )
    grad_weight, grad_bias, grad_head = pl.pallas_call(
        store_kernel,
        out_shape=(
            jax.ShapeDtypeStruct((TAPS**3, 2 * UNITS, SUB, chans), jnp.float32), row, row,
        ),
        in_specs=[vmem, vmem, vmem],
        out_specs=(hbm, hbm, hbm),
        scratch_shapes=[dma((TAPS**2 + 2,))],
        compiler_params=pltpu.CompilerParams(vmem_limit_bytes=8 * 1024 * 1024),
    )(grad_weight, grad_bias, grad_head)
    grad_weight = grad_weight.reshape(TAPS, TAPS, TAPS, chans, chans)
    return grad_weight, grad_bias.reshape(chans), grad_head.reshape(chans)


def solution(mesh):
    sizes = tuple(mesh.shape[axis] for axis in ("dp", "tm", "rows"))
    return jax.shard_map(
        functools.partial(per_device, sizes),
        mesh=mesh,
        in_specs=(P("dp", "tm", "rows", None, None), P(), P(), P()),
        out_specs=(P(), P(), P()),
        check_vma=False,
    )
```

```python
import functools
import math

import jax
import jax.numpy as jnp
from jax import lax
from jax.experimental import pallas as pl
from jax.experimental.pallas import tpu as pltpu
from jax.sharding import PartitionSpec as P

penalty_weight = 0.01
MESH = pl.DeviceIdType.MESH
SUB = 8
LANES = 128
TAPS = 3
SPAN = 120.0
RING = 4
DEEP = 8
CORES = 2
GROUPS = 4
SHARE = 7
UNITS = 16
UNROLL = 4
WAYS = 2
PARTS = 2 * GROUPS


def flip(m):
    return m + 1 - 2 * lax.rem(m, 2)


def mirror(m):
    return RING - 1 - m


def kernel(
    sizes, clips_ref, weight_ref, bias_hbm, head_hbm,
    out_ref, bias_out, head_out,
    bias_ref, head_ref, w_ref, clips_vm, clip_pad, score_pad, grad_pad, acc, slope_ref, curve_ref,
    cat_s, cat_p, stage_s, stage_p, raw_p, side_out, side_in, edge_out, edge_in, last_out, last_in, total,
    code1, land1, code2, land2, code3, land3, code4, land4, full, small_mine, small_land,
    local_sem, turn_send, turn_recv, halo_send, halo_recv, last_send, last_recv,
    pair_send, pair_recv, send1, recv1, send2, recv2,
    send3, recv3, send4, recv4, zsend, zrecv, qsend, qrecv, near_send, near_recv,
    far_send, far_recv, core_send, core_recv, small_send, small_recv,
):
    dp, tm, rows = sizes
    frames, wide, chans = clips_ref.shape
    cols = wide // RING
    lines = frames * RING
    count = lines * cols
    half = count // 2
    me = {"dp": lax.axis_index("dp"), "tm": lax.axis_index("tm"), "rows": lax.axis_index("rows")}
    core = lax.rem(me["tm"], CORES)
    here = {
        "x": me["rows"],
        "y": 2 * me["dp"] + lax.rem(me["tm"] // 2, 2),
        "z": me["tm"] // 4,
        "c": core,
    }

    def device(**moved):
        place = dict(me, **moved)
        return (place["dp"], place["tm"], place["rows"])

    def chip(**moved):
        place = dict(here, **moved)
        return (
            place["y"] // 2,
            place["z"] * 4 + lax.rem(place["y"], 2) * 2 + place["c"],
            place["x"],
        )

    partner = chip(c=1 - core)

    def ring_peers(axis, size):
        return [lax.rem(here[axis] + step, size) for step in range(1, size)]

    weight_copy = pltpu.make_async_copy(weight_ref, w_ref, local_sem.at[0])
    weight_copy.start()
    shift = 2 * core
    clip_copy = pltpu.make_async_copy(clips_ref, clips_vm, local_sem.at[1])
    clip_copy.start()
    bias_copy = pltpu.make_async_copy(bias_hbm, bias_ref, local_sem.at[2])
    head_copy = pltpu.make_async_copy(head_hbm, head_ref, local_sem.at[3])
    bias_copy.start()
    head_copy.start()
    for pad, base in ((clip_pad, shift), (score_pad, 0), (grad_pad, shift)):
        pad[:, 0] = jnp.zeros((pad.shape[0], cols, chans), pad.dtype)
        pad[:, RING + 1] = jnp.zeros((pad.shape[0], cols, chans), pad.dtype)
        for at in (base, base + frames + 1):
            pad[at, pl.ds(1, RING)] = jnp.zeros((RING, cols, chans), pad.dtype)
    edge_in[...] = jnp.zeros_like(edge_in)
    side_in[...] = jnp.zeros_like(side_in)
    last_in[...] = jnp.zeros_like(last_in)

    moves = [(t, r) for t in (-1, 0, 1) for r in (-1, 0, 1) if (t, r) != (0, 0)]

    def inside(t, r):
        ok = None
        for axis, step, size in (("tm", t, tm), ("rows", r, rows)):
            if step:
                cond = me[axis] > 0 if step < 0 else me[axis] < size - 1
                ok = cond if ok is None else jnp.logical_and(ok, cond)
        return ok

    barrier = pltpu.get_barrier_semaphore()
    friends = [partner]
    friends += [chip(x=other) for other in ring_peers("x", RING)]
    friends += [chip(y=other) for other in ring_peers("y", RING)]
    friends += [chip(z=other) for other in ring_peers("z", DEEP)]
    for friend in friends:
        pl.semaphore_signal(barrier, inc=1, device_id=friend, device_id_type=MESH)
    expected = len(friends)
    for t in (-1, 1):
        expected = expected + RING * inside(t, 0).astype(jnp.int32)

        @pl.when(inside(t, 0))
        def _():
            for row in range(RING):
                pl.semaphore_signal(
                    barrier, inc=1, device_id=device(tm=me["tm"] + t, rows=row),
                    device_id_type=MESH,
                )
    pl.semaphore_wait(barrier, expected)

    def send(src, dst, send_sem, recv_sem, target):
        return pltpu.make_async_remote_copy(
            src_ref=src, dst_ref=dst, send_sem=send_sem, recv_sem=recv_sem,
            device_id=target, device_id_type=MESH,
        )

    def turn_copy(t, step):
        other = lax.rem(me["rows"] + step, RING)
        part = pl.ds(pl.multiple_of(other * cols, cols), cols)
        base = shift if t == 0 else 2 - shift
        src = {0: pl.ds(0, frames), 1: pl.ds(frames - 1, 1), -1: pl.ds(0, 1)}[t]
        dst = {0: pl.ds(base + 1, frames), 1: pl.ds(base, 1), -1: pl.ds(base + frames + 1, 1)}[t]
        return send(
            clips_vm.at[src, part], clip_pad.at[dst, 1 + me["rows"]],
            turn_send.at[1 + t], turn_recv.at[1 + t],
            device(tm=me["tm"] + t, rows=other),
        )

    def side_copy(t, step):
        other = lax.rem(me["rows"] + step, RING)
        return send(
            side_out.at[other], side_in.at[1 - t, me["rows"]],
            turn_send.at[4 + t], turn_recv.at[4 + t],
            device(tm=me["tm"] + t, rows=other),
        )

    def turn_start():
        for step in range(1, RING):
            turn_copy(0, step).start()
        for other in range(RING):
            at = other * cols
            lines_out = [
                clips_vm[f, c : c + 1].astype(jnp.float32) if 0 <= c < wide
                else jnp.zeros((1, chans), jnp.float32)
                for c in (at - 1, at + cols) for f in range(frames)
            ]
            lines_out.append(jnp.zeros((SUB - 2 * frames, chans), jnp.float32))
            side_out[other] = jnp.concatenate(lines_out, axis=0).astype(jnp.bfloat16)
        for step in range(1, RING):
            side_copy(0, step).start()
        for t in (-1, 1):
            @pl.when(inside(t, 0))
            def _():
                for step in range(RING):
                    turn_copy(t, step).start()
                    side_copy(t, step).start()
        side_in[1, me["rows"]] = side_out[me["rows"]]

    def turn_wait(level):
        if level:
            block = clip_pad.at[pl.ds(shift + 1, frames), pl.ds(1, RING - 1)]
            copy = send(block, block, turn_send.at[1], turn_recv.at[1], partner)
            copy.wait_recv()
            copy.wait_send()
            return
        block = side_in.at[1, pl.ds(0, RING - 1)]
        copy = send(block, block, turn_send.at[4], turn_recv.at[4], partner)
        copy.wait_recv()
        copy.wait_send()
        for t in (-1, 1):
            block, side = clip_pad.at[shift, pl.ds(1, RING)], side_in.at[0]
            copies = [
                send(block, block, turn_send.at[1 + t], turn_recv.at[1 + t], partner),
                send(side, side, turn_send.at[4 + t], turn_recv.at[4 + t], partner),
            ]

            @pl.when(inside(t, 0))
            def _():
                for copy in copies:
                    copy.wait_send()

            @pl.when(inside(-t, 0))
            def _():
                for copy in copies:
                    copy.wait_recv()

        line = lax.broadcasted_iota(jnp.int32, (lines, chans), 0)
        for k in range(3):
            blocks = [side_in[k, r].astype(jnp.float32) for r in range(RING)]
            for side in range(2):
                value = jnp.zeros((lines, chans), jnp.float32)
                for r in range(RING):
                    for f in range(frames):
                        at = side * frames + f
                        value = jnp.where(
                            line == f * RING + r,
                            jnp.broadcast_to(blocks[r][at : at + 1], (lines, chans)), value,
                        )
                edge_in[0, side, k] = value

    def halo_copy(which, pad, t, r):
        slot = (which - 1) * len(moves) + moves.index((t, r))
        target = device(tm=me["tm"] + t, rows=me["rows"] + r)
        sems = halo_send.at[slot], halo_recv.at[slot]
        if r != 0:
            side = 0 if r > 0 else 1
            return send(edge_out.at[which - 1, side], edge_in.at[which, side, 1 - t], *sems, target)
        pair = pad.shape[0] > frames + 2
        mine, base = (shift, 2 - shift) if pair else (0, 0)
        src = mine + frames if t > 0 else mine + 1
        dst = base if t > 0 else base + frames + 1
        return send(
            pad.at[src, pl.ds(1, RING)], pad.at[dst, pl.ds(1, RING)], *sems, target
        )

    def edge_rows(value):
        block = value.reshape(lines, cols, value.shape[-1])
        return block[:, cols - 1], block[:, 0]

    def halo_start(which, pad, value):
        for level in (True, False):
            if not level:
                for side, rows_out in enumerate(edge_rows(value)):
                    edge_out[which - 1, side] = rows_out
            for t, r in moves:
                if (r == 0) != level:
                    continue

                @pl.when(inside(t, r))
                def _():
                    halo_copy(which, pad, t, r).start()

    def halo_wait(which, pad):
        for t, r in moves:
            @pl.when(inside(t, r))
            def _():
                halo_copy(which, pad, t, r).wait_send()

            @pl.when(inside(-t, -r))
            def _():
                halo_copy(which, pad, t, r).wait_recv()

    def columns(value):
        return lax.rem(lax.broadcasted_iota(jnp.int32, value.shape, 0), cols)

    def spread(edge):
        return jnp.broadcast_to(edge[:, None, :], (lines, cols, edge.shape[-1])).reshape(count, -1)

    def earlier(value, edge):
        return jnp.where(columns(value) == 0, spread(edge), pltpu.roll(value, 1, 0))

    def later(value, edge):
        return jnp.where(columns(value) == cols - 1, spread(edge), pltpu.roll(value, count - 1, 0))

    def pair_frames(pad, slot):
        block = pad.at[pl.ds(4 * core, 2), pl.ds(1, RING)]
        return send(block, block, pair_send.at[slot], pair_recv.at[slot], partner)

    def edge_left(which):
        line = lax.broadcasted_iota(jnp.int32, (lines, chans), 0)
        row = lax.rem(line, RING)

        def piece(side, s, q):
            below, level, above = (edge_in[which, side, k] for k in range(3))
            if s == 1:
                value = level
            else:
                value = pltpu.roll(level, RING, 0)
                if s == 0:
                    value = jnp.where(line < RING, pltpu.roll(below, RING, 0), value)
                else:
                    value = jnp.where(line < RING, value, pltpu.roll(above, RING, 0))
            if q == 0:
                value = jnp.where(row == 0, 0.0, pltpu.roll(value, 1, 0))
            elif q == 2:
                value = jnp.where(row == RING - 1, 0.0, pltpu.roll(value, lines - 1, 0))
            return value

        return [
            jnp.concatenate([
                jnp.concatenate([piece(side, s, q) for q in range(TAPS)], axis=1)
                for side in range(2)
            ], axis=0).astype(jnp.bfloat16)
            for s in range(TAPS)
        ]

    def conv(which, pad, transpose, wait, ready):
        base = shift if pad.shape[0] > frames + 2 else 0

        def left(at, size):
            return jnp.concatenate([
                pad[pl.ds(base + at, size), pl.ds(q, RING)].reshape(size * half, chans)
                for q in range(TAPS)
            ], axis=1)

        def product(value, s, d):
            a = TAPS - 1 - s if transpose else s
            taps = [
                w_ref[(a * TAPS + (TAPS - 1 - q if transpose else q)) * TAPS + d]
                for q in range(TAPS)
            ]
            if transpose:
                return lax.dot_general(
                    value, jnp.concatenate(taps, axis=1), (((1,), (1,)), ((), ())),
                    preferred_element_type=jnp.float32,
                )
            return jnp.dot(
                value, jnp.concatenate(taps, axis=0), preferred_element_type=jnp.float32
            )

        own = left(1, frames)
        for d in range(TAPS):
            level = product(own, 1, d)
            acc[d, pl.ds(0, half)] = level[:half] + product(own[half:], 2, d)
            acc[d, pl.ds(half, half)] = level[half:] + product(own[:half], 0, d)
        wait()
        ready()
        edges = edge_left(which)
        below = jnp.concatenate([left(0, 1), edges[0]], axis=0)
        above = jnp.concatenate([left(frames + 1, 1), edges[2]], axis=0)
        sums, sides = [], []
        for d in range(TAPS):
            low, high = product(below, 0, d), product(above, 2, d)
            sums.append(jnp.concatenate([
                acc[d, pl.ds(0, half)] + low[:half], acc[d, pl.ds(half, half)] + high[:half]
            ], axis=0))
            sides.append(
                None if d == 1 else low[half:] + high[half:] + product(edges[1], 1, d)
            )
        d0, d2 = (2, 0) if transpose else (0, 2)
        return (
            earlier(sums[d0], sides[d0][:lines]) + sums[1] + later(sums[d2], sides[d2][lines:])
        )


    def lane_half(value, mine=True):
        low, high = value[:, :LANES], value[:, LANES:]
        return jnp.where(core == 0, low, high) if mine else jnp.where(core == 0, high, low)

    def three(value, before, after):
        return jnp.concatenate(
            [later(value, after), value, earlier(value, before)], axis=1
        ).astype(jnp.bfloat16)

    clip_copy.wait()
    turn_start()
    mine = pl.ds(pl.multiple_of(me["rows"] * cols, cols), cols)
    clip_pad[pl.ds(shift + 1, frames), 1 + me["rows"]] = clips_vm[:, mine]
    weight_copy.wait()
    bias_copy.wait()
    head_copy.wait()
    pair_clips, pair_grads = pair_frames(clip_pad, 0), pair_frames(grad_pad, 1)
    turn_wait(True)
    pre = conv(0, clip_pad, False, lambda: turn_wait(False), pair_clips.start) + bias_ref[...]
    sig = jax.nn.sigmoid(pre)
    slope = sig * (1.0 + pre * (1.0 - sig))
    slope_ref[...] = slope
    curve_ref[...] = sig * (1.0 - sig) * (2.0 + pre * (1.0 - 2.0 * sig))
    score = (head_ref[...] * slope).astype(jnp.bfloat16)
    score_pad[pl.ds(1, frames), pl.ds(1, RING)] = score.reshape(frames, RING, cols, chans)
    halo_start(1, score_pad, score.astype(jnp.float32))

    input_grad = conv(
        1, score_pad, True, lambda: halo_wait(1, score_pad), lambda: None
    ).astype(jnp.bfloat16)
    grad_pad[pl.ds(shift + 1, frames), pl.ds(1, RING)] = input_grad.reshape(
        frames, RING, cols, chans
    )
    halo_start(2, grad_pad, input_grad.astype(jnp.float32))

    value = score_pad[pl.ds(1, frames), pl.ds(1, RING)].reshape(count, chans).astype(jnp.float32)
    for mine, ref in ((True, cat_s.at[core]), (False, stage_s)):
        ref[...] = three(
            lane_half(value, mine),
            lane_half(edge_in[1, 0, 1], mine), lane_half(edge_in[1, 1, 1], mine),
        )
    pair_s = send(stage_s, cat_s.at[core], pair_send.at[2], pair_recv.at[2], partner)
    pair_s.start()

    back = penalty_weight * conv(
        2, grad_pad, False, lambda: halo_wait(2, grad_pad), pair_grads.start
    )
    pre_grad = back * head_ref[...] * curve_ref[...]
    value = pre_grad.astype(jnp.bfloat16).astype(jnp.float32)
    for side, rows_out in enumerate(edge_rows(value)):
        last_out[side] = rows_out
    def last_copy(r, c):
        side = 0 if r > 0 else 1
        other = core if c == 0 else 1 - core
        return send(
            last_out.at[side], last_in.at[side, c], last_send.at[side], last_recv.at[side],
            device(tm=me["tm"] - core + other, rows=me["rows"] + r),
        )

    for r in (-1, 1):
        @pl.when(inside(0, r))
        def _():
            for c in range(CORES):
                last_copy(r, c).start()

    stage_p[...] = lane_half(value, False).astype(jnp.bfloat16)
    pair_p = send(stage_p, raw_p.at[core], pair_send.at[3], pair_recv.at[3], partner)
    pair_p.start()
    raw_p[core] = lane_half(value).astype(jnp.bfloat16)

    small_mine[...] = jnp.zeros_like(small_mine)
    for k, value in enumerate((pre_grad, back * slope_ref[...])):
        whole = jnp.sum(value, axis=0, keepdims=True)
        small_mine[pl.ds(2 * k, 1)] = whole[:, :LANES]
        small_mine[pl.ds(2 * k + 1, 1)] = whole[:, LANES:]
    small_targets = [
        [partner],
        [chip(x=other) for other in ring_peers("x", RING)],
        [chip(y=other) for other in ring_peers("y", RING)],
        [chip(z=other) for other in ring_peers("z", DEEP)],
    ]
    smalls = []

    def small_start(level):
        at = sum(len(group) for group in small_targets[:level])
        copies = []
        for k, target in enumerate(small_targets[level]):
            copy = send(
                small_mine.at[pl.ds(level * SUB, SUB)], small_land.at[pl.ds((at + k) * SUB, SUB)],
                small_send.at[0], small_recv.at[level], target,
            )
            copy.start()
            copies.append(at + k)
        smalls.append(copies)

    def small_end(level):
        value = small_mine[pl.ds(level * SUB, SUB)]
        slots = smalls[level]
        lands = small_land.at[pl.ds(slots[0] * SUB, len(slots) * SUB)]
        send(lands, lands, small_send.at[0], small_recv.at[level], partner).wait_recv()
        for slot in slots:
            value = value + small_land[pl.ds(slot * SUB, SUB)]
        small_mine[pl.ds((level + 1) * SUB, SUB)] = value

    small_start(0)

    routes = []
    for p in range(PARTS):
        first, second = ("x", "y") if p < GROUPS else ("y", "x")
        m = here[first]
        ways = []
        for v in range(WAYS):
            if v == 0:
                near, bit1, far, bit2 = flip(m), lax.rem((m + 1) // 2, 2), mirror(m), m // 2
            else:
                near, bit1, far, bit2 = mirror(m), m // 2, flip(m), lax.rem(m, 2)
            four = 8 * v + 4 * bit1
            two = four + 2 * bit2
            ways.append(dict(
                near=chip(**{first: near}), far=chip(**{first: far}),
                four=four, other4=16 * v + 4 - four, two=two, other2=2 * four + 2 - two,
            ))
        routes.append(dict(ways=ways, second=second))

    def unit_of(p, n):
        low, high = (way["two"] for way in routes[p]["ways"])
        upper = n // 2
        return (1 - upper) * (low + n) + upper * (high + n - 2)

    for p, route in enumerate(routes):
        route["unit"] = unit_of(p, here[route["second"]])

    def encode(p, base, units, code, at):
        def peak(k, tops):
            for t in range(SHARE):
                tops = jnp.maximum(tops, jnp.abs(total[p, base + k, t]))
            return tops

        top = lax.fori_loop(
            0, units, peak, jnp.zeros((SUB, LANES), jnp.float32), unroll=min(units, UNROLL)
        )
        top = (top * 1.01 + 1e-30).astype(jnp.bfloat16)
        rate = SPAN / top.astype(jnp.float32)
        code[(*at, units * SHARE)] = top

        def fill(k, carry):
            code[(*at, pl.ds(k * SHARE, SHARE))] = jnp.exp2(
                total[p, base + k] * rate[None]
            ).astype(jnp.bfloat16)
            return carry

        lax.fori_loop(0, units, fill, 0, unroll=min(units, UNROLL))

    def absorb(p, base, units, lands):
        scales = [
            land[(*at, units * SHARE)].astype(jnp.float32) * (1.0 / (SPAN * math.log(2.0)))
            for land, at in lands
        ]

        def add(k, carry):
            value = total[p, base + k]
            for (land, at), scale in zip(lands, scales):
                block = land[(*at, pl.ds(k * SHARE, SHARE))].astype(jnp.float32)
                value = value + jnp.log(block) * scale[None]
            total[p, base + k] = value
            return carry

        lax.fori_loop(0, units, add, 0, unroll=min(units, UNROLL))

    def halving(p, v, code, land, send_sem, recv_sem, to):
        return send(
            code.at[p, v], land.at[p, v], send_sem.at[0], recv_sem.at[p % GROUPS], routes[p]["ways"][v][to]
        )

    def arrived(block, recv_sem, slot):
        send(block, block, send1.at[0], recv_sem.at[slot], partner).wait_recv()

    def copy3(p):
        second = routes[p]["second"]
        return [
            send(
                code3.at[p, k], land3.at[p, k], send3.at[0], recv3.at[p % GROUPS],
                chip(**{second: other}),
            )
            for k, other in enumerate(ring_peers(second, RING))
        ]

    def start1(p):
        for v, way in enumerate(routes[p]["ways"]):
            encode(p, way["other4"], 4, code1, (p, v))
            halving(p, v, code1, land1, send1, recv1, "near").start()

    def start2(p):
        for v, way in enumerate(routes[p]["ways"]):
            encode(p, way["other2"], 2, code2, (p, v))
            halving(p, v, code2, land2, send2, recv2, "far").start()

    def start3(p):
        second = routes[p]["second"]
        for k, (copy, other) in enumerate(zip(copy3(p), ring_peers(second, RING))):
            encode(p, unit_of(p, other), 1, code3, (p, k))
            copy.start()

    def correlate(pad, cat, a, b):
        left = pad[a : a + 2 * frames, b : b + RING].reshape(2 * count, chans)
        right = cat[...].reshape(2 * count, cat.shape[-1])
        return lax.dot_general(
            left, right, (((0,), (0,)), ((), ())), preferred_element_type=jnp.float32
        )

    def tiles(value, h, d):
        block = value[h * UNITS * SUB : (h + 1) * UNITS * SUB, d * LANES : (d + 1) * LANES]
        return block.reshape(UNITS, SUB, LANES)

    def place(a, b, d):
        tap = (a * TAPS + b) * TAPS + d
        return tap // SHARE, tap % SHARE

    for h in range(2):
        total[h * GROUPS + GROUPS - 1, :, SHARE - 1] = jnp.zeros((UNITS, SUB, LANES), jnp.float32)
    pair_s.wait()
    pair_grads.wait()
    for a in range(TAPS):
        if a == 1:
            pair_clips.wait()
            pair_p.wait()
        for b in range(TAPS):
            value = penalty_weight * correlate(grad_pad, cat_s, a, b)
            level = correlate(clip_pad, raw_p, a, b) if a > 0 else None
            for d in range(TAPS):
                g, t = place(a, b, d)
                for h in range(2):
                    block = tiles(value, h, d)
                    if a > 0 and d == 1:
                        block = block + tiles(level, h, 0)
                    total[h * GROUPS + g, :, t] = block
    for b in range(TAPS):
        level = correlate(clip_pad, raw_p, 0, b)
        g, t = place(0, b, 1)
        for h in range(2):
            total[h * GROUPS + g, :, t] = total[h * GROUPS + g, :, t] + tiles(level, h, 0)
    for r in (-1, 1):
        side = 0 if r > 0 else 1
        both = last_in.at[side]
        copy = send(both, both, last_send.at[side], last_recv.at[side], partner)

        @pl.when(inside(0, r))
        def _():
            copy.wait_send()

        @pl.when(inside(0, -r))
        def _():
            copy.wait_recv()

    for c in range(CORES):
        at = core if c == 0 else 1 - core
        value = raw_p[at].astype(jnp.float32)
        cat_p[at] = jnp.concatenate([
            later(value, lane_half(last_in[1, c])), earlier(value, lane_half(last_in[0, c]))
        ], axis=1).astype(jnp.bfloat16)
    begun = 0
    for a in range(TAPS):
        for b in range(TAPS):
            value = correlate(clip_pad, cat_p, a, b)
            for d in (0, 2):
                g, t = place(a, b, d)
                for h in range(2):
                    p = h * GROUPS + g
                    block = tiles(value, h, d // 2)
                    total[p, :, t] = block + total[p, :, t]
            done = (a * TAPS + b + 1) * TAPS
            while begun < GROUPS and done >= min((begun + 1) * SHARE, TAPS**3):
                for h in range(2):
                    start1(h * GROUPS + begun)
                begun += 1

    small_end(0)
    small_start(1)
    order = [h * GROUPS + g for g in range(GROUPS) for h in range(2)]
    for p in order:
        if p < GROUPS:
            arrived(land1.at[pl.ds(0, 2)], recv1, p)
        for v, way in enumerate(routes[p]["ways"]):
            absorb(p, way["four"], 4, [(land1, (p, v))])
        start2(p)
    small_end(1)
    small_start(2)
    for p in order:
        if p < GROUPS:
            arrived(land2.at[pl.ds(0, 2)], recv2, p)
        for v, way in enumerate(routes[p]["ways"]):
            absorb(p, way["two"], 2, [(land2, (p, v))])
        start3(p)
    small_end(2)
    small_start(3)

    z = here["z"]

    def copy4(p):
        return send(code4.at[p], land4.at[z], send4.at[0], recv4.at[0], chip(z=p))

    for p in order:
        if p < GROUPS:
            arrived(land3.at[pl.ds(0, 2)], recv3, p)
        absorb(p, routes[p]["unit"], 1, [(land3, (p, k)) for k in range(RING - 1)])

        @pl.when(z != p)
        def _():
            encode(p, routes[p]["unit"], 1, code4, (p,))
            copy4(p).start()

    unit = None
    for p in range(PARTS):
        term = jnp.where(z == p, routes[p]["unit"], 0)
        unit = term if unit is None else unit + term
    others = ring_peers("z", DEEP)
    seven = land4.at[pl.ds(0, DEEP - 1)]
    send(seven, seven, send4.at[0], recv4.at[0], partner).wait_recv()
    absorb(z, unit, 1, [(land4, (other,)) for other in others])
    encode(z, unit, 1, full, (z, core, unit))

    def zcopy(k, other):
        block = full.at[z, core, unit]
        return send(block, block, zsend.at[0], zrecv.at[z], chip(z=other))

    def zgot(p):
        block = full.at[p, core, routes[p]["unit"]]
        return send(block, block, zsend.at[0], zrecv.at[p], chip(z=p))

    for k, other in enumerate(others):
        zcopy(k, other).start()
    small_end(3)

    def qcopies(p):
        second = routes[p]["second"]
        block = full.at[p, core, routes[p]["unit"]]
        return [
            send(block, block, qsend.at[0], qrecv.at[p % GROUPS], chip(**{second: other}))
            for k, other in enumerate(ring_peers(second, RING))
        ]

    def far_copy(p, v):
        block = full.at[p, core, pl.ds(routes[p]["ways"][v]["two"], 2)]
        return send(block, block, far_send.at[0], far_recv.at[p % GROUPS], routes[p]["ways"][v]["far"])

    def near_copy(p, v):
        block = full.at[p, core, pl.ds(routes[p]["ways"][v]["four"], 4)]
        return send(block, block, near_send.at[0], near_recv.at[p % GROUPS], routes[p]["ways"][v]["near"])

    def core_start(p, second):
        for way in routes[p]["ways"]:
            block = full.at[p, core, pl.ds(way["other4"] if second else way["four"], 4)]
            send(block, block, core_send.at[0], core_recv.at[2 * (p % GROUPS) + second], partner).start()

    def units(count):
        return full.at[0, 0, pl.ds(0, count)]

    for p in order:
        @pl.when(z != p)
        def _():
            zgot(p).wait_recv()

        for copy in qcopies(p):
            copy.start()
    for p in order:
        if p < GROUPS:
            arrived(units(2 * (RING - 1)), qrecv, p)
        for v in range(WAYS):
            far_copy(p, v).start()
    def reveal(p, c, which):
        h, g = p // GROUPS, p % GROUPS
        taps = min(SHARE, TAPS**3 - g * SHARE)
        lane = pl.ds(pl.multiple_of(c * LANES, LANES), LANES)

        def one(base, k, carry):
            scale = full[p, c, base + k, SHARE].astype(jnp.float32) * (1.0 / (SPAN * math.log(2.0)))
            block = full[p, c, base + k, pl.ds(0, taps)].astype(jnp.float32)
            out_ref[pl.ds(g * SHARE, taps), h * UNITS + base + k, :, lane] = (
                jnp.log(block) * scale[None]
            )
            return carry

        for way in routes[p]["ways"]:
            lax.fori_loop(0, 4, functools.partial(one, way[which]), 0, unroll=UNROLL)

    for k, ref in enumerate((bias_out, head_out)):
        at = (len(small_targets)) * SUB + 2 * k
        ref[:, pl.ds(0, LANES)] = small_mine[pl.ds(at, 1)]
        ref[:, pl.ds(LANES, LANES)] = small_mine[pl.ds(at + 1, 1)]
    def reveal_core(p, second):
        if p < GROUPS:
            arrived(units(16), core_recv, 2 * p + second)
        reveal(p, 1 - core, "other4" if second else "four")

    for k, p in enumerate(order):
        if p < GROUPS:
            arrived(units(8), far_recv, p)
        for v in range(WAYS):
            near_copy(p, v).start()
        core_start(p, 0)
        if k >= 1:
            reveal(order[k - 1], core, "four")
    reveal(order[-1], core, "four")
    for k, p in enumerate(order):
        reveal_core(p, 0)
        if p < GROUPS:
            arrived(units(16), near_recv, p)
        core_start(p, 1)
        if k >= 1:
            reveal(order[k - 1], core, "other4")
        if k >= 4:
            reveal_core(order[k - 4], 1)
    reveal(order[-1], core, "other4")
    for p in order[-4:]:
        reveal_core(p, 1)
    for block, sem in (
        (small_land, small_send), (code1, send1), (code2, send2), (code3, send3),
        (code4.at[pl.ds(0, DEEP - 1)], send4), (full.at[0, 0, pl.ds(0, DEEP - 1)], zsend),
        (full.at[pl.ds(0, 3), 0, pl.ds(0, 8)], qsend), (full.at[0], far_send),
        (full.at[pl.ds(0, 2)], near_send), (full.at[pl.ds(0, 4)], core_send),
    ):
        send(block, block, sem.at[0], sem.at[0], partner).wait_send()


def store_kernel(grad_ref, bias_ref, head_ref, grad_out, bias_out, head_out, sem):
    step = TAPS
    copies = [
        pltpu.make_async_copy(
            grad_ref.at[pl.ds(k * step, step)], grad_out.at[pl.ds(k * step, step)], sem.at[k]
        )
        for k in range(TAPS**3 // step)
    ]
    copies.append(pltpu.make_async_copy(bias_ref, bias_out, sem.at[TAPS**2]))
    copies.append(pltpu.make_async_copy(head_ref, head_out, sem.at[TAPS**2 + 1]))
    for copy in copies:
        copy.start()
    for copy in copies:
        copy.wait()


def per_device(sizes, clips, weight, bias, head):
    _, frames, _, cols, chans = clips.shape
    count = frames * cols
    lines = frames * RING
    dp, tm, rows = sizes
    assert (rows, dp * 2, tm // 4, chans) == (RING, RING, DEEP, 2 * LANES)
    dma = pltpu.SemaphoreType.DMA
    vmem = pl.BlockSpec(memory_space=pltpu.VMEM)
    hbm = pl.BlockSpec(memory_space=pltpu.HBM)
    row = jax.ShapeDtypeStruct((1, chans), jnp.float32)
    field = pltpu.VMEM((count, chans), jnp.float32)

    def pad(n):
        return pltpu.VMEM((n, RING + 2, cols // RING, chans), jnp.bfloat16)

    def coded(*lead, units):
        return pltpu.VMEM((*lead, units * SHARE + 1, SUB, LANES), jnp.bfloat16)

    cat = pltpu.VMEM((CORES, count, TAPS * LANES), jnp.bfloat16)
    stage = pltpu.VMEM((count, TAPS * LANES), jnp.bfloat16)
    smalls = 1 + 2 * (RING - 1) + DEEP - 1
    both = lambda n: [dma((n,)), dma((n,))]
    one = lambda n: [dma((1,)), dma((n,))]
    grad_weight, grad_bias, grad_head = pl.pallas_call(
        functools.partial(kernel, sizes),
        out_shape=(
            jax.ShapeDtypeStruct((TAPS**3, 2 * UNITS, SUB, chans), jnp.float32),
            row, row,
        ),
        in_specs=[hbm, hbm, hbm, hbm],
        out_specs=(vmem, vmem, vmem),
        scratch_shapes=[
            pltpu.VMEM((1, chans), jnp.float32), pltpu.VMEM((1, chans), jnp.float32),
            pltpu.VMEM((TAPS**3, chans, chans), jnp.bfloat16),
            pltpu.VMEM((frames, cols, chans), jnp.bfloat16),
            pad(2 * frames + 2), pad(frames + 2), pad(2 * frames + 2),
            pltpu.VMEM((TAPS, count, chans), jnp.float32),
            field, field,
            cat, pltpu.VMEM((CORES, count, 2 * LANES), jnp.bfloat16), stage, pltpu.VMEM((count, LANES), jnp.bfloat16),
            pltpu.VMEM((CORES, count, LANES), jnp.bfloat16),
            pltpu.VMEM((RING, SUB, chans), jnp.bfloat16),
            pltpu.VMEM((3, RING, SUB, chans), jnp.bfloat16),
            pltpu.VMEM((2, 2, lines, chans), jnp.float32),
            pltpu.VMEM((TAPS, 2, 3, lines, chans), jnp.float32),
            pltpu.VMEM((2, lines, chans), jnp.float32),
            pltpu.VMEM((2, CORES, lines, chans), jnp.float32),
            pltpu.VMEM((PARTS, UNITS, SHARE, SUB, LANES), jnp.float32),
            coded(PARTS, WAYS, units=4), coded(PARTS, WAYS, units=4),
            coded(PARTS, WAYS, units=2), coded(PARTS, WAYS, units=2),
            coded(PARTS, RING - 1, units=1), coded(PARTS, RING - 1, units=1),
            coded(DEEP, units=1), coded(DEEP, units=1),
            coded(PARTS, CORES, UNITS, units=1),
            pltpu.VMEM((5 * SUB, LANES), jnp.float32),
            pltpu.VMEM((smalls * SUB, LANES), jnp.float32),
            dma((4,)), *both(6), *both(16), *both(2), *both(4),
            *one(GROUPS), *one(GROUPS), *one(GROUPS), *one(1),
            *one(DEEP), *one(GROUPS), *one(GROUPS), *one(GROUPS), *one(2 * GROUPS), *one(4),
        ],
        compiler_params=pltpu.CompilerParams(
            collective_id=0, has_side_effects=True, vmem_limit_bytes=40 * 1024 * 1024
        ),
    )(
        *[
            pltpu.with_memory_space_constraint(value, pltpu.HBM)
            for value in (
                clips.reshape(frames, cols, chans), weight.reshape(TAPS**3, chans, chans),
                bias.reshape(1, chans), head.reshape(1, chans),
            )
        ]
    )
    grad_weight, grad_bias, grad_head = pl.pallas_call(
        store_kernel,
        out_shape=(
            jax.ShapeDtypeStruct((TAPS**3, 2 * UNITS, SUB, chans), jnp.float32), row, row,
        ),
        in_specs=[vmem, vmem, vmem],
        out_specs=(hbm, hbm, hbm),
        scratch_shapes=[dma((TAPS**2 + 2,))],
        compiler_params=pltpu.CompilerParams(vmem_limit_bytes=8 * 1024 * 1024),
    )(grad_weight, grad_bias, grad_head)
    grad_weight = grad_weight.reshape(TAPS, TAPS, TAPS, chans, chans)
    return grad_weight, grad_bias.reshape(chans), grad_head.reshape(chans)


def solution(mesh):
    sizes = tuple(mesh.shape[axis] for axis in ("dp", "tm", "rows"))
    return jax.shard_map(
        functools.partial(per_device, sizes),
        mesh=mesh,
        in_specs=(P("dp", "tm", "rows", None, None), P(), P(), P()),
        out_specs=(P(), P(), P()),
        check_vma=False,
    )
```

```python
import functools
import math

import jax
import jax.numpy as jnp
from jax import lax
from jax.experimental import pallas as pl
from jax.experimental.pallas import tpu as pltpu
from jax.sharding import PartitionSpec as P

penalty_weight = 0.01
MESH = pl.DeviceIdType.MESH
SUB = 8
LANES = 128
TAPS = 3
SPAN = 120.0
RING = 4
DEEP = 8
CORES = 2
GROUPS = 4
SHARE = 7
UNITS = 16
UNROLL = 4
WAYS = 2
PARTS = 2 * GROUPS


def flip(m):
    return m + 1 - 2 * lax.rem(m, 2)


def mirror(m):
    return RING - 1 - m


def kernel(
    sizes, clips_ref, weight_ref, bias_hbm, head_hbm,
    out_ref, bias_out, head_out,
    bias_ref, head_ref, w_ref, clips_vm, clip_pad, score_pad, grad_pad, acc, slope_ref, curve_ref,
    cat_s, cat_p, stage_s, stage_p, raw_p, side_out, side_in, edge_out, edge_in, last_out, last_in, total,
    code1, land1, code2, land2, code3, land3, code4, land4, full, small_mine, small_land,
    local_sem, turn_send, turn_recv, halo_send, halo_recv, last_send, last_recv,
    pair_send, pair_recv, send1, recv1, send2, recv2,
    send3, recv3, send4, recv4, zsend, zrecv, qsend, qrecv, near_send, near_recv,
    far_send, far_recv, core_send, core_recv, small_send, small_recv,
):
    dp, tm, rows = sizes
    frames, wide, chans = clips_ref.shape
    cols = wide // RING
    lines = frames * RING
    count = lines * cols
    half = count // 2
    me = {"dp": lax.axis_index("dp"), "tm": lax.axis_index("tm"), "rows": lax.axis_index("rows")}
    core = lax.rem(me["tm"], CORES)
    here = {
        "x": me["rows"],
        "y": 2 * me["dp"] + lax.rem(me["tm"] // 2, 2),
        "z": me["tm"] // 4,
        "c": core,
    }

    def device(**moved):
        place = dict(me, **moved)
        return (place["dp"], place["tm"], place["rows"])

    def chip(**moved):
        place = dict(here, **moved)
        return (
            place["y"] // 2,
            place["z"] * 4 + lax.rem(place["y"], 2) * 2 + place["c"],
            place["x"],
        )

    partner = chip(c=1 - core)

    def ring_peers(axis, size):
        return [lax.rem(here[axis] + step, size) for step in range(1, size)]

    weight_copy = pltpu.make_async_copy(weight_ref, w_ref, local_sem.at[0])
    weight_copy.start()
    shift = 2 * core
    clip_copy = pltpu.make_async_copy(clips_ref, clips_vm, local_sem.at[1])
    clip_copy.start()
    bias_copy = pltpu.make_async_copy(bias_hbm, bias_ref, local_sem.at[2])
    head_copy = pltpu.make_async_copy(head_hbm, head_ref, local_sem.at[3])
    bias_copy.start()
    head_copy.start()
    for pad, base in ((clip_pad, shift), (score_pad, 0), (grad_pad, shift)):
        pad[:, 0] = jnp.zeros((pad.shape[0], cols, chans), pad.dtype)
        pad[:, RING + 1] = jnp.zeros((pad.shape[0], cols, chans), pad.dtype)
        for at in (base, base + frames + 1):
            pad[at, pl.ds(1, RING)] = jnp.zeros((RING, cols, chans), pad.dtype)
    edge_in[...] = jnp.zeros_like(edge_in)
    side_in[...] = jnp.zeros_like(side_in)
    last_in[...] = jnp.zeros_like(last_in)

    moves = [(t, r) for t in (-1, 0, 1) for r in (-1, 0, 1) if (t, r) != (0, 0)]

    def inside(t, r):
        ok = None
        for axis, step, size in (("tm", t, tm), ("rows", r, rows)):
            if step:
                cond = me[axis] > 0 if step < 0 else me[axis] < size - 1
                ok = cond if ok is None else jnp.logical_and(ok, cond)
        return ok

    barrier = pltpu.get_barrier_semaphore()
    friends = [partner]
    friends += [chip(x=other) for other in ring_peers("x", RING)]
    friends += [chip(y=other) for other in ring_peers("y", RING)]
    friends += [chip(z=other) for other in ring_peers("z", DEEP)]
    for friend in friends:
        pl.semaphore_signal(barrier, inc=1, device_id=friend, device_id_type=MESH)
    expected = len(friends)
    for t in (-1, 1):
        expected = expected + RING * inside(t, 0).astype(jnp.int32)

        @pl.when(inside(t, 0))
        def _():
            for row in range(RING):
                pl.semaphore_signal(
                    barrier, inc=1, device_id=device(tm=me["tm"] + t, rows=row),
                    device_id_type=MESH,
                )
    pl.semaphore_wait(barrier, expected)

    def send(src, dst, send_sem, recv_sem, target):
        return pltpu.make_async_remote_copy(
            src_ref=src, dst_ref=dst, send_sem=send_sem, recv_sem=recv_sem,
            device_id=target, device_id_type=MESH,
        )

    def turn_copy(t, step):
        other = lax.rem(me["rows"] + step, RING)
        part = pl.ds(pl.multiple_of(other * cols, cols), cols)
        base = shift if t == 0 else 2 - shift
        src = {0: pl.ds(0, frames), 1: pl.ds(frames - 1, 1), -1: pl.ds(0, 1)}[t]
        dst = {0: pl.ds(base + 1, frames), 1: pl.ds(base, 1), -1: pl.ds(base + frames + 1, 1)}[t]
        return send(
            clips_vm.at[src, part], clip_pad.at[dst, 1 + me["rows"]],
            turn_send.at[1 + t], turn_recv.at[1 + t],
            device(tm=me["tm"] + t, rows=other),
        )

    def side_copy(t, step):
        other = lax.rem(me["rows"] + step, RING)
        return send(
            side_out.at[other], side_in.at[1 - t, me["rows"]],
            turn_send.at[4 + t], turn_recv.at[4 + t],
            device(tm=me["tm"] + t, rows=other),
        )

    def turn_start():
        for step in range(1, RING):
            turn_copy(0, step).start()
        for other in range(RING):
            at = other * cols
            lines_out = [
                clips_vm[f, c : c + 1].astype(jnp.float32) if 0 <= c < wide
                else jnp.zeros((1, chans), jnp.float32)
                for c in (at - 1, at + cols) for f in range(frames)
            ]
            lines_out.append(jnp.zeros((SUB - 2 * frames, chans), jnp.float32))
            side_out[other] = jnp.concatenate(lines_out, axis=0).astype(jnp.bfloat16)
        for step in range(1, RING):
            side_copy(0, step).start()
        for t in (-1, 1):
            @pl.when(inside(t, 0))
            def _():
                for step in range(RING):
                    turn_copy(t, step).start()
                    side_copy(t, step).start()
        side_in[1, me["rows"]] = side_out[me["rows"]]

    def turn_wait(level):
        if level:
            block = clip_pad.at[pl.ds(shift + 1, frames), pl.ds(1, RING - 1)]
            copy = send(block, block, turn_send.at[1], turn_recv.at[1], partner)
            copy.wait_recv()
            copy.wait_send()
            return
        block = side_in.at[1, pl.ds(0, RING - 1)]
        copy = send(block, block, turn_send.at[4], turn_recv.at[4], partner)
        copy.wait_recv()
        copy.wait_send()
        for t in (-1, 1):
            block, side = clip_pad.at[shift, pl.ds(1, RING)], side_in.at[0]
            copies = [
                send(block, block, turn_send.at[1 + t], turn_recv.at[1 + t], partner),
                send(side, side, turn_send.at[4 + t], turn_recv.at[4 + t], partner),
            ]

            @pl.when(inside(t, 0))
            def _():
                for copy in copies:
                    copy.wait_send()

            @pl.when(inside(-t, 0))
            def _():
                for copy in copies:
                    copy.wait_recv()

        line = lax.broadcasted_iota(jnp.int32, (lines, chans), 0)
        for k in range(3):
            blocks = [side_in[k, r].astype(jnp.float32) for r in range(RING)]
            for side in range(2):
                value = jnp.zeros((lines, chans), jnp.float32)
                for r in range(RING):
                    for f in range(frames):
                        at = side * frames + f
                        value = jnp.where(
                            line == f * RING + r,
                            jnp.broadcast_to(blocks[r][at : at + 1], (lines, chans)), value,
                        )
                edge_in[0, side, k] = value

    def halo_copy(which, pad, t, r):
        slot = (which - 1) * len(moves) + moves.index((t, r))
        target = device(tm=me["tm"] + t, rows=me["rows"] + r)
        sems = halo_send.at[slot], halo_recv.at[slot]
        if r != 0:
            side = 0 if r > 0 else 1
            return send(edge_out.at[which - 1, side], edge_in.at[which, side, 1 - t], *sems, target)
        pair = pad.shape[0] > frames + 2
        mine, base = (shift, 2 - shift) if pair else (0, 0)
        src = mine + frames if t > 0 else mine + 1
        dst = base if t > 0 else base + frames + 1
        return send(
            pad.at[src, pl.ds(1, RING)], pad.at[dst, pl.ds(1, RING)], *sems, target
        )

    def edge_rows(value):
        block = value.reshape(lines, cols, value.shape[-1])
        return block[:, cols - 1], block[:, 0]

    def halo_start(which, pad, value):
        for level in (True, False):
            if not level:
                for side, rows_out in enumerate(edge_rows(value)):
                    edge_out[which - 1, side] = rows_out
            for t, r in moves:
                if (r == 0) != level:
                    continue

                @pl.when(inside(t, r))
                def _():
                    halo_copy(which, pad, t, r).start()

    def halo_wait(which, pad):
        for t, r in moves:
            @pl.when(inside(t, r))
            def _():
                halo_copy(which, pad, t, r).wait_send()

            @pl.when(inside(-t, -r))
            def _():
                halo_copy(which, pad, t, r).wait_recv()

    def columns(value):
        return lax.rem(lax.broadcasted_iota(jnp.int32, value.shape, 0), cols)

    def spread(edge):
        return jnp.broadcast_to(edge[:, None, :], (lines, cols, edge.shape[-1])).reshape(count, -1)

    def earlier(value, edge):
        return jnp.where(columns(value) == 0, spread(edge), pltpu.roll(value, 1, 0))

    def later(value, edge):
        return jnp.where(columns(value) == cols - 1, spread(edge), pltpu.roll(value, count - 1, 0))

    def pair_frames(pad, slot):
        block = pad.at[pl.ds(4 * core, 2), pl.ds(1, RING)]
        return send(block, block, pair_send.at[slot], pair_recv.at[slot], partner)

    def edge_left(which):
        line = lax.broadcasted_iota(jnp.int32, (lines, chans), 0)
        row = lax.rem(line, RING)

        def piece(side, s, q):
            below, level, above = (edge_in[which, side, k] for k in range(3))
            if s == 1:
                value = level
            else:
                value = pltpu.roll(level, RING, 0)
                if s == 0:
                    value = jnp.where(line < RING, pltpu.roll(below, RING, 0), value)
                else:
                    value = jnp.where(line < RING, value, pltpu.roll(above, RING, 0))
            if q == 0:
                value = jnp.where(row == 0, 0.0, pltpu.roll(value, 1, 0))
            elif q == 2:
                value = jnp.where(row == RING - 1, 0.0, pltpu.roll(value, lines - 1, 0))
            return value

        return [
            jnp.concatenate([
                jnp.concatenate([piece(side, s, q) for q in range(TAPS)], axis=1)
                for side in range(2)
            ], axis=0).astype(jnp.bfloat16)
            for s in range(TAPS)
        ]

    def conv(which, pad, transpose, wait, ready):
        base = shift if pad.shape[0] > frames + 2 else 0

        def left(at, size):
            return jnp.concatenate([
                pad[pl.ds(base + at, size), pl.ds(q, RING)].reshape(size * half, chans)
                for q in range(TAPS)
            ], axis=1)

        def product(value, s, d):
            a = TAPS - 1 - s if transpose else s
            taps = [
                w_ref[(a * TAPS + (TAPS - 1 - q if transpose else q)) * TAPS + d]
                for q in range(TAPS)
            ]
            if transpose:
                return lax.dot_general(
                    value, jnp.concatenate(taps, axis=1), (((1,), (1,)), ((), ())),
                    preferred_element_type=jnp.float32,
                )
            return jnp.dot(
                value, jnp.concatenate(taps, axis=0), preferred_element_type=jnp.float32
            )

        own = left(1, frames)
        for d in range(TAPS):
            level = product(own, 1, d)
            acc[d, pl.ds(0, half)] = level[:half] + product(own[half:], 2, d)
            acc[d, pl.ds(half, half)] = level[half:] + product(own[:half], 0, d)
        wait()
        ready()
        edges = edge_left(which)
        below = jnp.concatenate([left(0, 1), edges[0]], axis=0)
        above = jnp.concatenate([left(frames + 1, 1), edges[2]], axis=0)
        sums, sides = [], []
        for d in range(TAPS):
            low, high = product(below, 0, d), product(above, 2, d)
            sums.append(jnp.concatenate([
                acc[d, pl.ds(0, half)] + low[:half], acc[d, pl.ds(half, half)] + high[:half]
            ], axis=0))
            sides.append(
                None if d == 1 else low[half:] + high[half:] + product(edges[1], 1, d)
            )
        d0, d2 = (2, 0) if transpose else (0, 2)
        return (
            earlier(sums[d0], sides[d0][:lines]) + sums[1] + later(sums[d2], sides[d2][lines:])
        )


    def lane_half(value, mine=True):
        low, high = value[:, :LANES], value[:, LANES:]
        return jnp.where(core == 0, low, high) if mine else jnp.where(core == 0, high, low)

    def three(value, before, after):
        return jnp.concatenate(
            [later(value, after), value, earlier(value, before)], axis=1
        ).astype(jnp.bfloat16)

    clip_copy.wait()
    turn_start()
    mine = pl.ds(pl.multiple_of(me["rows"] * cols, cols), cols)
    clip_pad[pl.ds(shift + 1, frames), 1 + me["rows"]] = clips_vm[:, mine]
    weight_copy.wait()
    bias_copy.wait()
    head_copy.wait()
    pair_clips, pair_grads = pair_frames(clip_pad, 0), pair_frames(grad_pad, 1)
    turn_wait(True)
    pre = conv(0, clip_pad, False, lambda: turn_wait(False), pair_clips.start) + bias_ref[...]
    sig = jax.nn.sigmoid(pre)
    slope = sig * (1.0 + pre * (1.0 - sig))
    slope_ref[...] = slope
    curve_ref[...] = sig * (1.0 - sig) * (2.0 + pre * (1.0 - 2.0 * sig))
    score = (head_ref[...] * slope).astype(jnp.bfloat16)
    score_pad[pl.ds(1, frames), pl.ds(1, RING)] = score.reshape(frames, RING, cols, chans)
    halo_start(1, score_pad, score.astype(jnp.float32))

    input_grad = conv(
        1, score_pad, True, lambda: halo_wait(1, score_pad), lambda: None
    ).astype(jnp.bfloat16)
    grad_pad[pl.ds(shift + 1, frames), pl.ds(1, RING)] = input_grad.reshape(
        frames, RING, cols, chans
    )
    halo_start(2, grad_pad, input_grad.astype(jnp.float32))

    value = score_pad[pl.ds(1, frames), pl.ds(1, RING)].reshape(count, chans).astype(jnp.float32)
    for mine, ref in ((True, cat_s.at[core]), (False, stage_s)):
        ref[...] = three(
            lane_half(value, mine),
            lane_half(edge_in[1, 0, 1], mine), lane_half(edge_in[1, 1, 1], mine),
        )
    pair_s = send(stage_s, cat_s.at[core], pair_send.at[2], pair_recv.at[2], partner)
    pair_s.start()

    back = penalty_weight * conv(
        2, grad_pad, False, lambda: halo_wait(2, grad_pad), pair_grads.start
    )
    pre_grad = back * head_ref[...] * curve_ref[...]
    value = pre_grad.astype(jnp.bfloat16).astype(jnp.float32)
    for side, rows_out in enumerate(edge_rows(value)):
        last_out[side] = rows_out
    def last_copy(r, c):
        side = 0 if r > 0 else 1
        other = core if c == 0 else 1 - core
        return send(
            last_out.at[side], last_in.at[side, c], last_send.at[side], last_recv.at[side],
            device(tm=me["tm"] - core + other, rows=me["rows"] + r),
        )

    for r in (-1, 1):
        @pl.when(inside(0, r))
        def _():
            for c in range(CORES):
                last_copy(r, c).start()

    stage_p[...] = lane_half(value, False).astype(jnp.bfloat16)
    pair_p = send(stage_p, raw_p.at[core], pair_send.at[3], pair_recv.at[3], partner)
    pair_p.start()
    raw_p[core] = lane_half(value).astype(jnp.bfloat16)

    small_mine[...] = jnp.zeros_like(small_mine)
    for k, value in enumerate((pre_grad, back * slope_ref[...])):
        whole = jnp.sum(value, axis=0, keepdims=True)
        small_mine[pl.ds(2 * k, 1)] = whole[:, :LANES]
        small_mine[pl.ds(2 * k + 1, 1)] = whole[:, LANES:]
    small_targets = [
        [partner],
        [chip(x=other) for other in ring_peers("x", RING)],
        [chip(y=other) for other in ring_peers("y", RING)],
        [chip(z=other) for other in ring_peers("z", DEEP)],
    ]
    smalls = []

    def small_start(level):
        at = sum(len(group) for group in small_targets[:level])
        copies = []
        for k, target in enumerate(small_targets[level]):
            copy = send(
                small_mine.at[pl.ds(level * SUB, SUB)], small_land.at[pl.ds((at + k) * SUB, SUB)],
                small_send.at[0], small_recv.at[level], target,
            )
            copy.start()
            copies.append(at + k)
        smalls.append(copies)

    def small_end(level):
        value = small_mine[pl.ds(level * SUB, SUB)]
        slots = smalls[level]
        lands = small_land.at[pl.ds(slots[0] * SUB, len(slots) * SUB)]
        send(lands, lands, small_send.at[0], small_recv.at[level], partner).wait_recv()
        for slot in slots:
            value = value + small_land[pl.ds(slot * SUB, SUB)]
        small_mine[pl.ds((level + 1) * SUB, SUB)] = value

    small_start(0)

    routes = []
    for p in range(PARTS):
        first, second = ("x", "y") if p < GROUPS else ("y", "x")
        m = here[first]
        ways = []
        for v in range(WAYS):
            if v == 0:
                near, bit1, far, bit2 = flip(m), lax.rem((m + 1) // 2, 2), mirror(m), m // 2
            else:
                near, bit1, far, bit2 = mirror(m), m // 2, flip(m), lax.rem(m, 2)
            four = 8 * v + 4 * bit1
            two = four + 2 * bit2
            ways.append(dict(
                near=chip(**{first: near}), far=chip(**{first: far}),
                four=four, other4=16 * v + 4 - four, two=two, other2=2 * four + 2 - two,
            ))
        routes.append(dict(ways=ways, second=second))

    def unit_of(p, n):
        low, high = (way["two"] for way in routes[p]["ways"])
        upper = n // 2
        return (1 - upper) * (low + n) + upper * (high + n - 2)

    for p, route in enumerate(routes):
        route["unit"] = unit_of(p, here[route["second"]])

    def encode(p, base, units, code, at):
        def peak(k, tops):
            for t in range(SHARE):
                tops = jnp.maximum(tops, jnp.abs(total[p, base + k, t]))
            return tops

        top = lax.fori_loop(
            0, units, peak, jnp.zeros((SUB, LANES), jnp.float32), unroll=min(units, UNROLL)
        )
        top = (top * 1.01 + 1e-30).astype(jnp.bfloat16)
        rate = SPAN / top.astype(jnp.float32)
        code[(*at, units * SHARE)] = top

        def fill(k, carry):
            code[(*at, pl.ds(k * SHARE, SHARE))] = jnp.exp2(
                total[p, base + k] * rate[None]
            ).astype(jnp.bfloat16)
            return carry

        lax.fori_loop(0, units, fill, 0, unroll=min(units, UNROLL))

    def absorb(p, base, units, lands):
        scales = [
            land[(*at, units * SHARE)].astype(jnp.float32) * (1.0 / (SPAN * math.log(2.0)))
            for land, at in lands
        ]

        def add(k, carry):
            value = total[p, base + k]
            for (land, at), scale in zip(lands, scales):
                block = land[(*at, pl.ds(k * SHARE, SHARE))].astype(jnp.float32)
                value = value + jnp.log(block) * scale[None]
            total[p, base + k] = value
            return carry

        lax.fori_loop(0, units, add, 0, unroll=min(units, UNROLL))

    def halving(p, v, code, land, send_sem, recv_sem, to):
        return send(
            code.at[p, v], land.at[p, v], send_sem.at[0], recv_sem.at[p], routes[p]["ways"][v][to]
        )

    def arrived(block, recv_sem, slot):
        send(block, block, send1.at[0], recv_sem.at[slot], partner).wait_recv()

    def copy3(p):
        second = routes[p]["second"]
        return [
            send(
                code3.at[p, k], land3.at[p, k], send3.at[0], recv3.at[p],
                chip(**{second: other}),
            )
            for k, other in enumerate(ring_peers(second, RING))
        ]

    def start1(p):
        for v, way in enumerate(routes[p]["ways"]):
            encode(p, way["other4"], 4, code1, (p, v))
            halving(p, v, code1, land1, send1, recv1, "near").start()

    def start2(p):
        for v, way in enumerate(routes[p]["ways"]):
            encode(p, way["other2"], 2, code2, (p, v))
            halving(p, v, code2, land2, send2, recv2, "far").start()

    def start3(p):
        second = routes[p]["second"]
        for k, (copy, other) in enumerate(zip(copy3(p), ring_peers(second, RING))):
            encode(p, unit_of(p, other), 1, code3, (p, k))
            copy.start()

    def correlate(pad, cat, a, b):
        left = pad[a : a + 2 * frames, b : b + RING].reshape(2 * count, chans)
        right = cat[...].reshape(2 * count, cat.shape[-1])
        return lax.dot_general(
            left, right, (((0,), (0,)), ((), ())), preferred_element_type=jnp.float32
        )

    def tiles(value, h, d):
        block = value[h * UNITS * SUB : (h + 1) * UNITS * SUB, d * LANES : (d + 1) * LANES]
        return block.reshape(UNITS, SUB, LANES)

    def place(a, b, d):
        tap = (a * TAPS + b) * TAPS + d
        return tap // SHARE, tap % SHARE

    for h in range(2):
        total[h * GROUPS + GROUPS - 1, :, SHARE - 1] = jnp.zeros((UNITS, SUB, LANES), jnp.float32)
    pair_s.wait()
    pair_grads.wait()
    for a in range(TAPS):
        if a == 1:
            pair_clips.wait()
            pair_p.wait()
        for b in range(TAPS):
            value = penalty_weight * correlate(grad_pad, cat_s, a, b)
            level = correlate(clip_pad, raw_p, a, b) if a > 0 else None
            for d in range(TAPS):
                g, t = place(a, b, d)
                for h in range(2):
                    block = tiles(value, h, d)
                    if a > 0 and d == 1:
                        block = block + tiles(level, h, 0)
                    total[h * GROUPS + g, :, t] = block
    for b in range(TAPS):
        level = correlate(clip_pad, raw_p, 0, b)
        g, t = place(0, b, 1)
        for h in range(2):
            total[h * GROUPS + g, :, t] = total[h * GROUPS + g, :, t] + tiles(level, h, 0)
    for r in (-1, 1):
        side = 0 if r > 0 else 1
        both = last_in.at[side]
        copy = send(both, both, last_send.at[side], last_recv.at[side], partner)

        @pl.when(inside(0, r))
        def _():
            copy.wait_send()

        @pl.when(inside(0, -r))
        def _():
            copy.wait_recv()

    for c in range(CORES):
        at = core if c == 0 else 1 - core
        value = raw_p[at].astype(jnp.float32)
        cat_p[at] = jnp.concatenate([
            later(value, lane_half(last_in[1, c])), earlier(value, lane_half(last_in[0, c]))
        ], axis=1).astype(jnp.bfloat16)
    begun = 0
    for a in range(TAPS):
        for b in range(TAPS):
            value = correlate(clip_pad, cat_p, a, b)
            for d in (0, 2):
                g, t = place(a, b, d)
                for h in range(2):
                    p = h * GROUPS + g
                    block = tiles(value, h, d // 2)
                    total[p, :, t] = block + total[p, :, t]
            done = (a * TAPS + b + 1) * TAPS
            while begun < GROUPS and done >= min((begun + 1) * SHARE, TAPS**3):
                for h in range(2):
                    start1(h * GROUPS + begun)
                begun += 1

    small_end(0)
    small_start(1)
    order = [h * GROUPS + g for g in range(GROUPS) for h in range(2)]
    for p in order:
        arrived(land1.at[p], recv1, p)
        for v, way in enumerate(routes[p]["ways"]):
            absorb(p, way["four"], 4, [(land1, (p, v))])
        start2(p)
    small_end(1)
    small_start(2)
    for p in order:
        arrived(land2.at[p], recv2, p)
        for v, way in enumerate(routes[p]["ways"]):
            absorb(p, way["two"], 2, [(land2, (p, v))])
        start3(p)
    small_end(2)
    small_start(3)

    z = here["z"]

    def copy4(p):
        return send(code4.at[p], land4.at[z], send4.at[0], recv4.at[0], chip(z=p))

    for p in order:
        arrived(land3.at[p], recv3, p)
        absorb(p, routes[p]["unit"], 1, [(land3, (p, k)) for k in range(RING - 1)])

        @pl.when(z != p)
        def _():
            encode(p, routes[p]["unit"], 1, code4, (p,))
            copy4(p).start()

    unit = None
    for p in range(PARTS):
        term = jnp.where(z == p, routes[p]["unit"], 0)
        unit = term if unit is None else unit + term
    others = ring_peers("z", DEEP)
    seven = land4.at[pl.ds(0, DEEP - 1)]
    send(seven, seven, send4.at[0], recv4.at[0], partner).wait_recv()
    absorb(z, unit, 1, [(land4, (other,)) for other in others])
    encode(z, unit, 1, full, (z, core, unit))

    def zcopy(k, other):
        block = full.at[z, core, unit]
        return send(block, block, zsend.at[0], zrecv.at[z], chip(z=other))

    def zgot(p):
        block = full.at[p, core, routes[p]["unit"]]
        return send(block, block, zsend.at[0], zrecv.at[p], chip(z=p))

    for k, other in enumerate(others):
        zcopy(k, other).start()
    small_end(3)

    def qcopies(p):
        second = routes[p]["second"]
        block = full.at[p, core, routes[p]["unit"]]
        return [
            send(block, block, qsend.at[0], qrecv.at[p], chip(**{second: other}))
            for k, other in enumerate(ring_peers(second, RING))
        ]

    def far_copy(p, v):
        block = full.at[p, core, pl.ds(routes[p]["ways"][v]["two"], 2)]
        return send(block, block, far_send.at[0], far_recv.at[p], routes[p]["ways"][v]["far"])

    def near_copy(p, v):
        block = full.at[p, core, pl.ds(routes[p]["ways"][v]["four"], 4)]
        return send(block, block, near_send.at[0], near_recv.at[p], routes[p]["ways"][v]["near"])

    def core_start(p, second):
        for way in routes[p]["ways"]:
            block = full.at[p, core, pl.ds(way["other4"] if second else way["four"], 4)]
            send(block, block, core_send.at[0], core_recv.at[2 * (p % GROUPS) + second], partner).start()

    def units(count):
        return full.at[0, 0, pl.ds(0, count)]

    for p in order:
        @pl.when(z != p)
        def _():
            zgot(p).wait_recv()

        for copy in qcopies(p):
            copy.start()
    for p in order:
        arrived(units(RING - 1), qrecv, p)
        for v in range(WAYS):
            far_copy(p, v).start()
    def reveal(p, c, which):
        h, g = p // GROUPS, p % GROUPS
        taps = min(SHARE, TAPS**3 - g * SHARE)
        lane = pl.ds(pl.multiple_of(c * LANES, LANES), LANES)

        def one(base, k, carry):
            scale = full[p, c, base + k, SHARE].astype(jnp.float32) * (1.0 / (SPAN * math.log(2.0)))
            block = full[p, c, base + k, pl.ds(0, taps)].astype(jnp.float32)
            out_ref[pl.ds(g * SHARE, taps), h * UNITS + base + k, :, lane] = (
                jnp.log(block) * scale[None]
            )
            return carry

        for way in routes[p]["ways"]:
            lax.fori_loop(0, 4, functools.partial(one, way[which]), 0, unroll=UNROLL)

    for k, ref in enumerate((bias_out, head_out)):
        at = (len(small_targets)) * SUB + 2 * k
        ref[:, pl.ds(0, LANES)] = small_mine[pl.ds(at, 1)]
        ref[:, pl.ds(LANES, LANES)] = small_mine[pl.ds(at + 1, 1)]
    def reveal_core(p, second):
        if p < GROUPS:
            arrived(units(16), core_recv, 2 * p + second)
        reveal(p, 1 - core, "other4" if second else "four")

    for k, p in enumerate(order):
        arrived(units(4), far_recv, p)
        for v in range(WAYS):
            near_copy(p, v).start()
        core_start(p, 0)
        if k >= 1:
            reveal(order[k - 1], core, "four")
    reveal(order[-1], core, "four")
    for k, p in enumerate(order):
        reveal_core(p, 0)
        arrived(units(8), near_recv, p)
        core_start(p, 1)
        if k >= 1:
            reveal(order[k - 1], core, "other4")
        if k >= 4:
            reveal_core(order[k - 4], 1)
    reveal(order[-1], core, "other4")
    for p in order[-4:]:
        reveal_core(p, 1)
    for block, sem in (
        (small_land, small_send), (code1, send1), (code2, send2), (code3, send3),
        (code4.at[pl.ds(0, DEEP - 1)], send4), (full.at[0, 0, pl.ds(0, DEEP - 1)], zsend),
        (full.at[pl.ds(0, 3), 0, pl.ds(0, 8)], qsend), (full.at[0], far_send),
        (full.at[pl.ds(0, 2)], near_send), (full.at[pl.ds(0, 4)], core_send),
    ):
        send(block, block, sem.at[0], sem.at[0], partner).wait_send()


def store_kernel(grad_ref, bias_ref, head_ref, grad_out, bias_out, head_out, sem):
    step = TAPS
    copies = [
        pltpu.make_async_copy(
            grad_ref.at[pl.ds(k * step, step)], grad_out.at[pl.ds(k * step, step)], sem.at[k]
        )
        for k in range(TAPS**3 // step)
    ]
    copies.append(pltpu.make_async_copy(bias_ref, bias_out, sem.at[TAPS**2]))
    copies.append(pltpu.make_async_copy(head_ref, head_out, sem.at[TAPS**2 + 1]))
    for copy in copies:
        copy.start()
    for copy in copies:
        copy.wait()


def per_device(sizes, clips, weight, bias, head):
    _, frames, _, cols, chans = clips.shape
    count = frames * cols
    lines = frames * RING
    dp, tm, rows = sizes
    assert (rows, dp * 2, tm // 4, chans) == (RING, RING, DEEP, 2 * LANES)
    dma = pltpu.SemaphoreType.DMA
    vmem = pl.BlockSpec(memory_space=pltpu.VMEM)
    hbm = pl.BlockSpec(memory_space=pltpu.HBM)
    row = jax.ShapeDtypeStruct((1, chans), jnp.float32)
    field = pltpu.VMEM((count, chans), jnp.float32)

    def pad(n):
        return pltpu.VMEM((n, RING + 2, cols // RING, chans), jnp.bfloat16)

    def coded(*lead, units):
        return pltpu.VMEM((*lead, units * SHARE + 1, SUB, LANES), jnp.bfloat16)

    cat = pltpu.VMEM((CORES, count, TAPS * LANES), jnp.bfloat16)
    stage = pltpu.VMEM((count, TAPS * LANES), jnp.bfloat16)
    smalls = 1 + 2 * (RING - 1) + DEEP - 1
    both = lambda n: [dma((n,)), dma((n,))]
    one = lambda n: [dma((1,)), dma((n,))]
    grad_weight, grad_bias, grad_head = pl.pallas_call(
        functools.partial(kernel, sizes),
        out_shape=(
            jax.ShapeDtypeStruct((TAPS**3, 2 * UNITS, SUB, chans), jnp.float32),
            row, row,
        ),
        in_specs=[hbm, hbm, hbm, hbm],
        out_specs=(vmem, vmem, vmem),
        scratch_shapes=[
            pltpu.VMEM((1, chans), jnp.float32), pltpu.VMEM((1, chans), jnp.float32),
            pltpu.VMEM((TAPS**3, chans, chans), jnp.bfloat16),
            pltpu.VMEM((frames, cols, chans), jnp.bfloat16),
            pad(2 * frames + 2), pad(frames + 2), pad(2 * frames + 2),
            pltpu.VMEM((TAPS, count, chans), jnp.float32),
            field, field,
            cat, pltpu.VMEM((CORES, count, 2 * LANES), jnp.bfloat16), stage, pltpu.VMEM((count, LANES), jnp.bfloat16),
            pltpu.VMEM((CORES, count, LANES), jnp.bfloat16),
            pltpu.VMEM((RING, SUB, chans), jnp.bfloat16),
            pltpu.VMEM((3, RING, SUB, chans), jnp.bfloat16),
            pltpu.VMEM((2, 2, lines, chans), jnp.float32),
            pltpu.VMEM((TAPS, 2, 3, lines, chans), jnp.float32),
            pltpu.VMEM((2, lines, chans), jnp.float32),
            pltpu.VMEM((2, CORES, lines, chans), jnp.float32),
            pltpu.VMEM((PARTS, UNITS, SHARE, SUB, LANES), jnp.float32),
            coded(PARTS, WAYS, units=4), coded(PARTS, WAYS, units=4),
            coded(PARTS, WAYS, units=2), coded(PARTS, WAYS, units=2),
            coded(PARTS, RING - 1, units=1), coded(PARTS, RING - 1, units=1),
            coded(DEEP, units=1), coded(DEEP, units=1),
            coded(PARTS, CORES, UNITS, units=1),
            pltpu.VMEM((5 * SUB, LANES), jnp.float32),
            pltpu.VMEM((smalls * SUB, LANES), jnp.float32),
            dma((4,)), *both(6), *both(16), *both(2), *both(4),
            *one(PARTS), *one(PARTS), *one(PARTS), *one(1),
            *one(DEEP), *one(PARTS), *one(PARTS), *one(PARTS), *one(2 * GROUPS), *one(4),
        ],
        compiler_params=pltpu.CompilerParams(
            collective_id=0, has_side_effects=True, vmem_limit_bytes=40 * 1024 * 1024
        ),
    )(
        *[
            pltpu.with_memory_space_constraint(value, pltpu.HBM)
            for value in (
                clips.reshape(frames, cols, chans), weight.reshape(TAPS**3, chans, chans),
                bias.reshape(1, chans), head.reshape(1, chans),
            )
        ]
    )
    grad_weight, grad_bias, grad_head = pl.pallas_call(
        store_kernel,
        out_shape=(
            jax.ShapeDtypeStruct((TAPS**3, 2 * UNITS, SUB, chans), jnp.float32), row, row,
        ),
        in_specs=[vmem, vmem, vmem],
        out_specs=(hbm, hbm, hbm),
        scratch_shapes=[dma((TAPS**2 + 2,))],
        compiler_params=pltpu.CompilerParams(vmem_limit_bytes=8 * 1024 * 1024),
    )(grad_weight, grad_bias, grad_head)
    grad_weight = grad_weight.reshape(TAPS, TAPS, TAPS, chans, chans)
    return grad_weight, grad_bias.reshape(chans), grad_head.reshape(chans)


def solution(mesh):
    sizes = tuple(mesh.shape[axis] for axis in ("dp", "tm", "rows"))
    return jax.shard_map(
        functools.partial(per_device, sizes),
        mesh=mesh,
        in_specs=(P("dp", "tm", "rows", None, None), P(), P(), P()),
        out_specs=(P(), P(), P()),
        check_vma=False,
    )
```

```python
import functools
import math

import jax
import jax.numpy as jnp
from jax import lax
from jax.experimental import pallas as pl
from jax.experimental.pallas import tpu as pltpu
from jax.sharding import PartitionSpec as P

penalty_weight = 0.01
MESH = pl.DeviceIdType.MESH
SUB = 8
LANES = 128
TAPS = 3
SPAN = 120.0
RING = 4
DEEP = 8
CORES = 2
GROUPS = 4
SHARE = 7
UNITS = 16
UNROLL = 4
WAYS = 2
PARTS = 2 * GROUPS


def flip(m):
    return m + 1 - 2 * lax.rem(m, 2)


def mirror(m):
    return RING - 1 - m


def kernel(
    sizes, clips_ref, weight_ref, bias_hbm, head_hbm,
    out_ref, bias_out, head_out,
    bias_ref, head_ref, w_ref, clips_vm, clip_pad, score_pad, grad_pad, acc, slope_ref, curve_ref,
    cat_s, cat_p, stage_s, stage_p, raw_p, side_out, side_in, edge_out, edge_in, last_out, last_in, total,
    code1, land1, code2, land2, code3, land3, code4, land4, full, small_mine, small_land,
    local_sem, turn_send, turn_recv, halo_send, halo_recv, last_send, last_recv,
    pair_send, pair_recv, send1, recv1, send2, recv2,
    send3, recv3, send4, recv4, zsend, zrecv, qsend, qrecv, near_send, near_recv,
    far_send, far_recv, core_send, core_recv, small_send, small_recv,
):
    dp, tm, rows = sizes
    frames, wide, chans = clips_ref.shape
    cols = wide // RING
    lines = frames * RING
    count = lines * cols
    half = count // 2
    me = {"dp": lax.axis_index("dp"), "tm": lax.axis_index("tm"), "rows": lax.axis_index("rows")}
    core = lax.rem(me["tm"], CORES)
    here = {
        "x": me["rows"],
        "y": 2 * me["dp"] + lax.rem(me["tm"] // 2, 2),
        "z": me["tm"] // 4,
        "c": core,
    }

    def device(**moved):
        place = dict(me, **moved)
        return (place["dp"], place["tm"], place["rows"])

    def chip(**moved):
        place = dict(here, **moved)
        return (
            place["y"] // 2,
            place["z"] * 4 + lax.rem(place["y"], 2) * 2 + place["c"],
            place["x"],
        )

    partner = chip(c=1 - core)

    def ring_peers(axis, size):
        return [lax.rem(here[axis] + step, size) for step in range(1, size)]

    weight_copy = pltpu.make_async_copy(weight_ref, w_ref, local_sem.at[0])
    weight_copy.start()
    shift = 2 * core
    clip_copy = pltpu.make_async_copy(clips_ref, clips_vm, local_sem.at[1])
    clip_copy.start()
    bias_copy = pltpu.make_async_copy(bias_hbm, bias_ref, local_sem.at[2])
    head_copy = pltpu.make_async_copy(head_hbm, head_ref, local_sem.at[3])
    bias_copy.start()
    head_copy.start()
    for pad, base in ((clip_pad, shift), (score_pad, 0), (grad_pad, shift)):
        pad[:, 0] = jnp.zeros((pad.shape[0], cols, chans), pad.dtype)
        pad[:, RING + 1] = jnp.zeros((pad.shape[0], cols, chans), pad.dtype)
        for at in (base, base + frames + 1):
            pad[at, pl.ds(1, RING)] = jnp.zeros((RING, cols, chans), pad.dtype)
    edge_in[...] = jnp.zeros_like(edge_in)
    side_in[...] = jnp.zeros_like(side_in)
    last_in[...] = jnp.zeros_like(last_in)

    moves = [(t, r) for t in (-1, 0, 1) for r in (-1, 0, 1) if (t, r) != (0, 0)]

    def inside(t, r):
        ok = None
        for axis, step, size in (("tm", t, tm), ("rows", r, rows)):
            if step:
                cond = me[axis] > 0 if step < 0 else me[axis] < size - 1
                ok = cond if ok is None else jnp.logical_and(ok, cond)
        return ok

    barrier = pltpu.get_barrier_semaphore()
    friends = [partner]
    friends += [chip(x=other) for other in ring_peers("x", RING)]
    friends += [chip(y=other) for other in ring_peers("y", RING)]
    friends += [chip(z=other) for other in ring_peers("z", DEEP)]
    for friend in friends:
        pl.semaphore_signal(barrier, inc=1, device_id=friend, device_id_type=MESH)
    expected = len(friends)
    for t in (-1, 1):
        expected = expected + RING * inside(t, 0).astype(jnp.int32)

        @pl.when(inside(t, 0))
        def _():
            for row in range(RING):
                pl.semaphore_signal(
                    barrier, inc=1, device_id=device(tm=me["tm"] + t, rows=row),
                    device_id_type=MESH,
                )
    pl.semaphore_wait(barrier, expected)

    def send(src, dst, send_sem, recv_sem, target):
        return pltpu.make_async_remote_copy(
            src_ref=src, dst_ref=dst, send_sem=send_sem, recv_sem=recv_sem,
            device_id=target, device_id_type=MESH,
        )

    def turn_copy(t, step):
        other = lax.rem(me["rows"] + step, RING)
        part = pl.ds(pl.multiple_of(other * cols, cols), cols)
        base = shift if t == 0 else 2 - shift
        src = {0: pl.ds(0, frames), 1: pl.ds(frames - 1, 1), -1: pl.ds(0, 1)}[t]
        dst = {0: pl.ds(base + 1, frames), 1: pl.ds(base, 1), -1: pl.ds(base + frames + 1, 1)}[t]
        return send(
            clips_vm.at[src, part], clip_pad.at[dst, 1 + me["rows"]],
            turn_send.at[1 + t], turn_recv.at[1 + t],
            device(tm=me["tm"] + t, rows=other),
        )

    def side_copy(t, step):
        other = lax.rem(me["rows"] + step, RING)
        return send(
            side_out.at[other], side_in.at[1 - t, me["rows"]],
            turn_send.at[4 + t], turn_recv.at[4 + t],
            device(tm=me["tm"] + t, rows=other),
        )

    def turn_start():
        for step in range(1, RING):
            turn_copy(0, step).start()
        for other in range(RING):
            at = other * cols
            lines_out = [
                clips_vm[f, c : c + 1].astype(jnp.float32) if 0 <= c < wide
                else jnp.zeros((1, chans), jnp.float32)
                for c in (at - 1, at + cols) for f in range(frames)
            ]
            lines_out.append(jnp.zeros((SUB - 2 * frames, chans), jnp.float32))
            side_out[other] = jnp.concatenate(lines_out, axis=0).astype(jnp.bfloat16)
        for step in range(1, RING):
            side_copy(0, step).start()
        for t in (-1, 1):
            @pl.when(inside(t, 0))
            def _():
                for step in range(RING):
                    turn_copy(t, step).start()
                    side_copy(t, step).start()
        side_in[1, me["rows"]] = side_out[me["rows"]]

    def turn_wait(level):
        if level:
            block = clip_pad.at[pl.ds(shift + 1, frames), pl.ds(1, RING - 1)]
            copy = send(block, block, turn_send.at[1], turn_recv.at[1], partner)
            copy.wait_recv()
            copy.wait_send()
            return
        block = side_in.at[1, pl.ds(0, RING - 1)]
        copy = send(block, block, turn_send.at[4], turn_recv.at[4], partner)
        copy.wait_recv()
        copy.wait_send()
        for t in (-1, 1):
            block, side = clip_pad.at[shift, pl.ds(1, RING)], side_in.at[0]
            copies = [
                send(block, block, turn_send.at[1 + t], turn_recv.at[1 + t], partner),
                send(side, side, turn_send.at[4 + t], turn_recv.at[4 + t], partner),
            ]

            @pl.when(inside(t, 0))
            def _():
                for copy in copies:
                    copy.wait_send()

            @pl.when(inside(-t, 0))
            def _():
                for copy in copies:
                    copy.wait_recv()

        line = lax.broadcasted_iota(jnp.int32, (lines, chans), 0)
        for k in range(3):
            blocks = [side_in[k, r].astype(jnp.float32) for r in range(RING)]
            for side in range(2):
                value = jnp.zeros((lines, chans), jnp.float32)
                for r in range(RING):
                    for f in range(frames):
                        at = side * frames + f
                        value = jnp.where(
                            line == f * RING + r,
                            jnp.broadcast_to(blocks[r][at : at + 1], (lines, chans)), value,
                        )
                edge_in[0, side, k] = value

    def halo_copy(which, pad, t, r):
        slot = (which - 1) * len(moves) + moves.index((t, r))
        target = device(tm=me["tm"] + t, rows=me["rows"] + r)
        sems = halo_send.at[slot], halo_recv.at[slot]
        if r != 0:
            side = 0 if r > 0 else 1
            return send(edge_out.at[which - 1, side], edge_in.at[which, side, 1 - t], *sems, target)
        pair = pad.shape[0] > frames + 2
        mine, base = (shift, 2 - shift) if pair else (0, 0)
        src = mine + frames if t > 0 else mine + 1
        dst = base if t > 0 else base + frames + 1
        return send(
            pad.at[src, pl.ds(1, RING)], pad.at[dst, pl.ds(1, RING)], *sems, target
        )

    def edge_rows(value):
        block = value.reshape(lines, cols, value.shape[-1])
        return block[:, cols - 1], block[:, 0]

    def halo_start(which, pad, value):
        for level in (True, False):
            if not level:
                for side, rows_out in enumerate(edge_rows(value)):
                    edge_out[which - 1, side] = rows_out
            for t, r in moves:
                if (r == 0) != level:
                    continue

                @pl.when(inside(t, r))
                def _():
                    halo_copy(which, pad, t, r).start()

    def halo_wait(which, pad):
        for t, r in moves:
            @pl.when(inside(t, r))
            def _():
                halo_copy(which, pad, t, r).wait_send()

            @pl.when(inside(-t, -r))
            def _():
                halo_copy(which, pad, t, r).wait_recv()

    def columns(value):
        return lax.rem(lax.broadcasted_iota(jnp.int32, value.shape, 0), cols)

    def spread(edge):
        return jnp.broadcast_to(edge[:, None, :], (lines, cols, edge.shape[-1])).reshape(count, -1)

    def earlier(value, edge):
        return jnp.where(columns(value) == 0, spread(edge), pltpu.roll(value, 1, 0))

    def later(value, edge):
        return jnp.where(columns(value) == cols - 1, spread(edge), pltpu.roll(value, count - 1, 0))

    def pair_frames(pad, slot):
        block = pad.at[pl.ds(4 * core, 2), pl.ds(1, RING)]
        return send(block, block, pair_send.at[slot], pair_recv.at[slot], partner)

    def edge_left(which):
        line = lax.broadcasted_iota(jnp.int32, (lines, chans), 0)
        row = lax.rem(line, RING)

        def piece(side, s, q):
            below, level, above = (edge_in[which, side, k] for k in range(3))
            if s == 1:
                value = level
            else:
                value = pltpu.roll(level, RING, 0)
                if s == 0:
                    value = jnp.where(line < RING, pltpu.roll(below, RING, 0), value)
                else:
                    value = jnp.where(line < RING, value, pltpu.roll(above, RING, 0))
            if q == 0:
                value = jnp.where(row == 0, 0.0, pltpu.roll(value, 1, 0))
            elif q == 2:
                value = jnp.where(row == RING - 1, 0.0, pltpu.roll(value, lines - 1, 0))
            return value

        return [
            jnp.concatenate([
                jnp.concatenate([piece(side, s, q) for q in range(TAPS)], axis=1)
                for side in range(2)
            ], axis=0).astype(jnp.bfloat16)
            for s in range(TAPS)
        ]

    def conv(which, pad, transpose, wait, ready):
        base = shift if pad.shape[0] > frames + 2 else 0

        def left(at, size):
            return jnp.concatenate([
                pad[pl.ds(base + at, size), pl.ds(q, RING)].reshape(size * half, chans)
                for q in range(TAPS)
            ], axis=1)

        def product(value, s, d):
            a = TAPS - 1 - s if transpose else s
            taps = [
                w_ref[(a * TAPS + (TAPS - 1 - q if transpose else q)) * TAPS + d]
                for q in range(TAPS)
            ]
            if transpose:
                return lax.dot_general(
                    value, jnp.concatenate(taps, axis=1), (((1,), (1,)), ((), ())),
                    preferred_element_type=jnp.float32,
                )
            return jnp.dot(
                value, jnp.concatenate(taps, axis=0), preferred_element_type=jnp.float32
            )

        own = left(1, frames)
        for d in range(TAPS):
            level = product(own, 1, d)
            acc[d, pl.ds(0, half)] = level[:half] + product(own[half:], 2, d)
            acc[d, pl.ds(half, half)] = level[half:] + product(own[:half], 0, d)
        wait()
        ready()
        edges = edge_left(which)
        below = jnp.concatenate([left(0, 1), edges[0]], axis=0)
        above = jnp.concatenate([left(frames + 1, 1), edges[2]], axis=0)
        sums, sides = [], []
        for d in range(TAPS):
            low, high = product(below, 0, d), product(above, 2, d)
            sums.append(jnp.concatenate([
                acc[d, pl.ds(0, half)] + low[:half], acc[d, pl.ds(half, half)] + high[:half]
            ], axis=0))
            sides.append(
                None if d == 1 else low[half:] + high[half:] + product(edges[1], 1, d)
            )
        d0, d2 = (2, 0) if transpose else (0, 2)
        return (
            earlier(sums[d0], sides[d0][:lines]) + sums[1] + later(sums[d2], sides[d2][lines:])
        )


    def lane_half(value, mine=True):
        low, high = value[:, :LANES], value[:, LANES:]
        return jnp.where(core == 0, low, high) if mine else jnp.where(core == 0, high, low)

    def three(value, before, after):
        return jnp.concatenate(
            [later(value, after), value, earlier(value, before)], axis=1
        ).astype(jnp.bfloat16)

    clip_copy.wait()
    turn_start()
    mine = pl.ds(pl.multiple_of(me["rows"] * cols, cols), cols)
    clip_pad[pl.ds(shift + 1, frames), 1 + me["rows"]] = clips_vm[:, mine]
    weight_copy.wait()
    bias_copy.wait()
    head_copy.wait()
    pair_clips, pair_grads = pair_frames(clip_pad, 0), pair_frames(grad_pad, 1)
    turn_wait(True)
    pre = conv(0, clip_pad, False, lambda: turn_wait(False), pair_clips.start) + bias_ref[...]
    sig = jax.nn.sigmoid(pre)
    slope = sig * (1.0 + pre * (1.0 - sig))
    slope_ref[...] = slope
    curve_ref[...] = sig * (1.0 - sig) * (2.0 + pre * (1.0 - 2.0 * sig))
    score = (head_ref[...] * slope).astype(jnp.bfloat16)
    score_pad[pl.ds(1, frames), pl.ds(1, RING)] = score.reshape(frames, RING, cols, chans)
    halo_start(1, score_pad, score.astype(jnp.float32))

    input_grad = conv(
        1, score_pad, True, lambda: halo_wait(1, score_pad), lambda: None
    ).astype(jnp.bfloat16)
    grad_pad[pl.ds(shift + 1, frames), pl.ds(1, RING)] = input_grad.reshape(
        frames, RING, cols, chans
    )
    halo_start(2, grad_pad, input_grad.astype(jnp.float32))

    value = score_pad[pl.ds(1, frames), pl.ds(1, RING)].reshape(count, chans).astype(jnp.float32)
    for mine, ref in ((True, cat_s.at[core]), (False, stage_s)):
        ref[...] = three(
            lane_half(value, mine),
            lane_half(edge_in[1, 0, 1], mine), lane_half(edge_in[1, 1, 1], mine),
        )
    pair_s = send(stage_s, cat_s.at[core], pair_send.at[2], pair_recv.at[2], partner)
    pair_s.start()

    back = penalty_weight * conv(
        2, grad_pad, False, lambda: halo_wait(2, grad_pad), pair_grads.start
    )
    pre_grad = back * head_ref[...] * curve_ref[...]
    value = pre_grad.astype(jnp.bfloat16).astype(jnp.float32)
    for side, rows_out in enumerate(edge_rows(value)):
        last_out[side] = rows_out
    def last_copy(r, c):
        side = 0 if r > 0 else 1
        other = core if c == 0 else 1 - core
        return send(
            last_out.at[side], last_in.at[side, c], last_send.at[side], last_recv.at[side],
            device(tm=me["tm"] - core + other, rows=me["rows"] + r),
        )

    for r in (-1, 1):
        @pl.when(inside(0, r))
        def _():
            for c in range(CORES):
                last_copy(r, c).start()

    stage_p[...] = lane_half(value, False).astype(jnp.bfloat16)
    pair_p = send(stage_p, raw_p.at[core], pair_send.at[3], pair_recv.at[3], partner)
    pair_p.start()
    raw_p[core] = lane_half(value).astype(jnp.bfloat16)

    small_mine[...] = jnp.zeros_like(small_mine)
    for k, value in enumerate((pre_grad, back * slope_ref[...])):
        whole = jnp.sum(value, axis=0, keepdims=True)
        small_mine[pl.ds(2 * k, 1)] = whole[:, :LANES]
        small_mine[pl.ds(2 * k + 1, 1)] = whole[:, LANES:]
    small_targets = [
        [partner],
        [chip(x=other) for other in ring_peers("x", RING)],
        [chip(y=other) for other in ring_peers("y", RING)],
        [chip(z=other) for other in ring_peers("z", DEEP)],
    ]
    smalls = []

    def small_start(level):
        at = sum(len(group) for group in small_targets[:level])
        copies = []
        for k, target in enumerate(small_targets[level]):
            copy = send(
                small_mine.at[pl.ds(level * SUB, SUB)], small_land.at[pl.ds((at + k) * SUB, SUB)],
                small_send.at[0], small_recv.at[level], target,
            )
            copy.start()
            copies.append(at + k)
        smalls.append(copies)

    def small_end(level):
        value = small_mine[pl.ds(level * SUB, SUB)]
        slots = smalls[level]
        lands = small_land.at[pl.ds(slots[0] * SUB, len(slots) * SUB)]
        send(lands, lands, small_send.at[0], small_recv.at[level], partner).wait_recv()
        for slot in slots:
            value = value + small_land[pl.ds(slot * SUB, SUB)]
        small_mine[pl.ds((level + 1) * SUB, SUB)] = value

    small_start(0)

    routes = []
    for p in range(PARTS):
        first, second = ("x", "y") if p < GROUPS else ("y", "x")
        m = here[first]
        ways = []
        for v in range(WAYS):
            if v == 0:
                near, bit1, far, bit2 = flip(m), lax.rem((m + 1) // 2, 2), mirror(m), m // 2
            else:
                near, bit1, far, bit2 = mirror(m), m // 2, flip(m), lax.rem(m, 2)
            four = 8 * v + 4 * bit1
            two = four + 2 * bit2
            ways.append(dict(
                near=chip(**{first: near}), far=chip(**{first: far}),
                four=four, other4=16 * v + 4 - four, two=two, other2=2 * four + 2 - two,
            ))
        routes.append(dict(ways=ways, second=second))

    def unit_of(p, n):
        low, high = (way["two"] for way in routes[p]["ways"])
        upper = n // 2
        return (1 - upper) * (low + n) + upper * (high + n - 2)

    for p, route in enumerate(routes):
        route["unit"] = unit_of(p, here[route["second"]])

    def encode(p, base, units, code, at):
        def peak(k, tops):
            for t in range(SHARE):
                tops = jnp.maximum(tops, jnp.abs(total[p, base + k, t]))
            return tops

        top = lax.fori_loop(
            0, units, peak, jnp.zeros((SUB, LANES), jnp.float32), unroll=min(units, UNROLL)
        )
        top = (top * 1.01 + 1e-30).astype(jnp.bfloat16)
        rate = SPAN / top.astype(jnp.float32)
        code[(*at, units * SHARE)] = top

        def fill(k, carry):
            code[(*at, pl.ds(k * SHARE, SHARE))] = jnp.exp2(
                total[p, base + k] * rate[None]
            ).astype(jnp.bfloat16)
            return carry

        lax.fori_loop(0, units, fill, 0, unroll=min(units, UNROLL))

    def absorb(p, base, units, lands):
        scales = [
            land[(*at, units * SHARE)].astype(jnp.float32) * (1.0 / (SPAN * math.log(2.0)))
            for land, at in lands
        ]

        def add(k, carry):
            value = total[p, base + k]
            for (land, at), scale in zip(lands, scales):
                block = land[(*at, pl.ds(k * SHARE, SHARE))].astype(jnp.float32)
                value = value + jnp.log(block) * scale[None]
            total[p, base + k] = value
            return carry

        lax.fori_loop(0, units, add, 0, unroll=min(units, UNROLL))

    def halving(p, v, code, land, send_sem, recv_sem, to):
        return send(
            code.at[p, v], land.at[p, v], send_sem.at[0], recv_sem.at[p], routes[p]["ways"][v][to]
        )

    def arrived(block, recv_sem, slot):
        send(block, block, send1.at[0], recv_sem.at[slot], partner).wait_recv()

    def copy3(p):
        second = routes[p]["second"]
        return [
            send(
                code3.at[p, k], land3.at[p, k], send3.at[0], recv3.at[p],
                chip(**{second: other}),
            )
            for k, other in enumerate(ring_peers(second, RING))
        ]

    def start1(p):
        for v, way in enumerate(routes[p]["ways"]):
            encode(p, way["other4"], 4, code1, (p, v))
            halving(p, v, code1, land1, send1, recv1, "near").start()

    def start2(p):
        for v, way in enumerate(routes[p]["ways"]):
            encode(p, way["other2"], 2, code2, (p, v))
            halving(p, v, code2, land2, send2, recv2, "far").start()

    def start3(p):
        second = routes[p]["second"]
        for k, (copy, other) in enumerate(zip(copy3(p), ring_peers(second, RING))):
            encode(p, unit_of(p, other), 1, code3, (p, k))
            copy.start()

    def correlate(pad, cat, a, b):
        left = pad[a : a + 2 * frames, b : b + RING].reshape(2 * count, chans)
        right = cat[...].reshape(2 * count, cat.shape[-1])
        return lax.dot_general(
            left, right, (((0,), (0,)), ((), ())), preferred_element_type=jnp.float32
        )

    def tiles(value, h, d):
        block = value[h * UNITS * SUB : (h + 1) * UNITS * SUB, d * LANES : (d + 1) * LANES]
        return block.reshape(UNITS, SUB, LANES)

    def place(a, b, d):
        tap = (a * TAPS + b) * TAPS + d
        return tap // SHARE, tap % SHARE

    for h in range(2):
        total[h * GROUPS + GROUPS - 1, :, SHARE - 1] = jnp.zeros((UNITS, SUB, LANES), jnp.float32)
    pair_s.wait()
    pair_grads.wait()
    for a in range(TAPS):
        if a == 1:
            pair_clips.wait()
            pair_p.wait()
        for b in range(TAPS):
            value = penalty_weight * correlate(grad_pad, cat_s, a, b)
            level = correlate(clip_pad, raw_p, a, b) if a > 0 else None
            for d in range(TAPS):
                g, t = place(a, b, d)
                for h in range(2):
                    block = tiles(value, h, d)
                    if a > 0 and d == 1:
                        block = block + tiles(level, h, 0)
                    total[h * GROUPS + g, :, t] = block
    for b in range(TAPS):
        level = correlate(clip_pad, raw_p, 0, b)
        g, t = place(0, b, 1)
        for h in range(2):
            total[h * GROUPS + g, :, t] = total[h * GROUPS + g, :, t] + tiles(level, h, 0)
    for r in (-1, 1):
        side = 0 if r > 0 else 1
        both = last_in.at[side]
        copy = send(both, both, last_send.at[side], last_recv.at[side], partner)

        @pl.when(inside(0, r))
        def _():
            copy.wait_send()

        @pl.when(inside(0, -r))
        def _():
            copy.wait_recv()

    for c in range(CORES):
        at = core if c == 0 else 1 - core
        value = raw_p[at].astype(jnp.float32)
        cat_p[at] = jnp.concatenate([
            later(value, lane_half(last_in[1, c])), earlier(value, lane_half(last_in[0, c]))
        ], axis=1).astype(jnp.bfloat16)
    begun = 0
    for a in range(TAPS):
        for b in range(TAPS):
            value = correlate(clip_pad, cat_p, a, b)
            for d in (0, 2):
                g, t = place(a, b, d)
                for h in range(2):
                    p = h * GROUPS + g
                    block = tiles(value, h, d // 2)
                    total[p, :, t] = block + total[p, :, t]
            done = (a * TAPS + b + 1) * TAPS
            while begun < GROUPS and done >= min((begun + 1) * SHARE, TAPS**3):
                for h in range(2):
                    start1(h * GROUPS + begun)
                begun += 1

    small_end(0)
    small_start(1)
    order = [h * GROUPS + g for g in range(GROUPS) for h in range(2)]
    for p in order:
        arrived(land1.at[p], recv1, p)
        for v, way in enumerate(routes[p]["ways"]):
            absorb(p, way["four"], 4, [(land1, (p, v))])
        start2(p)
    small_end(1)
    small_start(2)
    for p in order:
        arrived(land2.at[p], recv2, p)
        for v, way in enumerate(routes[p]["ways"]):
            absorb(p, way["two"], 2, [(land2, (p, v))])
        start3(p)
    small_end(2)
    small_start(3)

    z = here["z"]

    def copy4(p):
        return send(code4.at[p], land4.at[z], send4.at[0], recv4.at[0], chip(z=p))

    for p in order:
        arrived(land3.at[p], recv3, p)
        absorb(p, routes[p]["unit"], 1, [(land3, (p, k)) for k in range(RING - 1)])

        @pl.when(z != p)
        def _():
            encode(p, routes[p]["unit"], 1, code4, (p,))
            copy4(p).start()

    unit = None
    for p in range(PARTS):
        term = jnp.where(z == p, routes[p]["unit"], 0)
        unit = term if unit is None else unit + term
    others = ring_peers("z", DEEP)
    seven = land4.at[pl.ds(0, DEEP - 1)]
    send(seven, seven, send4.at[0], recv4.at[0], partner).wait_recv()
    absorb(z, unit, 1, [(land4, (other,)) for other in others])
    encode(z, unit, 1, full, (z, core, unit))

    def zcopy(k, other):
        block = full.at[z, core, unit]
        return send(block, block, zsend.at[0], zrecv.at[z], chip(z=other))

    def zgot(p):
        block = full.at[p, core, routes[p]["unit"]]
        return send(block, block, zsend.at[0], zrecv.at[p], chip(z=p))

    for k, other in enumerate(others):
        zcopy(k, other).start()
    small_end(3)

    def qcopies(p):
        second = routes[p]["second"]
        block = full.at[p, core, routes[p]["unit"]]
        return [
            send(block, block, qsend.at[0], qrecv.at[p], chip(**{second: other}))
            for k, other in enumerate(ring_peers(second, RING))
        ]

    def far_copy(p, v):
        block = full.at[p, core, pl.ds(routes[p]["ways"][v]["two"], 2)]
        return send(block, block, far_send.at[0], far_recv.at[p], routes[p]["ways"][v]["far"])

    def near_copy(p, v):
        block = full.at[p, core, pl.ds(routes[p]["ways"][v]["four"], 4)]
        return send(block, block, near_send.at[0], near_recv.at[p], routes[p]["ways"][v]["near"])

    def core_start(p, second):
        for way in routes[p]["ways"]:
            block = full.at[p, core, pl.ds(way["other4"] if second else way["four"], 4)]
            send(block, block, core_send.at[0], core_recv.at[2 * (p % GROUPS) + second], partner).start()

    def units(count):
        return full.at[0, 0, pl.ds(0, count)]

    for p in order:
        @pl.when(z != p)
        def _():
            zgot(p).wait_recv()

        for copy in qcopies(p):
            copy.start()
    for p in order:
        arrived(units(RING - 1), qrecv, p)
        for v in range(WAYS):
            far_copy(p, v).start()
    def reveal(p, c, which):
        h, g = p // GROUPS, p % GROUPS
        taps = min(SHARE, TAPS**3 - g * SHARE)
        lane = pl.ds(pl.multiple_of(c * LANES, LANES), LANES)

        def one(base, k, carry):
            scale = full[p, c, base + k, SHARE].astype(jnp.float32) * (1.0 / (SPAN * math.log(2.0)))
            block = full[p, c, base + k, pl.ds(0, taps)].astype(jnp.float32)
            out_ref[pl.ds(g * SHARE, taps), h * UNITS + base + k, :, lane] = (
                jnp.log(block) * scale[None]
            )
            return carry

        for way in routes[p]["ways"]:
            lax.fori_loop(0, 4, functools.partial(one, way[which]), 0, unroll=UNROLL)

    for k, ref in enumerate((bias_out, head_out)):
        at = (len(small_targets)) * SUB + 2 * k
        ref[:, pl.ds(0, LANES)] = small_mine[pl.ds(at, 1)]
        ref[:, pl.ds(LANES, LANES)] = small_mine[pl.ds(at + 1, 1)]
    def reveal_core(p, second):
        if p < GROUPS:
            arrived(units(16), core_recv, 2 * p + second)
        reveal(p, 1 - core, "other4" if second else "four")

    for k, p in enumerate(order):
        arrived(units(4), far_recv, p)
        for v in range(WAYS):
            near_copy(p, v).start()
        core_start(p, 0)
        if k >= 1:
            reveal(order[k - 1], core, "four")
    reveal(order[-1], core, "four")
    for k, p in enumerate(order):
        reveal_core(p, 0)
        arrived(units(8), near_recv, p)
        core_start(p, 1)
        if k >= 1:
            reveal(order[k - 1], core, "other4")
        if k >= 4:
            reveal_core(order[k - 4], 1)
    reveal(order[-1], core, "other4")
    for p in order[-4:]:
        reveal_core(p, 1)
    for block, sem in (
        (small_land, small_send), (code1, send1), (code2, send2), (code3, send3),
        (code4.at[pl.ds(0, DEEP - 1)], send4), (full.at[0, 0, pl.ds(0, DEEP - 1)], zsend),
        (full.at[pl.ds(0, 3), 0, pl.ds(0, 8)], qsend), (full.at[0], far_send),
        (full.at[pl.ds(0, 2)], near_send), (full.at[pl.ds(0, 4)], core_send),
    ):
        send(block, block, sem.at[0], sem.at[0], partner).wait_send()


def store_kernel(grad_ref, bias_ref, head_ref, grad_out, bias_out, head_out, sem):
    step = TAPS**2
    copies = [
        pltpu.make_async_copy(
            grad_ref.at[pl.ds(k * step, step)], grad_out.at[pl.ds(k * step, step)], sem.at[k]
        )
        for k in range(TAPS**3 // step)
    ]
    copies.append(pltpu.make_async_copy(bias_ref, bias_out, sem.at[TAPS]))
    copies.append(pltpu.make_async_copy(head_ref, head_out, sem.at[TAPS + 1]))
    for copy in copies:
        copy.start()
    for copy in copies:
        copy.wait()


def per_device(sizes, clips, weight, bias, head):
    _, frames, _, cols, chans = clips.shape
    count = frames * cols
    lines = frames * RING
    dp, tm, rows = sizes
    assert (rows, dp * 2, tm // 4, chans) == (RING, RING, DEEP, 2 * LANES)
    dma = pltpu.SemaphoreType.DMA
    vmem = pl.BlockSpec(memory_space=pltpu.VMEM)
    hbm = pl.BlockSpec(memory_space=pltpu.HBM)
    row = jax.ShapeDtypeStruct((1, chans), jnp.float32)
    field = pltpu.VMEM((count, chans), jnp.float32)

    def pad(n):
        return pltpu.VMEM((n, RING + 2, cols // RING, chans), jnp.bfloat16)

    def coded(*lead, units):
        return pltpu.VMEM((*lead, units * SHARE + 1, SUB, LANES), jnp.bfloat16)

    cat = pltpu.VMEM((CORES, count, TAPS * LANES), jnp.bfloat16)
    stage = pltpu.VMEM((count, TAPS * LANES), jnp.bfloat16)
    smalls = 1 + 2 * (RING - 1) + DEEP - 1
    both = lambda n: [dma((n,)), dma((n,))]
    one = lambda n: [dma((1,)), dma((n,))]
    grad_weight, grad_bias, grad_head = pl.pallas_call(
        functools.partial(kernel, sizes),
        out_shape=(
            jax.ShapeDtypeStruct((TAPS**3, 2 * UNITS, SUB, chans), jnp.float32),
            row, row,
        ),
        in_specs=[hbm, hbm, hbm, hbm],
        out_specs=(vmem, vmem, vmem),
        scratch_shapes=[
            pltpu.VMEM((1, chans), jnp.float32), pltpu.VMEM((1, chans), jnp.float32),
            pltpu.VMEM((TAPS**3, chans, chans), jnp.bfloat16),
            pltpu.VMEM((frames, cols, chans), jnp.bfloat16),
            pad(2 * frames + 2), pad(frames + 2), pad(2 * frames + 2),
            pltpu.VMEM((TAPS, count, chans), jnp.float32),
            field, field,
            cat, pltpu.VMEM((CORES, count, 2 * LANES), jnp.bfloat16), stage, pltpu.VMEM((count, LANES), jnp.bfloat16),
            pltpu.VMEM((CORES, count, LANES), jnp.bfloat16),
            pltpu.VMEM((RING, SUB, chans), jnp.bfloat16),
            pltpu.VMEM((3, RING, SUB, chans), jnp.bfloat16),
            pltpu.VMEM((2, 2, lines, chans), jnp.float32),
            pltpu.VMEM((TAPS, 2, 3, lines, chans), jnp.float32),
            pltpu.VMEM((2, lines, chans), jnp.float32),
            pltpu.VMEM((2, CORES, lines, chans), jnp.float32),
            pltpu.VMEM((PARTS, UNITS, SHARE, SUB, LANES), jnp.float32),
            coded(PARTS, WAYS, units=4), coded(PARTS, WAYS, units=4),
            coded(PARTS, WAYS, units=2), coded(PARTS, WAYS, units=2),
            coded(PARTS, RING - 1, units=1), coded(PARTS, RING - 1, units=1),
            coded(DEEP, units=1), coded(DEEP, units=1),
            coded(PARTS, CORES, UNITS, units=1),
            pltpu.VMEM((5 * SUB, LANES), jnp.float32),
            pltpu.VMEM((smalls * SUB, LANES), jnp.float32),
            dma((4,)), *both(6), *both(16), *both(2), *both(4),
            *one(PARTS), *one(PARTS), *one(PARTS), *one(1),
            *one(DEEP), *one(PARTS), *one(PARTS), *one(PARTS), *one(2 * GROUPS), *one(4),
        ],
        compiler_params=pltpu.CompilerParams(
            collective_id=0, has_side_effects=True, vmem_limit_bytes=40 * 1024 * 1024
        ),
    )(
        *[
            pltpu.with_memory_space_constraint(value, pltpu.HBM)
            for value in (
                clips.reshape(frames, cols, chans), weight.reshape(TAPS**3, chans, chans),
                bias.reshape(1, chans), head.reshape(1, chans),
            )
        ]
    )
    grad_weight, grad_bias, grad_head = pl.pallas_call(
        store_kernel,
        out_shape=(
            jax.ShapeDtypeStruct((TAPS**3, 2 * UNITS, SUB, chans), jnp.float32), row, row,
        ),
        in_specs=[vmem, vmem, vmem],
        out_specs=(hbm, hbm, hbm),
        scratch_shapes=[dma((TAPS + 2,))],
        compiler_params=pltpu.CompilerParams(vmem_limit_bytes=8 * 1024 * 1024),
    )(grad_weight, grad_bias, grad_head)
    grad_weight = grad_weight.reshape(TAPS, TAPS, TAPS, chans, chans)
    return grad_weight, grad_bias.reshape(chans), grad_head.reshape(chans)


def solution(mesh):
    sizes = tuple(mesh.shape[axis] for axis in ("dp", "tm", "rows"))
    return jax.shard_map(
        functools.partial(per_device, sizes),
        mesh=mesh,
        in_specs=(P("dp", "tm", "rows", None, None), P(), P(), P()),
        out_specs=(P(), P(), P()),
        check_vma=False,
    )
```
